32 devices in a mesh: head: 4 (over y, core), blk: 8 (over z, x).
Axes of the slice: x: 2, y: 2, z: 4, core: 2. Of those that a mesh axis runs over, the one named last changes fastest.
Arguments:
- block_input: bfloat16 [4096, 1024], P(('head', 'blk')), may hold values from -6 to 6
- span_order: int32 [32], replicated, may hold values from 0 to 31, each once
- norm1_gain: bfloat16 [1024], P(('head', 'blk')), may hold values from 0.099609375 to 1.8984375
- w_query: bfloat16 [1024, 1024], P(('head', 'blk')), may hold values from -0.1875 to 0.1875
- key_weight: bfloat16 [1024, 512], P(('head', 'blk')), may hold values from -0.1875 to 0.1875
- value_weight: bfloat16 [1024, 512], P(('head', 'blk')), may hold values from -0.1875 to 0.1875
- qk_gain: float32 [2, 64], replicated, may hold values from 0.5 to 3, as said below
- w_out: bfloat16 [1024, 1024], P(('head', 'blk')), may hold values from -6 to 6
- norm2_gain: bfloat16 [1024], P(('head', 'blk')), may hold values from 0.099609375 to 1.8984375
- w_gate: bfloat16 [1024, 4608], P(('head', 'blk')), may hold values from -0.1875 to 0.1875
- w_up: bfloat16 [1024, 4608], P(('head', 'blk')), may hold values from -0.1875 to 0.1875
- w_down: bfloat16 [4608, 1024], P(('head', 'blk')), may hold values from -0.09375 to 0.09375
- out_grad: bfloat16 [4096, 1024], P(('head', 'blk')), may hold values from -6 to 6
Outputs:
- block_output: bfloat16 [4096, 1024], P(('head', 'blk'))
- input_grad: bfloat16 [4096, 1024], P(('head', 'blk'))
- norm1_grad: float32 [1024], P(('head', 'blk'))
- query_grad: float32 [1024, 1024], P(('head', 'blk'))
- key_grad: float32 [1024, 512], P(('head', 'blk'))
- value_grad: float32 [1024, 512], P(('head', 'blk'))
- qk_gain_grad: float32 [2, 64], replicated
- out_proj_grad: float32 [1024, 1024], P(('head', 'blk'))
- norm2_grad: float32 [1024], P(('head', 'blk'))
- gate_grad: float32 [1024, 4608], P(('head', 'blk'))
- up_grad: float32 [1024, 4608], P(('head', 'blk'))
- down_grad: float32 [4608, 1024], P(('head', 'blk'))
The draws below stay inside these ranges and needn't reach their ends.
Inputs may be any that keep to these rules, and one draw needn't show every extreme that they name: Storage span c of 128 rows holds the sequence positions from span_order[c] * 128 on; every span place occurs once. `qk_gain`: positive gains.
All inputs are finite; a program needn't handle non-finite values.
Results may differ from the reference program's by a relative error of at most 0.02.
The reference program's roundings to bfloat16 on the way count: a program that leaves them out, or rounds other values in their place, can miss the bound.
Values may be sent and summed in bfloat16 or wider, within the bound.
A program may use at most 512 MiB of HBM per device.

```python
import math
import jax
import jax.numpy as jnp
from jax import lax

MODEL_WIDTH = 1024
QUERY_HEADS = 16
KEY_VALUE_HEADS = 8
HEAD_SIZE = 64
FF = 4608
TOK_DEV = 128
TOKENS = 4096
NCHUNK = 32
N_HEAD = 4
N_BLK = 8


def draw_qk_gain(key, part):
    return jax.random.uniform(key, (2, HEAD_SIZE), jnp.float32, 0.5, 1.5)


def with_spikes(values, stream_key, source, target, shards_of, factor):
    owner, partner = [(jnp.arange(values.shape[dim]) // (values.shape[dim] // shards_of)).reshape([-1 if axis == dim else 1 for axis in range(values.ndim)]) for dim in (source, target)]
    chosen = jax.random.permutation(stream_key, shards_of)[partner]
    strong = (owner == chosen) | (owner == (partner + shards_of // 2) % shards_of)
    return jnp.where(strong, factor * values, values)


def steps_of(stream_key, extent, split, low, top_value):
    def one(axis_at, blocks):
        draws = jax.random.uniform(jax.random.fold_in(jax.random.fold_in(stream_key, 6), axis_at), (blocks,), jnp.float32, low / len(split), top_value / len(split))
        return jnp.repeat(jnp.exp(draws), extent[axis_at] // blocks).reshape((-1,) + (1,) * (len(extent) - axis_at - 1))

    loudness = one(*split[0])
    for cut in split[1:]:
        loudness = loudness * one(*cut)
    return loudness


def scatter_about(rng, dims, deviation, bound, split=(), held_as=jnp.bfloat16):
    loudness = steps_of(rng, dims, split, -0.22, 0.18) if split else 1.0
    values = jax.random.normal(rng, dims, jnp.float32) * deviation * loudness
    return jnp.minimum(jnp.maximum(values, -bound), bound).astype(held_as)


def gaussian_with(rng, shape, width, bound, cuts, heavy, kind=jnp.bfloat16):
    entries = width * jax.random.normal(rng, shape, jnp.float32)
    if cuts:
        entries = entries * steps_of(rng, shape, cuts, -0.22, 0.18)
    return jnp.clip(with_spikes(entries, jax.random.fold_in(rng, 3), *heavy), -bound, bound).astype(kind)


def setup_inputs(seed: int = 0) -> dict:
    splits = jax.random.split(jax.random.key(seed), 14)
    block_input = gaussian_with(splits[0], (TOKENS, MODEL_WIDTH), 1.0, 6.0, ((0, 32),), (0, 1, 32, 2.75))
    span_order = jax.random.permutation(splits[1], NCHUNK).astype(jnp.int32)
    norm1_gain = jnp.clip(1.0 + 0.18 * jax.random.normal(splits[2], (MODEL_WIDTH,), jnp.float32), 0.099609375, 1.8984375).astype(jnp.bfloat16)
    w_query = scatter_about(splits[3], (MODEL_WIDTH, QUERY_HEADS * HEAD_SIZE), MODEL_WIDTH ** -0.5, 0.1875, ((0, 32),))
    key_weight = scatter_about(splits[4], (MODEL_WIDTH, KEY_VALUE_HEADS * HEAD_SIZE), MODEL_WIDTH ** -0.5, 0.1875, ((0, 32),))
    value_weight = scatter_about(splits[5], (MODEL_WIDTH, KEY_VALUE_HEADS * HEAD_SIZE), MODEL_WIDTH ** -0.5, 0.1875, ((0, 32),))
    qk_gain = draw_qk_gain(jax.random.fold_in(splits[13], 71), 0)
    w_out = scatter_about(splits[7], (QUERY_HEADS * HEAD_SIZE, MODEL_WIDTH), ((TOK_DEV * N_HEAD * N_BLK) ** 0.5 * (QUERY_HEADS * HEAD_SIZE) ** -0.5 * 0.5), 6.0, ((0, 32),))
    norm2_gain = jnp.clip(1.0 + 0.18 * jax.random.normal(splits[8], (MODEL_WIDTH,), jnp.float32), 0.099609375, 1.8984375).astype(jnp.bfloat16)
    w_gate = scatter_about(splits[9], (MODEL_WIDTH, FF), MODEL_WIDTH ** -0.5, 0.1875, ((0, 32),))
    w_up = scatter_about(splits[10], (MODEL_WIDTH, FF), MODEL_WIDTH ** -0.5, 0.1875, ((0, 32),))
    w_down = scatter_about(splits[11], (FF, MODEL_WIDTH), FF ** -0.5, 0.09375, ((0, 32),))
    out_grad = gaussian_with(splits[12], (TOKENS, MODEL_WIDTH), 1.0, 6.0, ((0, 32),), (0, 1, 32, 2.75))
    return {"block_input": block_input, "span_order": span_order, "norm1_gain": norm1_gain, "w_query": w_query, "key_weight": key_weight, "value_weight": value_weight, "qk_gain": qk_gain, "w_out": w_out, "norm2_gain": norm2_gain, "w_gate": w_gate, "w_up": w_up, "w_down": w_down, "out_grad": out_grad}


EPS = 1e-05
THETA = 1000000.0
NEG = -1e+30

def rms_norm(values, gain_vec):
    inverse = lax.rsqrt(lax.optimization_barrier(jnp.mean(values * values, axis=-1, keepdims=True)) + EPS)
    return values * inverse * gain_vec

def rotate(field_in, where_at):
    half_size = field_in.shape[-1] // 2
    frequency = jnp.exp(jnp.arange(half_size, dtype=jnp.float32) * jnp.float32(-2.0 * math.log(THETA) / field_in.shape[-1]))
    angles = where_at.astype(jnp.float32)[:, None] * frequency[None, :]
    cosine = jnp.cos(angles)[:, None, :]
    sine_part = jnp.sin(angles)[:, None, :]
    first_half = field_in[..., :half_size]
    second_half = field_in[..., half_size:]
    return jnp.concatenate([first_half * cosine - second_half * sine_part, second_half * cosine + first_half * sine_part], axis=-1)

def head_map(raw_rows, gain_vec, where_at):
    row_count = raw_rows.shape[0]
    shaped = raw_rows.reshape(row_count, -1, gain_vec.shape[0])
    return rotate(rms_norm(shaped, gain_vec), where_at).reshape(row_count, -1)

def split_heads(tensor_data, rows_per_block, with_share):
    if with_share:
        return tensor_data.astype(jnp.float32).reshape(rows_per_block, KEY_VALUE_HEADS, QUERY_HEADS // KEY_VALUE_HEADS, HEAD_SIZE).transpose(1, 0, 2, 3)
    return tensor_data.astype(jnp.float32).reshape(rows_per_block, KEY_VALUE_HEADS, HEAD_SIZE).transpose(1, 0, 2)

def attend(queries, keys, values):
    sequence_length = queries.shape[0]
    rows_per_block = min(4096, sequence_length)
    score_scale = HEAD_SIZE ** (-0.5)
    outputs = []
    totals = []
    for step_index in range(sequence_length // rows_per_block):
        stop_at = (step_index + 1) * rows_per_block
        query_ids = jnp.arange(step_index * rows_per_block, stop_at)
        causal = jnp.arange(stop_at)[None, :] <= query_ids[:, None]
        query_part = split_heads(queries[step_index * rows_per_block:stop_at], rows_per_block, True)
        key_part = split_heads(keys[:stop_at], stop_at, False)
        value_part = split_heads(values[:stop_at], stop_at, False)

        def one_head(operands):
            query_head, key_head, value_head = operands
            scores = jnp.einsum('qgd,nd->gqn', query_head, key_head, precision=lax.Precision.HIGHEST) * score_scale
            scores = jnp.where(causal, scores, NEG)
            row_max = lax.optimization_barrier(jnp.max(scores, axis=-1))
            weights = jnp.where(causal, jnp.exp(scores - row_max[..., None]), 0.0)
            row_sum = lax.optimization_barrier(jnp.sum(weights, axis=-1))
            rounded = lax.optimization_barrier(weights.astype(jnp.bfloat16)).astype(jnp.float32)
            mixed = jnp.einsum('gqn,nd->qgd', rounded, value_head, precision=lax.Precision.HIGHEST) / row_sum.T[:, :, None]
            return (mixed.astype(jnp.bfloat16), row_max + jnp.log(row_sum))
        mixed, log_total = lax.map(one_head, (query_part, key_part, value_part))
        outputs.append(mixed.transpose(1, 0, 2, 3).reshape(rows_per_block, -1))
        totals.append(log_total)
    return (jnp.concatenate(outputs, axis=0), jnp.concatenate(totals, axis=2))

def attend_back(queries, keys, values, attended, dattended, log_total):
    sequence_length = queries.shape[0]
    rows_per_block = min(4096, sequence_length)
    score_scale = HEAD_SIZE ** (-0.5)
    dquery_list = []
    key_gradient_total = jnp.zeros((sequence_length, KEY_VALUE_HEADS * HEAD_SIZE), jnp.float32)
    value_gradient_total = jnp.zeros((sequence_length, KEY_VALUE_HEADS * HEAD_SIZE), jnp.float32)
    for step_index in range(sequence_length // rows_per_block):
        begin = step_index * rows_per_block
        stop_at = begin + rows_per_block
        query_ids = jnp.arange(begin, stop_at)
        causal = jnp.arange(stop_at)[None, :] <= query_ids[:, None]
        query_part = split_heads(queries[begin:stop_at], rows_per_block, True)
        key_part = split_heads(keys[:stop_at], stop_at, False)
        value_part = split_heads(values[:stop_at], stop_at, False)
        out_part = split_heads(attended[begin:stop_at], rows_per_block, True)
        grad_part = split_heads(dattended[begin:stop_at], rows_per_block, True)
        total_part = log_total[:, :, begin:stop_at]

        def one_head(operands):
            query_head, key_head, value_head, out_head, grad_head, total_head = operands
            scores = jnp.einsum('qgd,nd->gqn', query_head, key_head, precision=lax.Precision.HIGHEST) * score_scale
            scores = jnp.where(causal, scores, NEG)
            prob_rows = jnp.where(causal, jnp.exp(scores - total_head[..., None]), 0.0)
            rounded = lax.optimization_barrier(prob_rows.astype(jnp.bfloat16)).astype(jnp.float32)
            dvalue = jnp.einsum('gqn,qgd->nd', rounded, grad_head, precision=lax.Precision.HIGHEST)
            dprob = jnp.einsum('qgd,nd->gqn', grad_head, value_head, precision=lax.Precision.HIGHEST)
            delta_rows = lax.optimization_barrier(jnp.sum(grad_head * out_head, axis=-1)).T
            dscore = prob_rows * (dprob - delta_rows[..., None])
            dscore = lax.optimization_barrier(dscore.astype(jnp.bfloat16)).astype(jnp.float32)
            dquery = jnp.einsum('gqn,nd->qgd', dscore, key_head, precision=lax.Precision.HIGHEST) * score_scale
            dkey = jnp.einsum('gqn,qgd->nd', dscore, query_head, precision=lax.Precision.HIGHEST) * score_scale
            return (dquery, dkey, dvalue)
        dquery, dkey, dvalue = lax.map(one_head, (query_part, key_part, value_part, out_part, grad_part, total_part))
        dquery_list.append(dquery.transpose(1, 0, 2, 3).reshape(rows_per_block, -1))
        key_gradient_total = key_gradient_total.at[:stop_at].add(dkey.transpose(1, 0, 2).reshape(stop_at, -1))
        value_gradient_total = value_gradient_total.at[:stop_at].add(dvalue.transpose(1, 0, 2).reshape(stop_at, -1))
    return (jnp.concatenate(dquery_list, axis=0), key_gradient_total, value_gradient_total)

def reference(block_input, span_order, norm1_gain, w_query, key_weight, value_weight, qk_gain, w_out, norm2_gain, w_gate, w_up, w_down, out_grad):
    row_ids = jnp.arange(TOKENS, dtype=jnp.int32)
    where_at = (span_order[row_ids // TOK_DEV] * TOK_DEV + row_ids % TOK_DEV).astype(jnp.int32)
    span_owner = jnp.argsort(span_order).astype(jnp.int32)
    by_place = (span_owner[row_ids // TOK_DEV] * TOK_DEV + row_ids % TOK_DEV).astype(jnp.int32)
    gain_one = norm1_gain.astype(jnp.float32)
    gain_two = norm2_gain.astype(jnp.float32)
    in_flat = block_input.astype(jnp.float32)
    normed = rms_norm(in_flat, gain_one).astype(jnp.bfloat16)
    q_raw = jnp.dot(normed, w_query, preferred_element_type=jnp.float32)
    k_raw = jnp.dot(normed, key_weight, preferred_element_type=jnp.float32)
    v_raw = jnp.dot(normed, value_weight, preferred_element_type=jnp.float32)

    def query_map(raw_rows, gain_vec):
        return head_map(raw_rows, gain_vec, where_at)
    queries = query_map(q_raw, qk_gain[0]).astype(jnp.bfloat16)
    keys = query_map(k_raw, qk_gain[1]).astype(jnp.bfloat16)
    values = v_raw.astype(jnp.bfloat16)
    sorted_q = queries[by_place]
    sorted_k = keys[by_place]
    sorted_v = values[by_place]
    out_sorted, log_total = attend(sorted_q, sorted_k, sorted_v)
    attended = out_sorted[where_at]
    middle = in_flat + jnp.dot(attended, w_out, preferred_element_type=jnp.float32)
    normed2 = rms_norm(middle, gain_two).astype(jnp.bfloat16)
    gate_rows = jnp.dot(normed2, w_gate, preferred_element_type=jnp.float32)
    up_rows = jnp.dot(normed2, w_up, preferred_element_type=jnp.float32)
    hidden = (jax.nn.silu(gate_rows) * up_rows).astype(jnp.bfloat16)
    block_output = (middle + jnp.dot(hidden, w_down, preferred_element_type=jnp.float32)).astype(jnp.bfloat16)
    dhidden = jnp.dot(out_grad, w_down.T, preferred_element_type=jnp.float32)
    down_grad = jnp.dot(hidden.T, out_grad, preferred_element_type=jnp.float32)
    _, gate_back = jax.vjp(lambda gate_in, up_in: jax.nn.silu(gate_in) * up_in, gate_rows, up_rows)
    dgate, dup = gate_back(dhidden)
    dgate = dgate.astype(jnp.bfloat16)
    dup = dup.astype(jnp.bfloat16)
    dnormed2 = jnp.dot(dgate, w_gate.T, preferred_element_type=jnp.float32) + jnp.dot(dup, w_up.T, preferred_element_type=jnp.float32)
    gate_grad = jnp.dot(normed2.T, dgate, preferred_element_type=jnp.float32)
    up_grad = jnp.dot(normed2.T, dup, preferred_element_type=jnp.float32)
    _, norm2_back = jax.vjp(rms_norm, middle, gain_two)
    dmiddle_norm, norm2_grad = norm2_back(dnormed2)
    dmiddle = out_grad.astype(jnp.float32) + dmiddle_norm
    dmiddle_b = dmiddle.astype(jnp.bfloat16)
    out_proj_grad = jnp.dot(attended.T, dmiddle_b, preferred_element_type=jnp.float32)
    dattended = jnp.dot(dmiddle_b, w_out.T, preferred_element_type=jnp.float32).astype(jnp.bfloat16)
    dq_sorted, dk_sorted, dv_sorted = attend_back(sorted_q, sorted_k, sorted_v, out_sorted, dattended[by_place], log_total)
    dqueries = dq_sorted.astype(jnp.bfloat16)[where_at]
    dkeys = dk_sorted.astype(jnp.bfloat16)[where_at]
    dvalues = dv_sorted.astype(jnp.bfloat16)[where_at]
    _, query_back = jax.vjp(query_map, q_raw, qk_gain[0])
    dq_raw, qgain_grad = query_back(dqueries.astype(jnp.float32))
    _, key_back = jax.vjp(query_map, k_raw, qk_gain[1])
    dk_raw, kgain_grad = key_back(dkeys.astype(jnp.float32))
    dq_raw = dq_raw.astype(jnp.bfloat16)
    dk_raw = dk_raw.astype(jnp.bfloat16)
    dnormed = jnp.dot(dq_raw, w_query.T, preferred_element_type=jnp.float32)
    dnormed = dnormed + jnp.dot(dk_raw, key_weight.T, preferred_element_type=jnp.float32)
    dnormed = dnormed + jnp.dot(dvalues, value_weight.T, preferred_element_type=jnp.float32)
    query_grad = jnp.dot(normed.T, dq_raw, preferred_element_type=jnp.float32)
    key_grad = jnp.dot(normed.T, dk_raw, preferred_element_type=jnp.float32)
    value_grad = jnp.dot(normed.T, dvalues, preferred_element_type=jnp.float32)
    _, norm1_back = jax.vjp(rms_norm, in_flat, gain_one)
    dinput_norm, norm1_grad = norm1_back(dnormed)
    input_grad = (dmiddle + dinput_norm).astype(jnp.bfloat16)
    qk_gain_grad = jnp.stack([qgain_grad, kgain_grad])
    return (block_output, input_grad, norm1_grad, query_grad, key_grad, value_grad, qk_gain_grad, out_proj_grad, norm2_grad, gate_grad, up_grad, down_grad)
```

```python
import functools
import math

import jax
import jax.numpy as jnp
from jax import lax
from jax.experimental import pallas as pl
from jax.experimental.pallas import tpu as pltpu
from jax.sharding import PartitionSpec as P

EPS = 1e-05
THETA = 1000000.0
NEG = -1e30
CORES = 2
INNER = 2
MESH = pl.DeviceIdType.MESH
F32 = jnp.float32
BF16 = jnp.bfloat16


def here():
    head = lax.axis_index("head")
    blk = lax.axis_index("blk")
    return head // CORES, head % CORES, blk // INNER, blk % INNER


def device(y, c, z, x):
    return (y * CORES + c, z * INNER + x)


def rank(y, c, x):
    return (y * CORES + c) * INNER + x


def plane_peers(place):
    y, c, z, x = place
    peers = []
    for bits in range(1, 8):
        py = 1 - y if bits & 4 else y
        pc = 1 - c if bits & 2 else c
        px = 1 - x if bits & 1 else x
        peers.append((device(py, pc, z, px), rank(py, pc, px), (py * CORES + pc, px)))
    return peers


def line_peers(place):
    y, c, z, x = place
    outer = lax.axis_size("blk") // INNER
    forth = [lax.rem(z + k, outer) for k in range(1, outer)]
    back = [lax.rem(z + outer - k, outer) for k in range(1, outer)]
    return [(device(y, c, f, x), f, b) for f, b in zip(forth, back)]


def greet(devices):
    barrier = pltpu.get_barrier_semaphore()
    for dev in devices:
        pl.semaphore_signal(barrier, inc=1, device_id=dev, device_id_type=MESH)
    pl.semaphore_wait(barrier, len(devices))


class Mail:
    def __init__(self, sems):
        self.sends, self.recvs = sems
        self.used = 0
        self.open = []

    def take(self, count):
        first = self.used
        self.used += count
        return first

    def send(self, slot, src, dst, dev):
        copy = pltpu.make_async_remote_copy(
            src_ref=src,
            dst_ref=dst,
            send_sem=self.sends.at[slot],
            recv_sem=self.recvs.at[slot],
            device_id=dev,
            device_id_type=MESH,
        )
        copy.start()
        self.open.append(copy)

    def arrive(self, slot, dst, dev):
        pltpu.make_async_remote_copy(
            src_ref=dst,
            dst_ref=dst,
            send_sem=self.sends.at[slot],
            recv_sem=self.recvs.at[slot],
            device_id=dev,
            device_id_type=MESH,
        ).wait_recv()

    def close(self):
        for copy in self.open:
            copy.wait_send()


def near(place):
    y, c, z, x = place
    return device(y, 1 - c, z, x), device(y, c, z, 1 - x), device(1 - y, c, z, x)


class PlaneGather:
    COPIES = 11

    def __init__(self, mail, place, src, out):
        self.mail, self.place, self.src, self.out = mail, place, src, out
        self.base = mail.take(self.COPIES)
        half = src.shape[0] // 2
        self.top, self.bot = pl.ds(0, half), pl.ds(half, half)

    def begin(self):
        y, c, z, x = self.place
        pair, xn, yn = near(self.place)
        me = rank(y, c, x)
        send, base, src, out = self.mail.send, self.base, self.src, self.out
        top, bot = self.top, self.bot
        send(base + 0, src.at[top], out.at[me, top], xn)
        send(base + 1, src.at[bot], out.at[me, bot], yn)
        send(base + 2, src.at[bot], out.at[me, bot], xn)
        send(base + 3, src.at[top], out.at[me, top], yn)
        send(base + 4, src, out.at[me], pair)
        out[me] = src[...]

    def middle(self):
        y, c, z, x = self.place
        pair, xn, yn = near(self.place)
        xr, yr = rank(y, c, 1 - x), rank(1 - y, c, x)
        send, arrive, base, out = self.mail.send, self.mail.arrive, self.base, self.out
        top, bot = self.top, self.bot
        arrive(base + 0, out.at[xr, top], xn)
        send(base + 5, out.at[xr, top], out.at[xr, top], yn)
        arrive(base + 1, out.at[yr, bot], yn)
        send(base + 6, out.at[yr, bot], out.at[yr, bot], xn)
        arrive(base + 2, out.at[xr, bot], xn)
        send(base + 7, out.at[xr], out.at[xr], pair)
        arrive(base + 3, out.at[yr, top], yn)
        send(base + 8, out.at[yr], out.at[yr], pair)

    def end(self):
        y, c, z, x = self.place
        pair, xn, yn = near(self.place)
        dr = rank(1 - y, c, 1 - x)
        send, arrive, base, out = self.mail.send, self.mail.arrive, self.base, self.out
        top, bot = self.top, self.bot
        arrive(base + 5, out.at[dr, top], yn)
        send(base + 9, out.at[dr, top], out.at[dr, top], pair)
        arrive(base + 6, out.at[dr, bot], xn)
        send(base + 10, out.at[dr, bot], out.at[dr, bot], pair)
        arrive(base + 4, out.at[rank(y, 1 - c, x)], pair)
        arrive(base + 7, out.at[rank(y, 1 - c, 1 - x)], pair)
        arrive(base + 8, out.at[rank(1 - y, 1 - c, x)], pair)
        far = rank(1 - y, 1 - c, 1 - x)
        arrive(base + 9, out.at[far, top], pair)
        arrive(base + 10, out.at[far, bot], pair)


class PlaneScatter:
    COPIES = 10

    def __init__(self, mail, place, parts, out, bufs):
        self.mail, self.place, self.parts, self.out = mail, place, parts, out
        self.first, self.held, self.via_x, self.via_y, self.last = bufs
        self.base = mail.take(self.COPIES)
        half = out.shape[0] // 2
        self.top, self.bot = pl.ds(0, half), pl.ds(half, half)

    @staticmethod
    def scratch(rows, cols):
        half = rows // 2
        return [
            pltpu.VMEM((2, 2, rows, cols), BF16),
            pltpu.VMEM((2, 2, rows, cols), BF16),
            pltpu.VMEM((2, half, cols), BF16),
            pltpu.VMEM((2, half, cols), BF16),
            pltpu.VMEM((4, half, cols), BF16),
        ]

    def begin(self):
        y, c, z, x = self.place
        pair, xn, yn = near(self.place)
        for slot, (py, px) in enumerate(((1 - y, 1 - x), (y, 1 - x), (1 - y, x), (y, x))):
            self.mail.send(
                self.base + slot,
                self.parts.at[rank(py, 1 - c, px)],
                self.first.at[py, px],
                pair,
            )

    def joined(self, slot, py, px):
        y, c, z, x = self.place
        pair, xn, yn = near(self.place)
        self.mail.arrive(self.base + slot, self.first.at[py, px], pair)
        return self.parts[rank(py, c, px)].astype(F32) + self.first[py, px].astype(F32)

    def middle(self):
        y, c, z, x = self.place
        pair, xn, yn = near(self.place)
        send, base, held = self.mail.send, self.base, self.held
        top, bot = self.top, self.bot
        held[1 - y, 1 - x] = self.joined(0, 1 - y, 1 - x).astype(BF16)
        send(base + 4, held.at[1 - y, 1 - x, top], self.via_x.at[1 - y], xn)
        send(base + 5, held.at[1 - y, 1 - x, bot], self.via_y.at[1 - x], yn)
        held[y, 1 - x] = self.joined(1, y, 1 - x).astype(BF16)
        send(base + 6, held.at[y, 1 - x, top], self.via_x.at[y], xn)
        held[1 - y, x] = self.joined(2, 1 - y, x).astype(BF16)
        send(base + 7, held.at[1 - y, x, bot], self.via_y.at[x], yn)
        self.out[...] = self.joined(3, y, x)

    def end(self):
        y, c, z, x = self.place
        pair, xn, yn = near(self.place)
        send, arrive, base, held = self.mail.send, self.mail.arrive, self.base, self.held
        top, bot, last, out = self.top, self.bot, self.last, self.out
        arrive(base + 4, self.via_x.at[1 - y], xn)
        last[0] = (held[1 - y, x, top].astype(F32) + self.via_x[1 - y].astype(F32)).astype(BF16)
        send(base + 8, last.at[0], last.at[2], yn)
        arrive(base + 5, self.via_y.at[1 - x], yn)
        last[1] = (held[y, 1 - x, bot].astype(F32) + self.via_y[1 - x].astype(F32)).astype(BF16)
        send(base + 9, last.at[1], last.at[3], xn)
        arrive(base + 6, self.via_x.at[y], xn)
        out[top] = out[top] + self.via_x[y].astype(F32)
        arrive(base + 7, self.via_y.at[x], yn)
        out[bot] = out[bot] + self.via_y[x].astype(F32)
        arrive(base + 8, last.at[2], yn)
        out[top] = out[top] + last[2].astype(F32)
        arrive(base + 9, last.at[3], xn)
        out[bot] = out[bot] + last[3].astype(F32)


class PlaneSwap:
    COPIES = 7

    def __init__(self, mail, place, src, out):
        self.mail, self.place, self.src, self.out = mail, place, src, out
        self.base = mail.take(self.COPIES)

    def begin(self):
        y, c, z, x = self.place
        me = rank(y, c, x)
        for slot, (dev, other, _) in enumerate(plane_peers(self.place)):
            self.mail.send(self.base + slot, self.src.at[other], self.out.at[me], dev)
        self.out[me] = self.src[me]

    def end(self):
        for slot, (dev, other, _) in enumerate(plane_peers(self.place)):
            self.mail.arrive(self.base + slot, self.out.at[other], dev)


def call(body, name, ident, outs, args, copies, scratch=()):
    spec = pl.BlockSpec(memory_space=pltpu.VMEM)
    return pl.pallas_call(
        body,
        name=name,
        out_shape=tuple(jax.ShapeDtypeStruct(shape, dtype) for shape, dtype in outs),
        in_specs=[spec] * len(args),
        out_specs=tuple([spec] * len(outs)),
        scratch_shapes=[
            pltpu.SemaphoreType.DMA((copies,)),
            pltpu.SemaphoreType.DMA((copies,)),
            *scratch,
        ],
        compiler_params=pltpu.CompilerParams(
            collective_id=ident, has_side_effects=True, vmem_limit_bytes=60 * 1024 * 1024
        ),
    )(*args)


def start_kernel(x_ref, w_ref, g_ref, gu_ref, xp_ref, wq_ref, gain_ref, gus_ref, ss, rs):
    place = y, c, z, x = here()
    me = rank(y, c, x)
    head = y * CORES + c
    mail = Mail((ss, rs))
    peers, line = plane_peers(place), line_peers(place)
    greet([p[0] for p in peers] + [p[0] for p in line])
    w_base, g_base = mail.take(7), mail.take(7)
    zw_base, zg_base = mail.take(len(line)), mail.take(len(line))
    for slot, (dev, other, _) in enumerate(peers):
        mail.send(g_base + slot, g_ref, gain_ref.at[z, me], dev)
        mail.send(w_base + slot, w_ref.at[other], wq_ref.at[head, z, x], dev)
    gain_ref[z, me] = g_ref[...]
    wq_ref[head, z, x] = w_ref[me]
    rows = PlaneGather(mail, place, x_ref, xp_ref)
    swap = PlaneSwap(mail, place, gu_ref, gus_ref)
    rows.begin()
    for slot, (dev, other, (oh, ox)) in enumerate(peers):
        mail.arrive(g_base + slot, gain_ref.at[z, other], dev)
        mail.arrive(w_base + slot, wq_ref.at[oh, z, ox], dev)
    for slot, (dev, _, _) in enumerate(line):
        mail.send(zg_base + slot, gain_ref.at[z], gain_ref.at[z], dev)
        mail.send(zw_base + slot, wq_ref.at[:, z], wq_ref.at[:, z], dev)
    rows.middle()
    swap.begin()
    rows.end()
    for slot, (dev, _, back) in enumerate(line):
        mail.arrive(zg_base + slot, gain_ref.at[back], dev)
        mail.arrive(zw_base + slot, wq_ref.at[:, back], dev)
    swap.end()
    mail.close()


def line_kernel(kv_ref, og_ref, kvs_ref, ogs_ref, ss, rs):
    place = y, c, z, x = here()
    mail = Mail((ss, rs))
    line = line_peers(place)
    greet([p[0] for p in line] + list(near(place)))
    base = mail.take(len(line))
    for slot, (dev, _, _) in enumerate(line):
        mail.send(base + slot, kv_ref, kvs_ref.at[z], dev)
    rows = PlaneGather(mail, place, og_ref, ogs_ref)
    rows.begin()
    kvs_ref[z] = kv_ref[...]
    rows.middle()
    rows.end()
    for slot, (dev, _, back) in enumerate(line):
        mail.arrive(base + slot, kvs_ref.at[back], dev)
    mail.close()


def gather_kernel(src_ref, out_ref, ss, rs):
    place = here()
    mail = Mail((ss, rs))
    greet(list(near(place)))
    rows = PlaneGather(mail, place, src_ref, out_ref)
    rows.begin()
    rows.middle()
    rows.end()
    mail.close()


def scatter_kernel(parts_ref, out_ref, ss, rs, *bufs):
    place = here()
    mail = Mail((ss, rs))
    greet(list(near(place)))
    rows = PlaneScatter(mail, place, parts_ref, out_ref, bufs)
    rows.begin()
    rows.middle()
    rows.end()
    mail.close()


def back_kernel(dkv_ref, parts_ref, kv_ref, out_ref, ss, rs, got, *bufs):
    place = y, c, z, x = here()
    mail = Mail((ss, rs))
    line = line_peers(place)
    greet([p[0] for p in line] + list(near(place)))
    base = mail.take(len(line))
    for slot, (dev, forth, _) in enumerate(line):
        mail.send(base + slot, dkv_ref.at[forth], got.at[slot], dev)
    rows = PlaneScatter(mail, place, parts_ref, out_ref, bufs)
    rows.begin()
    rows.middle()
    rows.end()
    total = dkv_ref[z].astype(F32)
    for slot, (dev, _, _) in enumerate(line):
        mail.arrive(base + slot, got.at[slot], dev)
        total = total + got[slot].astype(F32)
    kv_ref[...] = total
    mail.close()


def last_kernel(parts_ref, w_ref, gu_ref, out_ref, ws_ref, gus_ref, ss, rs, got, held, *bufs):
    place = y, c, z, x = here()
    me = rank(y, c, x)
    mail = Mail((ss, rs))
    peers, line = plane_peers(place), line_peers(place)
    greet([p[0] for p in line] + [p[0] for p in peers])
    base = mail.take(len(line))
    w_base = mail.take(7)
    for slot, (dev, forth, _) in enumerate(line):
        mail.send(base + slot, w_ref.at[:, forth], got.at[slot], dev)
    rows = PlaneScatter(mail, place, parts_ref, out_ref, bufs)
    swap = PlaneSwap(mail, place, gu_ref, gus_ref)
    rows.begin()
    rows.middle()
    swap.begin()
    rows.end()
    total = w_ref[:, z].astype(F32)
    for slot, (dev, _, _) in enumerate(line):
        mail.arrive(base + slot, got.at[slot], dev)
        total = total + got[slot].astype(F32)
    held[...] = total.reshape(held.shape)
    for slot, (dev, other, _) in enumerate(peers):
        mail.send(w_base + slot, held.at[other], ws_ref.at[me], dev)
    ws_ref[me] = held[me]
    for slot, (dev, other, _) in enumerate(peers):
        mail.arrive(w_base + slot, ws_ref.at[other], dev)
    swap.end()
    mail.close()


def small_kernel(v_ref, out_ref, ss, rs, got, held):
    place = y, c, z, x = here()
    me = rank(y, c, x)
    mail = Mail((ss, rs))
    peers, line = plane_peers(place), line_peers(place)
    greet([p[0] for p in line] + [p[0] for p in peers])
    p_base, z_base = mail.take(7), mail.take(len(line))
    for slot, (dev, other, _) in enumerate(peers):
        mail.send(p_base + slot, v_ref, got.at[me], dev)
    got[me] = v_ref[...]
    for slot, (dev, other, _) in enumerate(peers):
        mail.arrive(p_base + slot, got.at[other], dev)
    held[z] = jnp.sum(got[...], axis=0)
    for slot, (dev, _, _) in enumerate(line):
        mail.send(z_base + slot, held.at[z], held.at[z], dev)
    for slot, (dev, _, back) in enumerate(line):
        mail.arrive(z_base + slot, held.at[back], dev)
    out_ref[...] = jnp.sum(held[...], axis=0)
    mail.close()


def rms_norm(values, gain_vec):
    inverse = lax.rsqrt(jnp.mean(values * values, axis=-1, keepdims=True) + EPS)
    return values * inverse * gain_vec


def rotate(field_in, where_at):
    half_size = field_in.shape[-1] // 2
    frequency = jnp.exp(
        jnp.arange(half_size, dtype=F32) * F32(-2.0 * math.log(THETA) / field_in.shape[-1])
    )
    angles = where_at.astype(F32)[:, None] * frequency[None, :]
    cosine = jnp.cos(angles)[:, None, :]
    sine_part = jnp.sin(angles)[:, None, :]
    first_half = field_in[..., :half_size]
    second_half = field_in[..., half_size:]
    return jnp.concatenate(
        [
            first_half * cosine - second_half * sine_part,
            second_half * cosine + first_half * sine_part,
        ],
        axis=-1,
    )


def head_map(raw_rows, gain_vec, where_at):
    row_count = raw_rows.shape[0]
    shaped = raw_rows.reshape(row_count, -1, gain_vec.shape[0])
    return rotate(rms_norm(shaped, gain_vec), where_at).reshape(row_count, -1)


def shifts(outer, step):
    return [
        (z * INNER + x, ((z + step) % outer) * INNER + x)
        for z in range(outer)
        for x in range(INNER)
    ]


def line_gather(piece, axis, full_shape, z, outer):
    full = jnp.zeros(full_shape, piece.dtype)
    full = lax.dynamic_update_slice_in_dim(full, jnp.expand_dims(piece, axis), z, axis)
    for step in range(1, outer):
        got = lax.ppermute(piece, "blk", shifts(outer, step))
        full = lax.dynamic_update_slice_in_dim(
            full, jnp.expand_dims(got, axis), (z + outer - step) % outer, axis
        )
    return full


def line_scatter(parts, axis, z, outer):
    total = lax.dynamic_index_in_dim(parts, z, axis, keepdims=False).astype(F32)
    for step in range(1, outer):
        piece = lax.dynamic_index_in_dim(parts, (z + step) % outer, axis, keepdims=False)
        total = total + lax.ppermute(piece.astype(BF16), "blk", shifts(outer, step)).astype(F32)
    return total


def dot(a, b):
    return jnp.dot(a, b, preferred_element_type=F32)


def local(
    block_input,
    span_order,
    norm1_gain,
    w_query,
    key_weight,
    value_weight,
    qk_gain,
    w_out,
    norm2_gain,
    w_gate,
    w_up,
    w_down,
    out_grad,
):
    heads = lax.axis_size("head")
    blocks = lax.axis_size("blk")
    outer = blocks // INNER
    plane = heads * INNER
    z = lax.axis_index("blk") // INNER
    x_at = lax.axis_index("blk") % INNER
    rows, width = block_input.shape
    head_size = qk_gain.shape[1]
    w_rows = w_query.shape[0]
    f_rows = w_down.shape[0]
    q_cols = w_query.shape[1] // plane
    k_cols = key_weight.shape[1] // plane
    share = q_cols // k_cols
    a_cols = q_cols + 2 * k_cols
    ff = f_rows * outer
    tokens = plane * rows
    score_scale = float(head_size) ** (-0.5)

    by_place = span_order.reshape(heads, outer, INNER)
    own_spans = lax.dynamic_index_in_dim(by_place, z, 1, keepdims=False).reshape(plane)
    all_spans = by_place.transpose(1, 0, 2).reshape(outer * plane)
    inside = jnp.arange(rows, dtype=jnp.int32)
    tok_where = (own_spans[:, None] * rows + inside[None, :]).reshape(tokens)
    key_where = (all_spans[:, None] * rows + inside[None, :]).reshape(outer * tokens)

    w8 = jnp.concatenate(
        [
            w_query.reshape(w_rows, plane, q_cols),
            key_weight.reshape(w_rows, plane, k_cols),
            value_weight.reshape(w_rows, plane, k_cols),
        ],
        axis=-1,
    ).transpose(1, 0, 2)

    def cut(weight):
        shaped = weight.reshape(w_rows, heads, outer, INNER, f_rows)
        return shaped.transpose(1, 3, 0, 2, 4).reshape(plane, w_rows, ff)

    gu8 = jnp.concatenate([cut(w_gate), cut(w_up)], axis=-1)
    gains = jnp.zeros((16, 128), BF16)
    gains = gains.at[0, :w_rows].set(norm1_gain).at[1, :w_rows].set(norm2_gain)
    down_full = line_gather(w_down, 0, (outer, f_rows, width), z, outer).reshape(ff, width)
    out_all = lax.all_gather(w_out, "blk", axis=0, tiled=True)

    n_line = outer - 1
    x_all, wqkv, gains_all, gu_piece = call(
        start_kernel,
        "start",
        1,
        [
            ((plane, rows, width), BF16),
            ((heads, outer, INNER, w_rows, a_cols), BF16),
            ((outer, plane, 16, 128), BF16),
            ((plane, w_rows, 2 * ff), BF16),
        ],
        (block_input, w8, gains, gu8),
        14 + 2 * n_line + PlaneGather.COPIES + PlaneSwap.COPIES,
    )
    wqkv = wqkv.reshape(width, a_cols)
    gains_all = (
        gains_all[:, :, :2, :w_rows]
        .reshape(outer, heads, INNER, 2, w_rows)
        .transpose(3, 1, 0, 2, 4)
        .reshape(2, width)
        .astype(F32)
    )
    gain_one, gain_two = gains_all[0], gains_all[1]
    gu_full = line_gather(
        gu_piece.reshape(heads, INNER * w_rows, 2 * ff),
        1,
        (heads, outer, INNER * w_rows, 2 * ff),
        z,
        outer,
    ).reshape(width, 2 * ff)

    normed = rms_norm(x_all.reshape(tokens, width).astype(F32), gain_one).astype(BF16)
    qkv_raw = dot(normed, wqkv)
    q_raw = qkv_raw[:, :q_cols]
    k_raw = qkv_raw[:, q_cols : q_cols + k_cols]
    v_raw = qkv_raw[:, q_cols + k_cols :]

    def query_map(raw_rows, gain_vec):
        return head_map(raw_rows, gain_vec, tok_where)

    queries = query_map(q_raw, qk_gain[0]).astype(BF16)
    keys = query_map(k_raw, qk_gain[1]).astype(BF16)
    kv = jnp.concatenate([keys, v_raw.astype(BF16)], axis=-1)
    kv_all, og_all = call(
        line_kernel,
        "line",
        2,
        [((outer, tokens, 2 * k_cols), BF16), ((plane, rows, width), BF16)],
        (kv, out_grad),
        n_line + PlaneGather.COPIES,
    )
    og_all = og_all.reshape(tokens, width)
    k_all = kv_all[:, :, :k_cols].reshape(outer * tokens, k_cols)
    v_all = kv_all[:, :, k_cols:].reshape(outer * tokens, k_cols)
    q_three = queries.reshape(tokens, share, head_size)
    causal = key_where[None, :] <= tok_where[:, None]
    scores = jnp.einsum("qgd,nd->gqn", q_three, k_all, preferred_element_type=F32) * score_scale
    scores = jnp.where(causal, scores, NEG)
    row_max = jnp.max(scores, axis=-1)
    weights = jnp.where(causal, jnp.exp(scores - row_max[..., None]), 0.0)
    row_sum = jnp.sum(weights, axis=-1)
    mixed = jnp.einsum("gqn,nd->qgd", weights.astype(BF16), v_all, preferred_element_type=F32)
    attended3 = (mixed / row_sum.T[..., None]).astype(BF16)
    log_total = row_max + jnp.log(row_sum)
    attended = attended3.reshape(tokens, q_cols)

    out_mine = lax.dynamic_slice_in_dim(out_all, x_at * q_cols, q_cols, 0)

    def scatter(parts, name, ident):
        return call(
            scatter_kernel,
            name,
            ident,
            [((rows, width), F32)],
            (parts.astype(BF16).reshape(plane, rows, width),),
            PlaneScatter.COPIES,
            PlaneScatter.scratch(rows, width),
        )[0]

    def gather(block, name, ident):
        return call(
            gather_kernel,
            name,
            ident,
            [((plane, rows, width), BF16)],
            (block,),
            PlaneGather.COPIES,
        )[0].reshape(tokens, width)

    in_flat = block_input.astype(F32)
    middle = in_flat + scatter(dot(attended, out_mine), "mix", 3)
    normed2_own = rms_norm(middle, gain_two).astype(BF16)
    normed2 = gather(normed2_own, "widen", 4)

    gu_rows = dot(normed2, gu_full)
    gate_rows, up_rows = gu_rows[:, :ff], gu_rows[:, ff:]
    hidden, gate_back = jax.vjp(lambda a, b: jax.nn.silu(a) * b, gate_rows, up_rows)
    hidden = hidden.astype(BF16)
    dhidden = dot(og_all, down_full.T)
    dgate, dup = gate_back(dhidden)
    dgu = jnp.concatenate([dgate.astype(BF16), dup.astype(BF16)], axis=-1)
    dnormed2 = scatter(dot(dgu, gu_full.T), "narrow", 5)
    out_parts = dot(hidden, down_full).astype(BF16).reshape(plane, rows, width)
    gu_grad = dot(normed2.T, dgu)
    down_grad = dot(hidden.T, og_all)
    down_grad = line_scatter(down_grad.reshape(outer, f_rows, width), 0, z, outer)
    gu_grad = line_scatter(
        gu_grad.reshape(heads, outer, INNER * w_rows, 2 * ff), 1, z, outer
    ).reshape(plane, w_rows, 2 * ff)

    _, norm2_back = jax.vjp(rms_norm, middle, gain_two)
    dmiddle_norm, norm2_grad = norm2_back(dnormed2)
    dmiddle = out_grad.astype(F32) + dmiddle_norm
    dmid_all = gather(dmiddle.astype(BF16), "spread", 6)

    out_proj = dot(attended.T, dmid_all)
    out_proj = jnp.where(
        (jnp.arange(INNER) == x_at)[:, None, None], out_proj[None], 0.0
    ).reshape(INNER * q_cols, width)
    out_proj_grad = lax.psum_scatter(out_proj, "blk", scatter_dimension=0, tiled=True)
    dattended = dot(dmid_all, out_mine.T).astype(BF16)
    grad_three = dattended.reshape(tokens, share, head_size)
    delta = jnp.sum(grad_three.astype(F32) * attended3.astype(F32), axis=-1).T
    prob = jnp.where(causal, jnp.exp(scores - log_total[..., None]), 0.0)
    dvalues = jnp.einsum("gqn,qgd->nd", prob.astype(BF16), grad_three, preferred_element_type=F32)
    dprob = jnp.einsum("qgd,nd->gqn", grad_three, v_all, preferred_element_type=F32)
    dscore = (prob * (dprob - delta[..., None])).astype(BF16)
    dqueries = jnp.einsum("gqn,nd->qgd", dscore, k_all, preferred_element_type=F32) * score_scale
    dkeys = jnp.einsum("gqn,qgd->nd", dscore, q_three, preferred_element_type=F32) * score_scale
    dkv = jnp.concatenate([dkeys, dvalues], axis=-1).astype(BF16)
    dkv_own, ffn_out = call(
        back_kernel,
        "back",
        7,
        [((tokens, 2 * k_cols), F32), ((rows, width), F32)],
        (dkv.reshape(outer, tokens, 2 * k_cols), out_parts),
        n_line + PlaneScatter.COPIES,
        [pltpu.VMEM((n_line, tokens, 2 * k_cols), BF16)] + PlaneScatter.scratch(rows, width),
    )
    block_output = (middle + ffn_out).astype(BF16)
    dkv_own = dkv_own.astype(BF16)
    dqueries = dqueries.reshape(tokens, q_cols).astype(BF16)
    _, query_back = jax.vjp(query_map, q_raw, qk_gain[0])
    dq_raw, qgain_grad = query_back(dqueries.astype(F32))
    _, key_back = jax.vjp(query_map, k_raw, qk_gain[1])
    dk_raw, kgain_grad = key_back(dkv_own[:, :k_cols].astype(F32))
    dqkv = jnp.concatenate(
        [dq_raw.astype(BF16), dk_raw.astype(BF16), dkv_own[:, k_cols:]], axis=-1
    )
    wqkv_grad = dot(normed.T, dqkv).astype(BF16)
    dnormed, wqkv_own, gu_own = call(
        last_kernel,
        "last",
        8,
        [
            ((rows, width), F32),
            ((plane, w_rows, a_cols), F32),
            ((plane, w_rows, 2 * ff), BF16),
        ],
        (
            dot(dqkv, wqkv.T).astype(BF16).reshape(plane, rows, width),
            wqkv_grad.reshape(heads, outer, INNER, w_rows, a_cols),
            gu_grad.astype(BF16),
        ),
        n_line + 7 + PlaneScatter.COPIES + PlaneSwap.COPIES,
        [
            pltpu.VMEM((n_line, heads, INNER, w_rows, a_cols), BF16),
            pltpu.VMEM((plane, w_rows, a_cols), F32),
        ]
        + PlaneScatter.scratch(rows, width),
    )
    _, norm1_back = jax.vjp(rms_norm, in_flat, gain_one)
    dinput_norm, norm1_grad = norm1_back(dnormed)
    input_grad = (dmiddle + dinput_norm).astype(BF16)

    small = jnp.concatenate([norm1_grad, norm2_grad, qgain_grad, kgain_grad])
    small_rows = -(-small.shape[0] // 1024) * 8
    small = jnp.pad(small, (0, small_rows * 128 - small.shape[0])).reshape(small_rows, 128)
    summed = call(
        small_kernel,
        "small",
        9,
        [((small_rows, 128), F32)],
        (small,),
        7 + n_line,
        [pltpu.VMEM((plane, small_rows, 128), F32), pltpu.VMEM((outer, small_rows, 128), F32)],
    )[0].reshape(-1)
    own = (lax.axis_index("head") * blocks + lax.axis_index("blk")) * w_rows
    norm1_out = lax.dynamic_slice_in_dim(summed, own, w_rows)
    norm2_out = lax.dynamic_slice_in_dim(summed, width + own, w_rows)
    qk_gain_grad = summed[2 * width : 2 * width + 2 * head_size].reshape(2, head_size)

    def columns(blocks_in):
        return blocks_in.transpose(1, 0, 2).reshape(w_rows, -1)

    query_grad = columns(wqkv_own[:, :, :q_cols])
    key_grad = columns(wqkv_own[:, :, q_cols : q_cols + k_cols])
    value_grad = columns(wqkv_own[:, :, q_cols + k_cols :])

    def uncut(blocks_in):
        shaped = blocks_in.astype(F32).reshape(heads, INNER, w_rows, outer, f_rows)
        return shaped.transpose(2, 0, 3, 1, 4).reshape(w_rows, -1)

    gate_grad = uncut(gu_own[:, :, :ff])
    up_grad = uncut(gu_own[:, :, ff:])
    return (
        block_output,
        input_grad,
        norm1_out,
        query_grad,
        key_grad,
        value_grad,
        qk_gain_grad,
        out_proj_grad,
        norm2_out,
        gate_grad,
        up_grad,
        down_grad,
    )


def solution(mesh):
    split = P(("head", "blk"), None)
    line = P(("head", "blk"))
    in_specs = (split, P(), line, split, split, split, P(), split, line, split, split, split, split)
    out_specs = (split, split, line, split, split, split, P(), split, line, split, split, split)
    return jax.shard_map(local, mesh=mesh, in_specs=in_specs, out_specs=out_specs, check_vma=False)
```

```python
import functools
import math

import jax
import jax.numpy as jnp
from jax import lax
from jax.experimental import pallas as pl
from jax.experimental.pallas import tpu as pltpu
from jax.sharding import PartitionSpec as P

EPS = 1e-05
THETA = 1000000.0
CORES = 2
INNER = 2
MESH = pl.DeviceIdType.MESH
F32 = jnp.float32
BF16 = jnp.bfloat16


def here():
    head = lax.axis_index("head")
    blk = lax.axis_index("blk")
    return head // CORES, head % CORES, blk // INNER, blk % INNER


def device(y, c, z, x):
    return (y * CORES + c, z * INNER + x)


def rank(y, c, x):
    return (y * CORES + c) * INNER + x


def plane_peers(place):
    y, c, z, x = place
    peers = []
    for bits in range(1, 8):
        py = 1 - y if bits & 4 else y
        pc = 1 - c if bits & 2 else c
        px = 1 - x if bits & 1 else x
        peers.append((device(py, pc, z, px), rank(py, pc, px), (py * CORES + pc, px)))
    return peers


def line_peers(place):
    y, c, z, x = place
    outer = lax.axis_size("blk") // INNER
    forth = [lax.rem(z + k, outer) for k in range(1, outer)]
    back = [lax.rem(z + outer - k, outer) for k in range(1, outer)]
    return [(device(y, c, f, x), f, b) for f, b in zip(forth, back)]


def greet(devices):
    barrier = pltpu.get_barrier_semaphore()
    for dev in devices:
        pl.semaphore_signal(barrier, inc=1, device_id=dev, device_id_type=MESH)
    pl.semaphore_wait(barrier, len(devices))


class Mail:
    def __init__(self, sems):
        self.sends, self.recvs = sems
        self.used = 0
        self.open = []

    def take(self, count):
        first = self.used
        self.used += count
        return first

    def copy(self, slot, src, dst, dev, landing=None):
        return pltpu.make_async_remote_copy(
            src_ref=src,
            dst_ref=dst,
            send_sem=self.sends.at[slot],
            recv_sem=self.recvs.at[slot if landing is None else landing],
            device_id=dev,
            device_id_type=MESH,
        )

    def send(self, slot, src, dst, dev, landing=None):
        copy = self.copy(slot, src, dst, dev, landing)
        copy.start()
        self.open.append(copy)

    def arrive(self, slot, dst, dev):
        self.copy(slot, dst, dst, dev).wait_recv()

    def close(self):
        for copy in self.open:
            copy.wait_send()


def near(place):
    y, c, z, x = place
    return device(y, 1 - c, z, x), device(y, c, z, 1 - x), device(1 - y, c, z, x)


class PlaneGather:
    COPIES = 11

    def __init__(self, mail, place, src, out):
        self.mail, self.place, self.src, self.out = mail, place, src, out
        self.base = mail.take(self.COPIES)
        half = src.shape[0] // 2
        self.top, self.bot = pl.ds(0, half), pl.ds(half, half)

    def begin(self):
        y, c, z, x = self.place
        pair, xn, yn = near(self.place)
        me = rank(y, c, x)
        send, base, src, out = self.mail.send, self.base, self.src, self.out
        top, bot = self.top, self.bot
        send(base + 0, src.at[top], out.at[me, top], xn)
        send(base + 1, src.at[bot], out.at[me, bot], yn)
        send(base + 2, src.at[bot], out.at[me, bot], xn)
        send(base + 3, src.at[top], out.at[me, top], yn)
        send(base + 4, src, out.at[me], pair)
        out[me] = src[...]

    def middle(self):
        y, c, z, x = self.place
        pair, xn, yn = near(self.place)
        xr, yr = rank(y, c, 1 - x), rank(1 - y, c, x)
        send, arrive, base, out = self.mail.send, self.mail.arrive, self.base, self.out
        top, bot = self.top, self.bot
        arrive(base + 0, out.at[xr, top], xn)
        send(base + 5, out.at[xr, top], out.at[xr, top], yn)
        arrive(base + 1, out.at[yr, bot], yn)
        send(base + 6, out.at[yr, bot], out.at[yr, bot], xn)
        arrive(base + 2, out.at[xr, bot], xn)
        send(base + 7, out.at[xr], out.at[xr], pair)
        arrive(base + 3, out.at[yr, top], yn)
        send(base + 8, out.at[yr], out.at[yr], pair)

    def end(self):
        y, c, z, x = self.place
        pair, xn, yn = near(self.place)
        dr = rank(1 - y, c, 1 - x)
        send, arrive, base, out = self.mail.send, self.mail.arrive, self.base, self.out
        top, bot = self.top, self.bot
        arrive(base + 5, out.at[dr, top], yn)
        send(base + 9, out.at[dr, top], out.at[dr, top], pair)
        arrive(base + 6, out.at[dr, bot], xn)
        send(base + 10, out.at[dr, bot], out.at[dr, bot], pair)
        arrive(base + 4, out.at[rank(y, 1 - c, x)], pair)
        arrive(base + 7, out.at[rank(y, 1 - c, 1 - x)], pair)
        arrive(base + 8, out.at[rank(1 - y, 1 - c, x)], pair)
        far = rank(1 - y, 1 - c, 1 - x)
        arrive(base + 9, out.at[far, top], pair)
        arrive(base + 10, out.at[far, bot], pair)


class PlaneScatter:
    COPIES = 10

    def __init__(self, mail, place, parts, out, bufs):
        self.mail, self.place, self.parts, self.out = mail, place, parts, out
        self.first, self.held, self.via_x, self.via_y, self.last = bufs
        self.base = mail.take(self.COPIES)
        half = out.shape[0] // 2
        self.top, self.bot = pl.ds(0, half), pl.ds(half, half)

    @staticmethod
    def scratch(rows, cols):
        half = rows // 2
        return [
            pltpu.VMEM((2, 2, rows, cols), BF16),
            pltpu.VMEM((2, 2, rows, cols), BF16),
            pltpu.VMEM((2, half, cols), BF16),
            pltpu.VMEM((2, half, cols), BF16),
            pltpu.VMEM((4, half, cols), BF16),
        ]

    def begin(self):
        y, c, z, x = self.place
        pair, xn, yn = near(self.place)
        for slot, (py, px) in enumerate(((1 - y, 1 - x), (y, 1 - x), (1 - y, x), (y, x))):
            self.mail.send(
                self.base + slot,
                self.parts.at[rank(py, 1 - c, px)],
                self.first.at[py, px],
                pair,
            )

    def joined(self, slot, py, px):
        y, c, z, x = self.place
        pair, xn, yn = near(self.place)
        self.mail.arrive(self.base + slot, self.first.at[py, px], pair)
        return self.parts[rank(py, c, px)].astype(F32) + self.first[py, px].astype(F32)

    def middle(self):
        y, c, z, x = self.place
        pair, xn, yn = near(self.place)
        send, base, held = self.mail.send, self.base, self.held
        top, bot = self.top, self.bot
        held[1 - y, 1 - x] = self.joined(0, 1 - y, 1 - x).astype(BF16)
        send(base + 4, held.at[1 - y, 1 - x, top], self.via_x.at[1 - y], xn)
        send(base + 5, held.at[1 - y, 1 - x, bot], self.via_y.at[1 - x], yn)
        held[y, 1 - x] = self.joined(1, y, 1 - x).astype(BF16)
        send(base + 6, held.at[y, 1 - x, top], self.via_x.at[y], xn)
        held[1 - y, x] = self.joined(2, 1 - y, x).astype(BF16)
        send(base + 7, held.at[1 - y, x, bot], self.via_y.at[x], yn)
        self.out[...] = self.joined(3, y, x)

    def end(self):
        y, c, z, x = self.place
        pair, xn, yn = near(self.place)
        send, arrive, base, held = self.mail.send, self.mail.arrive, self.base, self.held
        top, bot, last, out = self.top, self.bot, self.last, self.out
        arrive(base + 4, self.via_x.at[1 - y], xn)
        last[0] = (held[1 - y, x, top].astype(F32) + self.via_x[1 - y].astype(F32)).astype(BF16)
        send(base + 8, last.at[0], last.at[2], yn)
        arrive(base + 5, self.via_y.at[1 - x], yn)
        last[1] = (held[y, 1 - x, bot].astype(F32) + self.via_y[1 - x].astype(F32)).astype(BF16)
        send(base + 9, last.at[1], last.at[3], xn)
        arrive(base + 6, self.via_x.at[y], xn)
        out[top] = out[top] + self.via_x[y].astype(F32)
        arrive(base + 7, self.via_y.at[x], yn)
        out[bot] = out[bot] + self.via_y[x].astype(F32)
        arrive(base + 8, last.at[2], yn)
        out[top] = out[top] + last[2].astype(F32)
        arrive(base + 9, last.at[3], xn)
        out[bot] = out[bot] + last[3].astype(F32)


class PlaneSwap:
    COPIES = 7

    def __init__(self, mail, place, src, out):
        self.mail, self.place, self.src, self.out = mail, place, src, out
        self.base = mail.take(self.COPIES)

    def begin(self):
        y, c, z, x = self.place
        me = rank(y, c, x)
        for slot, (dev, other, _) in enumerate(plane_peers(self.place)):
            self.mail.send(self.base + slot, self.src.at[other], self.out.at[me], dev)
        self.out[me] = self.src[me]

    def end(self):
        for slot, (dev, other, _) in enumerate(plane_peers(self.place)):
            self.mail.arrive(self.base + slot, self.out.at[other], dev)


def blk_peers(place):
    y, c, z, x = place
    outer = lax.axis_size("blk") // INNER
    others = [device(y, c, lax.rem(z + k, outer), 1 - x) for k in range(1, outer)]
    return [p[0] for p in line_peers(place)] + others


class RowsOut:
    def __init__(self, mail, place, src, out):
        self.mail, self.place, self.src, self.out = mail, place, src, out
        self.outer = lax.axis_size("blk") // INNER
        self.per = self.outer // INNER
        self.base = mail.take(self.outer)

    def first(self):
        y, c, z, x = self.place
        return self.mail.copy(
            self.base,
            self.src,
            self.out.at[lax.rem(z, self.per), x],
            device(y, c, z, 1 - x),
            self.base + lax.rem(z, self.per) * INNER + x,
        )

    def begin(self):
        y, c, z, x = self.place
        to = z // self.per
        landing = self.base + lax.rem(z, self.per) * INNER + x
        place_there = self.out.at[lax.rem(z, self.per), x]

        @pl.when(to != x)
        def _():
            self.first().start()

        @pl.when(to == x)
        def _():
            self.out[lax.rem(z, self.per), x] = self.src[...]

        for k in range(1, self.outer):
            dev = device(y, c, lax.rem(z + k, self.outer), to)
            self.mail.send(self.base + k, self.src, place_there, dev, landing)

    def end(self):
        y, c, z, x = self.place

        @pl.when(z // self.per != x)
        def _():
            self.first().wait_send()

        for j in range(self.per):
            for ox in range(INNER):
                oz = x * self.per + j
                own = (oz == z) & (x * 0 + ox == x)

                @pl.when(jnp.logical_not(own))
                def _():
                    self.mail.arrive(
                        self.base + j * INNER + ox, self.out.at[j, ox], device(y, c, oz, ox)
                    )


class RowsBack:
    def __init__(self, mail, place, parts, got, out):
        self.mail, self.place, self.parts, self.got, self.out = mail, place, parts, got, out
        self.outer = lax.axis_size("blk") // INNER
        self.per = self.outer // INNER
        self.base = mail.take(self.outer)

    def copies(self):
        y, c, z, x = self.place
        for j in range(self.per):
            for ox in range(INNER):
                oz = x * self.per + j
                own = (oz == z) & (x * 0 + ox == x)
                copy = self.mail.copy(
                    self.base + j * INNER + ox,
                    self.parts.at[j, ox],
                    self.got.at[z],
                    device(y, c, oz, ox),
                    self.base + z,
                )
                yield j, ox, own, copy

    def begin(self):
        y, c, z, x = self.place
        for j, ox, own, copy in self.copies():

            @pl.when(own)
            def _():
                self.got[z] = self.parts[j, ox]

            @pl.when(jnp.logical_not(own))
            def _():
                copy.start()

    def end(self):
        y, c, z, x = self.place
        for j, ox, own, copy in self.copies():

            @pl.when(jnp.logical_not(own))
            def _():
                copy.wait_send()

        to = z // self.per
        for oz in range(self.outer):

            @pl.when(jnp.logical_not((z == oz) & (to == x)))
            def _():
                self.mail.arrive(self.base + oz, self.got.at[oz], device(y, c, z * 0 + oz, to))

        total = self.got[0].astype(F32)
        for oz in range(1, self.outer):
            total = total + self.got[oz].astype(F32)
        self.out[...] = total


def call(body, name, ident, outs, args, copies, scratch=()):
    spec = pl.BlockSpec(memory_space=pltpu.VMEM)
    return pl.pallas_call(
        body,
        name=name,
        out_shape=tuple(jax.ShapeDtypeStruct(shape, dtype) for shape, dtype in outs),
        in_specs=[spec] * len(args),
        out_specs=tuple([spec] * len(outs)),
        scratch_shapes=[
            pltpu.SemaphoreType.DMA((copies,)),
            pltpu.SemaphoreType.DMA((copies,)),
            *scratch,
        ],
        compiler_params=pltpu.CompilerParams(
            collective_id=ident, has_side_effects=True, vmem_limit_bytes=60 * 1024 * 1024
        ),
    )(*args)


def start_kernel(
    x_ref, w_ref, g_ref, gu_ref, wo_ref, xp_ref, wq_ref, gain_ref, gus_ref, wos_ref, ss, rs
):
    place = y, c, z, x = here()
    me = rank(y, c, x)
    head = y * CORES + c
    mail = Mail((ss, rs))
    peers, line = plane_peers(place), line_peers(place)
    greet([p[0] for p in peers] + blk_peers(place))
    w_base, g_base = mail.take(7), mail.take(7)
    zw_base, zg_base = mail.take(len(line)), mail.take(len(line))
    for slot, (dev, other, _) in enumerate(peers):
        mail.send(g_base + slot, g_ref, gain_ref.at[z, me], dev)
        mail.send(w_base + slot, w_ref.at[other], wq_ref.at[head, z, x], dev)
    gain_ref[z, me] = g_ref[...]
    wq_ref[head, z, x] = w_ref[me]
    rows = PlaneGather(mail, place, x_ref, xp_ref)
    swap = PlaneSwap(mail, place, gu_ref, gus_ref)
    block = RowsOut(mail, place, wo_ref, wos_ref)
    rows.begin()
    block.begin()
    for slot, (dev, other, (oh, ox)) in enumerate(peers):
        mail.arrive(g_base + slot, gain_ref.at[z, other], dev)
        mail.arrive(w_base + slot, wq_ref.at[oh, z, ox], dev)
    for slot, (dev, _, _) in enumerate(line):
        mail.send(zg_base + slot, gain_ref.at[z], gain_ref.at[z], dev)
        mail.send(zw_base + slot, wq_ref.at[:, z], wq_ref.at[:, z], dev)
    rows.middle()
    swap.begin()
    rows.end()
    for slot, (dev, _, back) in enumerate(line):
        mail.arrive(zg_base + slot, gain_ref.at[back], dev)
        mail.arrive(zw_base + slot, wq_ref.at[:, back], dev)
    block.end()
    swap.end()
    mail.close()


def line_kernel(kv_ref, og_ref, kvs_ref, ogs_ref, ss, rs):
    place = y, c, z, x = here()
    mail = Mail((ss, rs))
    line = line_peers(place)
    greet([p[0] for p in line] + list(near(place)))
    base = mail.take(len(line))
    for slot, (dev, _, _) in enumerate(line):
        mail.send(base + slot, kv_ref, kvs_ref.at[z], dev)
    rows = PlaneGather(mail, place, og_ref, ogs_ref)
    rows.begin()
    kvs_ref[z] = kv_ref[...]
    rows.middle()
    rows.end()
    for slot, (dev, _, back) in enumerate(line):
        mail.arrive(base + slot, kvs_ref.at[back], dev)
    mail.close()


def gather_kernel(src_ref, out_ref, ss, rs):
    place = here()
    mail = Mail((ss, rs))
    greet(list(near(place)))
    rows = PlaneGather(mail, place, src_ref, out_ref)
    rows.begin()
    rows.middle()
    rows.end()
    mail.close()


def scatter_kernel(parts_ref, out_ref, ss, rs, *bufs):
    place = here()
    mail = Mail((ss, rs))
    greet(list(near(place)))
    rows = PlaneScatter(mail, place, parts_ref, out_ref, bufs)
    rows.begin()
    rows.middle()
    rows.end()
    mail.close()


def back_kernel(dkv_ref, parts_ref, op_ref, kv_ref, out_ref, ops_ref, ss, rs, got, op_got, *bufs):
    place = y, c, z, x = here()
    mail = Mail((ss, rs))
    line = line_peers(place)
    pair, xn, yn = near(place)
    greet(blk_peers(place) + [pair, xn, yn])
    base = mail.take(len(line))
    for slot, (dev, forth, _) in enumerate(line):
        mail.send(base + slot, dkv_ref.at[forth], got.at[slot], dev)
    rows = PlaneScatter(mail, place, parts_ref, out_ref, bufs)
    block = RowsBack(mail, place, op_ref, op_got, ops_ref)
    rows.begin()
    block.begin()
    rows.middle()
    rows.end()
    total = dkv_ref[z].astype(F32)
    for slot, (dev, _, _) in enumerate(line):
        mail.arrive(base + slot, got.at[slot], dev)
        total = total + got[slot].astype(F32)
    kv_ref[...] = total
    block.end()
    mail.close()


def last_kernel(parts_ref, w_ref, gu_ref, out_ref, ws_ref, gus_ref, ss, rs, got, held, *bufs):
    place = y, c, z, x = here()
    me = rank(y, c, x)
    mail = Mail((ss, rs))
    peers, line = plane_peers(place), line_peers(place)
    greet([p[0] for p in line] + [p[0] for p in peers])
    base = mail.take(len(line))
    w_base = mail.take(7)
    for slot, (dev, forth, _) in enumerate(line):
        mail.send(base + slot, w_ref.at[:, forth], got.at[slot], dev)
    rows = PlaneScatter(mail, place, parts_ref, out_ref, bufs)
    swap = PlaneSwap(mail, place, gu_ref, gus_ref)
    rows.begin()
    rows.middle()
    swap.begin()
    rows.end()
    total = w_ref[:, z].astype(F32)
    for slot, (dev, _, _) in enumerate(line):
        mail.arrive(base + slot, got.at[slot], dev)
        total = total + got[slot].astype(F32)
    held[...] = total.reshape(held.shape)
    for slot, (dev, other, _) in enumerate(peers):
        mail.send(w_base + slot, held.at[other], ws_ref.at[me], dev)
    ws_ref[me] = held[me]
    for slot, (dev, other, _) in enumerate(peers):
        mail.arrive(w_base + slot, ws_ref.at[other], dev)
    swap.end()
    mail.close()


def small_kernel(v_ref, out_ref, ss, rs, got, held):
    place = y, c, z, x = here()
    me = rank(y, c, x)
    mail = Mail((ss, rs))
    peers, line = plane_peers(place), line_peers(place)
    greet([p[0] for p in line] + [p[0] for p in peers])
    p_base, z_base = mail.take(7), mail.take(len(line))
    for slot, (dev, other, _) in enumerate(peers):
        mail.send(p_base + slot, v_ref, got.at[me], dev)
    got[me] = v_ref[...]
    for slot, (dev, other, _) in enumerate(peers):
        mail.arrive(p_base + slot, got.at[other], dev)
    held[z] = jnp.sum(got[...], axis=0)
    for slot, (dev, _, _) in enumerate(line):
        mail.send(z_base + slot, held.at[z], held.at[z], dev)
    for slot, (dev, _, back) in enumerate(line):
        mail.arrive(z_base + slot, held.at[back], dev)
    out_ref[...] = jnp.sum(held[...], axis=0)
    mail.close()


SPANS = 4
LOG2E = math.log2(math.e)
NT = (((1,), (1,)), ((), ()))


def lanes(shape):
    return lax.broadcasted_iota(jnp.int32, shape, len(shape) - 1)


def stack_left(block, size):
    wide = block.astype(F32)
    left = lanes(wide.shape) < size
    first = jnp.where(left, wide, 0.0)
    second = jnp.where(left, pltpu.roll(wide, size, 1), 0.0)
    return jnp.concatenate([first, second], axis=0).astype(BF16)


def stack_right(block, size):
    wide = block.astype(F32)
    right = lanes(wide.shape) >= size
    first = jnp.where(right, pltpu.roll(wide, size, 1), 0.0)
    second = jnp.where(right, wide, 0.0)
    return jnp.concatenate([first, second], axis=0).astype(BF16)


def forward_kernel(own_ref, at_ref, q_ref, kv_ref, out_ref, lse_ref, keys, ones):
    count, rows, size2 = q_ref.shape
    size = size2 // 2
    scale = float(size) ** (-0.5) * LOG2E
    step = SPANS * rows

    def place_rows(p, carry):
        block = kv_ref[at_ref[p]]
        keys[pl.ds(p * rows, rows)] = block
        ones[pl.ds(p * rows, rows)] = jnp.where(lanes(block.shape) < size, 1.0, block).astype(BF16)
        return carry

    lax.fori_loop(0, kv_ref.shape[0], place_rows, 0)

    def one_block(r, carry):
        place = own_ref[r]
        queries = stack_left(q_ref[r], size)

        def weights(c):
            part = keys[pl.ds(c * step, step)]
            scores = lax.dot_general(queries, part, NT, preferred_element_type=F32)
            return jnp.exp2(scores * scale)

        def mix(c, held, total):
            part = ones[pl.ds(c * step, step)]
            return total + jnp.dot(held.astype(BF16), part, preferred_element_type=F32)

        def full(c, total):
            return mix(c, weights(c), total)

        last = place // SPANS
        total = lax.fori_loop(0, last, full, jnp.zeros((2 * rows, size2), F32))
        held = weights(last)
        row = lax.broadcasted_iota(jnp.int32, held.shape, 0)
        row = jnp.where(row >= rows, row - rows, row) + (place - last * SPANS) * rows
        held = jnp.where(lanes(held.shape) <= row, held, 0.0)
        total = mix(last, held, total)
        divided = total / total[:, :1]
        left = lanes((rows, size2)) < size
        out_ref[r] = jnp.where(left, pltpu.roll(divided[:rows], size, 1), divided[rows:]).astype(
            BF16
        )
        lse_ref[r] = jnp.log2(total.T[:8])
        return carry

    lax.fori_loop(0, count, one_block, 0)


def backward_kernel(
    own_ref, at_ref, q_ref, kv_ref, out_ref, do_ref, lse_ref, dq_ref, dkv_ref, keys, turned, sums
):
    count, rows, size2 = q_ref.shape
    size = size2 // 2
    scale = float(size) ** (-0.5)
    step = SPANS * rows
    spans = kv_ref.shape[0]

    def place_rows(p, carry):
        block = kv_ref[at_ref[p]]
        keys[pl.ds(p * rows, rows)] = block
        turned[:, pl.ds(p * rows, rows)] = block.astype(F32).T.astype(BF16)
        return carry

    lax.fori_loop(0, spans, place_rows, 0)
    sums[...] = jnp.zeros_like(sums)

    def one_block(r, carry):
        place = own_ref[r]
        queries = stack_left(q_ref[r], size)
        grads = stack_right(do_ref[r], size)
        both = (do_ref[r].astype(F32) * out_ref[r].astype(F32)).T
        delta = jnp.concatenate(
            [jnp.sum(both[:size], axis=0)[None], jnp.sum(both[size:], axis=0)[None]], axis=1
        )
        lse = lse_ref[r][:1]

        def one_step(c, total, masked):
            at = pl.ds(pl.multiple_of(c * step, step), step)
            part = keys[at]
            scores = lax.dot_general(part, queries, NT, preferred_element_type=F32)
            prob = jnp.exp2(scores * (scale * LOG2E) - lse)
            if masked:
                key = lax.broadcasted_iota(jnp.int32, prob.shape, 0)
                row = lanes(prob.shape)
                row = jnp.where(row >= rows, row - rows, row) + (place - c * SPANS) * rows
                prob = jnp.where(key <= row, prob, 0.0)
            dprob = lax.dot_general(part, grads, NT, preferred_element_type=F32)
            dscore = (prob * (dprob - delta)).astype(BF16)
            sums[at] += jnp.dot(dscore, queries, preferred_element_type=F32) + jnp.dot(
                prob.astype(BF16), grads, preferred_element_type=F32
            )
            return total + jnp.dot(turned[:, at], dscore, preferred_element_type=F32)

        last = place // SPANS
        total = lax.fori_loop(
            0, last, lambda c, t: one_step(c, t, False), jnp.zeros((size2, 2 * rows), F32)
        )
        total = one_step(last, total, True).T * scale
        left = lanes((rows, size2)) < size
        dq_ref[r] = jnp.where(left, total[:rows], pltpu.roll(total[rows:], size, 1)).astype(BF16)
        return carry

    lax.fori_loop(0, count, one_block, 0)

    def give_rows(p, carry):
        block = sums[pl.ds(p * rows, rows)]
        factor = jnp.where(lanes(block.shape) < size, scale, 1.0)
        dkv_ref[at_ref[p]] = (block * factor).astype(BF16)
        return carry

    lax.fori_loop(0, spans, give_rows, 0)


def attention(body, name, own, at, args, outs, scratch, flops):
    vmem = pl.BlockSpec(memory_space=pltpu.VMEM)
    smem = pl.BlockSpec(memory_space=pltpu.SMEM)
    return pl.pallas_call(
        body,
        name=name,
        out_shape=tuple(jax.ShapeDtypeStruct(shape, dtype) for shape, dtype in outs),
        in_specs=[smem, smem] + [vmem] * len(args),
        out_specs=tuple([vmem] * len(outs)),
        scratch_shapes=scratch,
        cost_estimate=pl.CostEstimate(flops=flops, bytes_accessed=4 << 20, transcendentals=0),
        compiler_params=pltpu.CompilerParams(vmem_limit_bytes=60 * 1024 * 1024),
    )(own, at, *args)


def rms_norm(values, gain_vec):
    inverse = lax.rsqrt(jnp.mean(values * values, axis=-1, keepdims=True) + EPS)
    return values * inverse * gain_vec


def rotate(field_in, where_at):
    half_size = field_in.shape[-1] // 2
    frequency = jnp.exp(
        jnp.arange(half_size, dtype=F32) * F32(-2.0 * math.log(THETA) / field_in.shape[-1])
    )
    angles = where_at.astype(F32)[:, None] * frequency[None, :]
    cosine = jnp.cos(angles)[:, None, :]
    sine_part = jnp.sin(angles)[:, None, :]
    first_half = field_in[..., :half_size]
    second_half = field_in[..., half_size:]
    return jnp.concatenate(
        [
            first_half * cosine - second_half * sine_part,
            second_half * cosine + first_half * sine_part,
        ],
        axis=-1,
    )


def head_map(raw_rows, gain_vec, where_at):
    row_count = raw_rows.shape[0]
    shaped = raw_rows.reshape(row_count, -1, gain_vec.shape[0])
    return rotate(rms_norm(shaped, gain_vec), where_at).reshape(row_count, -1)


def shifts(outer, step):
    return [
        (z * INNER + x, ((z + step) % outer) * INNER + x)
        for z in range(outer)
        for x in range(INNER)
    ]


def line_gather(piece, axis, full_shape, z, outer):
    full = jnp.zeros(full_shape, piece.dtype)
    full = lax.dynamic_update_slice_in_dim(full, jnp.expand_dims(piece, axis), z, axis)
    for step in range(1, outer):
        got = lax.ppermute(piece, "blk", shifts(outer, step))
        full = lax.dynamic_update_slice_in_dim(
            full, jnp.expand_dims(got, axis), (z + outer - step) % outer, axis
        )
    return full


def line_scatter(parts, axis, z, outer):
    total = lax.dynamic_index_in_dim(parts, z, axis, keepdims=False).astype(F32)
    for step in range(1, outer):
        piece = lax.dynamic_index_in_dim(parts, (z + step) % outer, axis, keepdims=False)
        total = total + lax.ppermute(piece.astype(BF16), "blk", shifts(outer, step)).astype(F32)
    return total


def dot(a, b):
    return jnp.dot(a, b, preferred_element_type=F32)


def local(
    block_input,
    span_order,
    norm1_gain,
    w_query,
    key_weight,
    value_weight,
    qk_gain,
    w_out,
    norm2_gain,
    w_gate,
    w_up,
    w_down,
    out_grad,
):
    heads = lax.axis_size("head")
    blocks = lax.axis_size("blk")
    outer = blocks // INNER
    plane = heads * INNER
    z = lax.axis_index("blk") // INNER
    rows, width = block_input.shape
    head_size = qk_gain.shape[1]
    w_rows = w_query.shape[0]
    f_rows = w_down.shape[0]
    q_cols = w_query.shape[1] // plane
    k_cols = key_weight.shape[1] // plane
    a_cols = q_cols + 2 * k_cols
    ff = f_rows * outer
    tokens = plane * rows

    by_place = span_order.reshape(heads, outer, INNER)
    own_spans = lax.dynamic_index_in_dim(by_place, z, 1, keepdims=False).reshape(plane)
    all_spans = by_place.transpose(1, 0, 2).reshape(outer * plane)
    inside = jnp.arange(rows, dtype=jnp.int32)
    tok_where = (own_spans[:, None] * rows + inside[None, :]).reshape(tokens)

    w8 = jnp.concatenate(
        [
            w_query.reshape(w_rows, plane, q_cols),
            key_weight.reshape(w_rows, plane, k_cols),
            value_weight.reshape(w_rows, plane, k_cols),
        ],
        axis=-1,
    ).transpose(1, 0, 2)

    def cut(weight):
        shaped = weight.reshape(w_rows, heads, outer, INNER, f_rows)
        return shaped.transpose(1, 3, 0, 2, 4).reshape(plane, w_rows, ff)

    gu8 = jnp.concatenate([cut(w_gate), cut(w_up)], axis=-1)
    gains = jnp.zeros((16, 128), BF16)
    gains = gains.at[0, :w_rows].set(norm1_gain).at[1, :w_rows].set(norm2_gain)
    down_full = line_gather(w_down, 0, (outer, f_rows, width), z, outer).reshape(ff, width)

    n_line = outer - 1
    x_all, wqkv, gains_all, gu_piece, out_mine = call(
        start_kernel,
        "start",
        1,
        [
            ((plane, rows, width), BF16),
            ((heads, outer, INNER, w_rows, a_cols), BF16),
            ((outer, plane, 16, 128), BF16),
            ((plane, w_rows, 2 * ff), BF16),
            ((outer // INNER, INNER, w_rows, width), BF16),
        ],
        (block_input, w8, gains, gu8, w_out),
        14 + 2 * n_line + PlaneGather.COPIES + PlaneSwap.COPIES + outer,
    )
    out_mine = out_mine.reshape(q_cols, width)
    wqkv = wqkv.reshape(width, a_cols)
    gains_all = (
        gains_all[:, :, :2, :w_rows]
        .reshape(outer, heads, INNER, 2, w_rows)
        .transpose(3, 1, 0, 2, 4)
        .reshape(2, width)
        .astype(F32)
    )
    gain_one, gain_two = gains_all[0], gains_all[1]
    gu_full = line_gather(
        gu_piece.reshape(heads, INNER * w_rows, 2 * ff),
        1,
        (heads, outer, INNER * w_rows, 2 * ff),
        z,
        outer,
    ).reshape(width, 2 * ff)

    normed = rms_norm(x_all.reshape(tokens, width).astype(F32), gain_one).astype(BF16)
    qkv_raw = dot(normed, wqkv)
    q_raw = qkv_raw[:, :q_cols]
    k_raw = qkv_raw[:, q_cols : q_cols + k_cols]
    v_raw = qkv_raw[:, q_cols + k_cols :]

    def query_map(raw_rows, gain_vec):
        return head_map(raw_rows, gain_vec, tok_where)

    queries = query_map(q_raw, qk_gain[0]).astype(BF16)
    keys = query_map(k_raw, qk_gain[1]).astype(BF16)
    kv = jnp.concatenate([keys, v_raw.astype(BF16)], axis=-1)
    kv_all, og_all = call(
        line_kernel,
        "line",
        2,
        [((outer, tokens, 2 * k_cols), BF16), ((plane, rows, width), BF16)],
        (kv, out_grad),
        n_line + PlaneGather.COPIES,
    )
    og_all = og_all.reshape(tokens, width)
    spans = outer * plane
    span_at = jnp.sum(
        jnp.where(
            all_spans[:, None] == jnp.arange(spans, dtype=jnp.int32)[None, :],
            jnp.arange(spans, dtype=jnp.int32)[:, None],
            0,
        ),
        axis=0,
    )
    q_blocks = queries.reshape(plane, rows, q_cols)
    kv_blocks = kv_all.reshape(spans, rows, q_cols)
    attended, log_total = attention(
        forward_kernel,
        "attend",
        own_spans,
        span_at,
        (q_blocks, kv_blocks),
        [((plane, rows, q_cols), BF16), ((plane, 8, 2 * rows), F32)],
        [pltpu.VMEM((spans * rows, q_cols), BF16), pltpu.VMEM((spans * rows, q_cols), BF16)],
        8 * tokens * spans * rows * q_cols,
    )
    attended_rows = attended.reshape(tokens, q_cols)

    def scatter(parts, name, ident):
        return call(
            scatter_kernel,
            name,
            ident,
            [((rows, width), F32)],
            (parts.astype(BF16).reshape(plane, rows, width),),
            PlaneScatter.COPIES,
            PlaneScatter.scratch(rows, width),
        )[0]

    def gather(block, name, ident):
        return call(
            gather_kernel,
            name,
            ident,
            [((plane, rows, width), BF16)],
            (block,),
            PlaneGather.COPIES,
        )[0].reshape(tokens, width)

    in_flat = block_input.astype(F32)
    middle = in_flat + scatter(dot(attended_rows, out_mine), "mix", 3)
    normed2_own = rms_norm(middle, gain_two).astype(BF16)
    normed2 = gather(normed2_own, "widen", 4)

    gu_rows = dot(normed2, gu_full)
    gate_rows, up_rows = gu_rows[:, :ff], gu_rows[:, ff:]
    hidden, gate_back = jax.vjp(lambda a, b: jax.nn.silu(a) * b, gate_rows, up_rows)
    hidden = hidden.astype(BF16)
    dhidden = dot(og_all, down_full.T)
    dgate, dup = gate_back(dhidden)
    dgu = jnp.concatenate([dgate.astype(BF16), dup.astype(BF16)], axis=-1)
    dnormed2 = scatter(dot(dgu, gu_full.T), "narrow", 5)
    out_parts = dot(hidden, down_full).astype(BF16).reshape(plane, rows, width)
    gu_grad = dot(normed2.T, dgu)
    down_grad = dot(hidden.T, og_all)
    down_grad = line_scatter(down_grad.reshape(outer, f_rows, width), 0, z, outer)
    gu_grad = line_scatter(
        gu_grad.reshape(heads, outer, INNER * w_rows, 2 * ff), 1, z, outer
    ).reshape(plane, w_rows, 2 * ff)

    _, norm2_back = jax.vjp(rms_norm, middle, gain_two)
    dmiddle_norm, norm2_grad = norm2_back(dnormed2)
    dmiddle = out_grad.astype(F32) + dmiddle_norm
    dmid_all = gather(dmiddle.astype(BF16), "spread", 6)

    out_proj = dot(attended_rows.T, dmid_all)
    dattended = dot(dmid_all, out_mine.T).astype(BF16)
    dqueries, dkv = attention(
        backward_kernel,
        "attend_back",
        own_spans,
        span_at,
        (q_blocks, kv_blocks, attended, dattended.reshape(plane, rows, q_cols), log_total),
        [((plane, rows, q_cols), BF16), ((spans, rows, q_cols), BF16)],
        [
            pltpu.VMEM((spans * rows, q_cols), BF16),
            pltpu.VMEM((q_cols, spans * rows), BF16),
            pltpu.VMEM((spans * rows, q_cols), F32),
        ],
        20 * tokens * spans * rows * q_cols,
    )
    dkv_own, ffn_out, out_proj_grad = call(
        back_kernel,
        "back",
        7,
        [((tokens, 2 * k_cols), F32), ((rows, width), F32), ((w_rows, width), F32)],
        (
            dkv.reshape(outer, tokens, 2 * k_cols),
            out_parts,
            out_proj.astype(BF16).reshape(outer // INNER, INNER, w_rows, width),
        ),
        n_line + PlaneScatter.COPIES + outer,
        [
            pltpu.VMEM((n_line, tokens, 2 * k_cols), BF16),
            pltpu.VMEM((outer, w_rows, width), BF16),
        ]
        + PlaneScatter.scratch(rows, width),
    )
    block_output = (middle + ffn_out).astype(BF16)
    dkv_own = dkv_own.astype(BF16)
    dqueries = dqueries.reshape(tokens, q_cols)
    _, query_back = jax.vjp(query_map, q_raw, qk_gain[0])
    dq_raw, qgain_grad = query_back(dqueries.astype(F32))
    _, key_back = jax.vjp(query_map, k_raw, qk_gain[1])
    dk_raw, kgain_grad = key_back(dkv_own[:, :k_cols].astype(F32))
    dqkv = jnp.concatenate(
        [dq_raw.astype(BF16), dk_raw.astype(BF16), dkv_own[:, k_cols:]], axis=-1
    )
    wqkv_grad = dot(normed.T, dqkv).astype(BF16)
    dnormed, wqkv_own, gu_own = call(
        last_kernel,
        "last",
        8,
        [
            ((rows, width), F32),
            ((plane, w_rows, a_cols), F32),
            ((plane, w_rows, 2 * ff), BF16),
        ],
        (
            dot(dqkv, wqkv.T).astype(BF16).reshape(plane, rows, width),
            wqkv_grad.reshape(heads, outer, INNER, w_rows, a_cols),
            gu_grad.astype(BF16),
        ),
        n_line + 7 + PlaneScatter.COPIES + PlaneSwap.COPIES,
        [
            pltpu.VMEM((n_line, heads, INNER, w_rows, a_cols), BF16),
            pltpu.VMEM((plane, w_rows, a_cols), F32),
        ]
        + PlaneScatter.scratch(rows, width),
    )
    _, norm1_back = jax.vjp(rms_norm, in_flat, gain_one)
    dinput_norm, norm1_grad = norm1_back(dnormed)
    input_grad = (dmiddle + dinput_norm).astype(BF16)

    small = jnp.concatenate([norm1_grad, norm2_grad, qgain_grad, kgain_grad])
    small_rows = -(-small.shape[0] // 1024) * 8
    small = jnp.pad(small, (0, small_rows * 128 - small.shape[0])).reshape(small_rows, 128)
    summed = call(
        small_kernel,
        "small",
        9,
        [((small_rows, 128), F32)],
        (small,),
        7 + n_line,
        [pltpu.VMEM((plane, small_rows, 128), F32), pltpu.VMEM((outer, small_rows, 128), F32)],
    )[0].reshape(-1)
    own = (lax.axis_index("head") * blocks + lax.axis_index("blk")) * w_rows
    norm1_out = lax.dynamic_slice_in_dim(summed, own, w_rows)
    norm2_out = lax.dynamic_slice_in_dim(summed, width + own, w_rows)
    qk_gain_grad = summed[2 * width : 2 * width + 2 * head_size].reshape(2, head_size)

    def columns(blocks_in):
        return blocks_in.transpose(1, 0, 2).reshape(w_rows, -1)

    query_grad = columns(wqkv_own[:, :, :q_cols])
    key_grad = columns(wqkv_own[:, :, q_cols : q_cols + k_cols])
    value_grad = columns(wqkv_own[:, :, q_cols + k_cols :])

    def uncut(blocks_in):
        shaped = blocks_in.astype(F32).reshape(heads, INNER, w_rows, outer, f_rows)
        return shaped.transpose(2, 0, 3, 1, 4).reshape(w_rows, -1)

    gate_grad = uncut(gu_own[:, :, :ff])
    up_grad = uncut(gu_own[:, :, ff:])
    return (
        block_output,
        input_grad,
        norm1_out,
        query_grad,
        key_grad,
        value_grad,
        qk_gain_grad,
        out_proj_grad,
        norm2_out,
        gate_grad,
        up_grad,
        down_grad,
    )


def solution(mesh):
    split = P(("head", "blk"), None)
    line = P(("head", "blk"))
    in_specs = (split, P(), line, split, split, split, P(), split, line, split, split, split, split)
    out_specs = (split, split, line, split, split, split, P(), split, line, split, split, split)
    return jax.shard_map(local, mesh=mesh, in_specs=in_specs, out_specs=out_specs, check_vma=False)
```

```python
import functools
import math

import jax
import jax.numpy as jnp
from jax import lax
from jax.experimental import pallas as pl
from jax.experimental.pallas import tpu as pltpu
from jax.sharding import PartitionSpec as P

EPS = 1e-05
THETA = 1000000.0
LANES = 128
CORES = 2
INNER = 2
MESH = pl.DeviceIdType.MESH
F32 = jnp.float32
BF16 = jnp.bfloat16
NT = (((1,), (1,)), ((), ()))
TN = (((0,), (0,)), ((), ()))


def here():
    head = lax.axis_index("head")
    blk = lax.axis_index("blk")
    return head // CORES, head % CORES, blk // INNER, blk % INNER


def device(y, c, z, x):
    return (y * CORES + c, z * INNER + x)


def rank(y, c, x):
    return (y * CORES + c) * INNER + x


def plane_peers(place):
    y, c, z, x = place
    peers = []
    for bits in range(1, 8):
        py = 1 - y if bits & 4 else y
        pc = 1 - c if bits & 2 else c
        px = 1 - x if bits & 1 else x
        peers.append((device(py, pc, z, px), rank(py, pc, px), (py * CORES + pc, px)))
    return peers


def line_peers(place):
    y, c, z, x = place
    outer = lax.axis_size("blk") // INNER
    forth = [lax.rem(z + k, outer) for k in range(1, outer)]
    back = [lax.rem(z + outer - k, outer) for k in range(1, outer)]
    return [(device(y, c, f, x), f, b) for f, b in zip(forth, back)]


def greet(devices):
    barrier = pltpu.get_barrier_semaphore()
    for dev in devices:
        pl.semaphore_signal(barrier, inc=1, device_id=dev, device_id_type=MESH)
    pl.semaphore_wait(barrier, len(devices))


class Mail:
    def __init__(self, sems):
        self.sends, self.recvs = sems
        self.used = 0
        self.open = []

    def take(self, count):
        first = self.used
        self.used += count
        return first

    def copy(self, slot, src, dst, dev, landing=None):
        return pltpu.make_async_remote_copy(
            src_ref=src,
            dst_ref=dst,
            send_sem=self.sends.at[slot],
            recv_sem=self.recvs.at[slot if landing is None else landing],
            device_id=dev,
            device_id_type=MESH,
        )

    def send(self, slot, src, dst, dev, landing=None):
        copy = self.copy(slot, src, dst, dev, landing)
        copy.start()
        self.open.append(copy)

    def arrive(self, slot, dst, dev):
        self.copy(slot, dst, dst, dev).wait_recv()

    def close(self):
        for copy in self.open:
            copy.wait_send()


def near(place):
    y, c, z, x = place
    return device(y, 1 - c, z, x), device(y, c, z, 1 - x), device(1 - y, c, z, x)


class PlaneGather:
    COPIES = 11

    def __init__(self, mail, place, src, out):
        self.mail, self.place, self.src, self.out = mail, place, src, out
        self.base = mail.take(self.COPIES)
        half = src.shape[0] // 2
        self.top, self.bot = pl.ds(0, half), pl.ds(half, half)

    def begin(self):
        y, c, z, x = self.place
        pair, xn, yn = near(self.place)
        me = rank(y, c, x)
        send, base, src, out = self.mail.send, self.base, self.src, self.out
        top, bot = self.top, self.bot
        send(base + 0, src.at[top], out.at[me, top], xn)
        send(base + 1, src.at[bot], out.at[me, bot], yn)
        send(base + 2, src.at[bot], out.at[me, bot], xn)
        send(base + 3, src.at[top], out.at[me, top], yn)
        send(base + 4, src, out.at[me], pair)
        out[me] = src[...]

    def middle(self):
        y, c, z, x = self.place
        pair, xn, yn = near(self.place)
        xr, yr = rank(y, c, 1 - x), rank(1 - y, c, x)
        send, arrive, base, out = self.mail.send, self.mail.arrive, self.base, self.out
        top, bot = self.top, self.bot
        arrive(base + 0, out.at[xr, top], xn)
        send(base + 5, out.at[xr, top], out.at[xr, top], yn)
        arrive(base + 1, out.at[yr, bot], yn)
        send(base + 6, out.at[yr, bot], out.at[yr, bot], xn)
        arrive(base + 2, out.at[xr, bot], xn)
        send(base + 7, out.at[xr], out.at[xr], pair)
        arrive(base + 3, out.at[yr, top], yn)
        send(base + 8, out.at[yr], out.at[yr], pair)

    def end(self):
        y, c, z, x = self.place
        pair, xn, yn = near(self.place)
        dr = rank(1 - y, c, 1 - x)
        send, arrive, base, out = self.mail.send, self.mail.arrive, self.base, self.out
        top, bot = self.top, self.bot
        arrive(base + 5, out.at[dr, top], yn)
        send(base + 9, out.at[dr, top], out.at[dr, top], pair)
        arrive(base + 6, out.at[dr, bot], xn)
        send(base + 10, out.at[dr, bot], out.at[dr, bot], pair)
        arrive(base + 4, out.at[rank(y, 1 - c, x)], pair)
        arrive(base + 7, out.at[rank(y, 1 - c, 1 - x)], pair)
        arrive(base + 8, out.at[rank(1 - y, 1 - c, x)], pair)
        far = rank(1 - y, 1 - c, 1 - x)
        arrive(base + 9, out.at[far, top], pair)
        arrive(base + 10, out.at[far, bot], pair)


class PlaneScatter:
    COPIES = 10

    def __init__(self, mail, place, parts, out, bufs, make=None):
        self.mail, self.place, self.parts, self.out = mail, place, parts, out
        self.make = make or (lambda block: None)
        self.first, self.held, self.via_x, self.via_y, self.last = bufs
        self.base = mail.take(self.COPIES)
        half = out.shape[0] // 2
        self.top, self.bot = pl.ds(0, half), pl.ds(half, half)

    @staticmethod
    def scratch(rows, cols):
        half = rows // 2
        return [
            pltpu.VMEM((2, 2, rows, cols), BF16),
            pltpu.VMEM((2, 2, rows, cols), BF16),
            pltpu.VMEM((2, half, cols), BF16),
            pltpu.VMEM((2, half, cols), BF16),
            pltpu.VMEM((4, half, cols), BF16),
        ]

    def begin(self):
        y, c, z, x = self.place
        pair, xn, yn = near(self.place)
        for slot, (py, px) in enumerate(((1 - y, 1 - x), (y, 1 - x), (1 - y, x), (y, x))):
            self.make(rank(py, 1 - c, px))
            self.mail.send(
                self.base + slot,
                self.parts.at[rank(py, 1 - c, px)],
                self.first.at[py, px],
                pair,
            )

    def joined(self, slot, py, px):
        y, c, z, x = self.place
        pair, xn, yn = near(self.place)
        self.make(rank(py, c, px))
        self.mail.arrive(self.base + slot, self.first.at[py, px], pair)
        return self.parts[rank(py, c, px)].astype(F32) + self.first[py, px].astype(F32)

    def middle(self):
        y, c, z, x = self.place
        pair, xn, yn = near(self.place)
        send, base, held = self.mail.send, self.base, self.held
        top, bot = self.top, self.bot
        held[1 - y, 1 - x] = self.joined(0, 1 - y, 1 - x).astype(BF16)
        send(base + 4, held.at[1 - y, 1 - x, top], self.via_x.at[1 - y], xn)
        send(base + 5, held.at[1 - y, 1 - x, bot], self.via_y.at[1 - x], yn)
        held[y, 1 - x] = self.joined(1, y, 1 - x).astype(BF16)
        send(base + 6, held.at[y, 1 - x, top], self.via_x.at[y], xn)
        held[1 - y, x] = self.joined(2, 1 - y, x).astype(BF16)
        send(base + 7, held.at[1 - y, x, bot], self.via_y.at[x], yn)
        self.out[...] = self.joined(3, y, x)

    def end(self):
        y, c, z, x = self.place
        pair, xn, yn = near(self.place)
        send, arrive, base, held = self.mail.send, self.mail.arrive, self.base, self.held
        top, bot, last, out = self.top, self.bot, self.last, self.out
        arrive(base + 4, self.via_x.at[1 - y], xn)
        last[0] = (held[1 - y, x, top].astype(F32) + self.via_x[1 - y].astype(F32)).astype(BF16)
        send(base + 8, last.at[0], last.at[2], yn)
        arrive(base + 5, self.via_y.at[1 - x], yn)
        last[1] = (held[y, 1 - x, bot].astype(F32) + self.via_y[1 - x].astype(F32)).astype(BF16)
        send(base + 9, last.at[1], last.at[3], xn)
        arrive(base + 6, self.via_x.at[y], xn)
        out[top] = out[top] + self.via_x[y].astype(F32)
        arrive(base + 7, self.via_y.at[x], yn)
        out[bot] = out[bot] + self.via_y[x].astype(F32)
        arrive(base + 8, last.at[2], yn)
        out[top] = out[top] + last[2].astype(F32)
        arrive(base + 9, last.at[3], xn)
        out[bot] = out[bot] + last[3].astype(F32)


class LineGather:
    def __init__(self, mail, place, src, out):
        self.mail, self.place, self.src, self.out = mail, place, src, out
        self.line = line_peers(place)
        self.base = mail.take(len(self.line))

    def begin(self):
        z = self.place[2]
        for slot, (dev, _, _) in enumerate(self.line):
            self.mail.send(self.base + slot, self.src, self.out.at[z], dev)
        self.out[z] = self.src[...]

    def end(self):
        for slot, (dev, _, back) in enumerate(self.line):
            self.mail.arrive(self.base + slot, self.out.at[back], dev)


class LineScatter:
    def __init__(self, mail, place, parts, got):
        self.mail, self.place, self.parts, self.got = mail, place, parts, got
        self.line = line_peers(place)
        self.base = mail.take(len(self.line))

    def begin(self):
        for slot, (dev, forth, _) in enumerate(self.line):
            self.mail.send(self.base + slot, self.parts.at[forth], self.got.at[slot], dev)

    def end(self):
        total = self.parts[self.place[2]].astype(F32)
        for slot, (dev, _, _) in enumerate(self.line):
            self.mail.arrive(self.base + slot, self.got.at[slot], dev)
            total = total + self.got[slot].astype(F32)
        return total


class PlaneSwap:
    COPIES = 7

    def __init__(self, mail, place, src, out):
        self.mail, self.place, self.src, self.out = mail, place, src, out
        self.base = mail.take(self.COPIES)

    def begin(self):
        y, c, z, x = self.place
        me = rank(y, c, x)
        for slot, (dev, other, _) in enumerate(plane_peers(self.place)):
            self.mail.send(self.base + slot, self.src.at[other], self.out.at[me], dev)
        self.out[me] = self.src[me]

    def end(self):
        for slot, (dev, other, _) in enumerate(plane_peers(self.place)):
            self.mail.arrive(self.base + slot, self.out.at[other], dev)


def blk_peers(place):
    y, c, z, x = place
    outer = lax.axis_size("blk") // INNER
    others = [device(y, c, lax.rem(z + k, outer), 1 - x) for k in range(1, outer)]
    return [p[0] for p in line_peers(place)] + others


class RowsOut:
    def __init__(self, mail, place, src, out):
        self.mail, self.place, self.src, self.out = mail, place, src, out
        self.outer = lax.axis_size("blk") // INNER
        self.per = self.outer // INNER
        self.base = mail.take(self.outer)

    def first(self):
        y, c, z, x = self.place
        return self.mail.copy(
            self.base,
            self.src,
            self.out.at[lax.rem(z, self.per), x],
            device(y, c, z, 1 - x),
            self.base + lax.rem(z, self.per) * INNER + x,
        )

    def begin(self):
        y, c, z, x = self.place
        to = z // self.per
        landing = self.base + lax.rem(z, self.per) * INNER + x
        place_there = self.out.at[lax.rem(z, self.per), x]

        @pl.when(to != x)
        def _():
            self.first().start()

        @pl.when(to == x)
        def _():
            self.out[lax.rem(z, self.per), x] = self.src[...]

        for k in range(1, self.outer):
            dev = device(y, c, lax.rem(z + k, self.outer), to)
            self.mail.send(self.base + k, self.src, place_there, dev, landing)

    def end(self):
        y, c, z, x = self.place

        @pl.when(z // self.per != x)
        def _():
            self.first().wait_send()

        for j in range(self.per):
            for ox in range(INNER):
                oz = x * self.per + j
                own = (oz == z) & (x * 0 + ox == x)

                @pl.when(jnp.logical_not(own))
                def _():
                    self.mail.arrive(
                        self.base + j * INNER + ox, self.out.at[j, ox], device(y, c, oz, ox)
                    )


class RowsBack:
    def __init__(self, mail, place, parts, got, out):
        self.mail, self.place, self.parts, self.got, self.out = mail, place, parts, got, out
        self.outer = lax.axis_size("blk") // INNER
        self.per = self.outer // INNER
        self.base = mail.take(self.outer)

    def copies(self):
        y, c, z, x = self.place
        for j in range(self.per):
            for ox in range(INNER):
                oz = x * self.per + j
                own = (oz == z) & (x * 0 + ox == x)
                copy = self.mail.copy(
                    self.base + j * INNER + ox,
                    self.parts.at[j, ox],
                    self.got.at[z],
                    device(y, c, oz, ox),
                    self.base + z,
                )
                yield j, ox, own, copy

    def begin(self):
        y, c, z, x = self.place
        for j, ox, own, copy in self.copies():

            @pl.when(own)
            def _():
                self.got[z] = self.parts[j, ox]

            @pl.when(jnp.logical_not(own))
            def _():
                copy.start()

    def end(self):
        y, c, z, x = self.place
        for j, ox, own, copy in self.copies():

            @pl.when(jnp.logical_not(own))
            def _():
                copy.wait_send()

        to = z // self.per
        for oz in range(self.outer):

            @pl.when(jnp.logical_not((z == oz) & (to == x)))
            def _():
                self.mail.arrive(self.base + oz, self.got.at[oz], device(y, c, z * 0 + oz, to))

        total = self.got[0].astype(F32)
        for oz in range(1, self.outer):
            total = total + self.got[oz].astype(F32)
        self.out[...] = total


def call(body, name, ident, outs, args, copies, scratch=()):
    spec = pl.BlockSpec(memory_space=pltpu.VMEM)
    return pl.pallas_call(
        body,
        name=name,
        out_shape=tuple(jax.ShapeDtypeStruct(shape, dtype) for shape, dtype in outs),
        in_specs=[spec] * len(args),
        out_specs=tuple([spec] * len(outs)),
        scratch_shapes=[
            pltpu.SemaphoreType.DMA((copies,)),
            pltpu.SemaphoreType.DMA((copies,)),
            *scratch,
        ],
        compiler_params=pltpu.CompilerParams(
            collective_id=ident, has_side_effects=True, vmem_limit_bytes=60 * 1024 * 1024
        ),
    )(*args)


def lanes(shape):
    return lax.broadcasted_iota(jnp.int32, shape, len(shape) - 1)


def rms_of(values):
    return lax.rsqrt(jnp.mean(values * values, axis=-1, keepdims=True) + EPS)


def rms_back(values, gain_vec, grad):
    inverse = rms_of(values)
    shaped = grad * gain_vec
    mean = jnp.mean(values * shaped, axis=-1, keepdims=True)
    dgain = jnp.sum(grad * values * inverse, axis=0, keepdims=True)
    return inverse * shaped - values * (inverse * inverse * inverse * mean), dgain


def per_head(values, size):
    left = lanes(values.shape) < size
    first = jnp.sum(jnp.where(left, values, 0.0), axis=-1, keepdims=True)
    second = jnp.sum(jnp.where(left, 0.0, values), axis=-1, keepdims=True)
    return jnp.where(left, first, second)


def head_rms(values, size):
    return lax.rsqrt(per_head(values * values, size) * (1.0 / size) + EPS)


def swap_halves(values, size):
    half = size // 2
    width = values.shape[-1]
    first = lanes(values.shape) % size < half
    return jnp.where(first, pltpu.roll(values, width - half, 1), pltpu.roll(values, half, 1))


def turn(cos_ref, sin_ref, r):
    cos, sin = cos_ref[r], sin_ref[r]
    return (
        jnp.concatenate([cos, cos, cos, cos], axis=0).T,
        jnp.concatenate([-sin, sin, -sin, sin], axis=0).T,
    )


def head_forward(raw, gain_vec, cos, sin, size):
    values = raw * head_rms(raw, size) * gain_vec
    return values * cos + swap_halves(values, size) * sin


def head_back(raw, gain_vec, cos, sin, size, grad):
    grad = grad * cos - swap_halves(grad, size) * sin
    inverse = head_rms(raw, size)
    shaped = grad * gain_vec
    mean = per_head(raw * shaped, size) * (1.0 / size)
    dgain = jnp.sum(grad * raw * inverse, axis=0, keepdims=True)
    return inverse * shaped - raw * (inverse * inverse * inverse * mean), dgain


def start_kernel(
    x_ref, q_ref, k_ref, v_ref, g1_ref, g2_ref, gu_ref, wo_ref,
    xp_ref, wq_ref, gain_ref, gus_ref, wos_ref,
    ss, rs, w_ref, g_ref, gs_ref,
):
    place = y, c, z, x = here()
    me = rank(y, c, x)
    head = y * CORES + c
    mail = Mail((ss, rs))
    peers, line = plane_peers(place), line_peers(place)
    plane, w_rows, cols = w_ref.shape
    q_cols = q_ref.shape[1] // plane
    k_cols = k_ref.shape[1] // plane
    g_ref[...] = jnp.zeros_like(g_ref)
    g_ref[0:1, :w_rows] = g1_ref[...]
    g_ref[1:2, :w_rows] = g2_ref[...]
    keys, values = k_ref[...].astype(F32), v_ref[...].astype(F32)
    for p in range(plane):
        at = slice(p * k_cols, (p + 1) * k_cols)
        pair = jnp.concatenate([keys[:, at], values[:, at]], axis=1)
        w_ref[p, :, :q_cols] = q_ref[:, p * q_cols : (p + 1) * q_cols]
        w_ref[p, :, q_cols:] = pair.astype(BF16)
    greet([p[0] for p in peers] + blk_peers(place))
    w_base, g_base = mail.take(7), mail.take(7)
    zw_base, zg_base = mail.take(len(line)), mail.take(len(line))
    for slot, (dev, other, _) in enumerate(peers):
        mail.send(g_base + slot, g_ref, gs_ref.at[z, me], dev)
        mail.send(w_base + slot, w_ref.at[other], wq_ref.at[head, z, x], dev)
    gs_ref[z, me] = g_ref[...]
    wq_ref[head, z, x] = w_ref[me]
    rows = PlaneGather(mail, place, x_ref, xp_ref)
    swap = PlaneSwap(mail, place, gu_ref, gus_ref)
    block = RowsOut(mail, place, wo_ref, wos_ref)
    rows.begin()
    for slot, (dev, other, (oh, ox)) in enumerate(peers):
        mail.arrive(g_base + slot, gs_ref.at[z, other], dev)
        mail.arrive(w_base + slot, wq_ref.at[oh, z, ox], dev)
    for slot, (dev, _, _) in enumerate(line):
        mail.send(zg_base + slot, gs_ref.at[z], gs_ref.at[z], dev)
        mail.send(zw_base + slot, wq_ref.at[:, z], wq_ref.at[:, z], dev)
    block.begin()
    rows.middle()
    swap.begin()
    rows.end()
    for slot, (dev, _, back) in enumerate(line):
        mail.arrive(zg_base + slot, gs_ref.at[back], dev)
        mail.arrive(zw_base + slot, wq_ref.at[:, back], dev)
    heads, outer = wq_ref.shape[:2]
    gain_ref[...] = jnp.zeros_like(gain_ref)
    for row in range(2):
        gain_ref[row : row + 1] = jnp.concatenate(
            [
                gs_ref[oz, oh * INNER + ox].astype(F32)[row : row + 1, :w_rows]
                for oh in range(heads)
                for oz in range(outer)
                for ox in range(INNER)
            ],
            axis=1,
        )
    block.end()
    swap.end()
    mail.close()


def line_kernel(
    x_ref, w_ref, gain_ref, qk_ref, cos_ref, sin_ref, og_ref,
    q_ref, kvs_ref, raw_ref, norm_ref, ogs_ref,
    ss, rs, kv_ref,
):
    place = y, c, z, x = here()
    mail = Mail((ss, rs))
    line = line_peers(place)
    greet([p[0] for p in line] + list(near(place)))
    rows = PlaneGather(mail, place, og_ref, ogs_ref)
    base = mail.take(2 * len(line))
    rows.begin()
    count, tok, _ = x_ref.shape
    q_cols = q_ref.shape[2]
    size = q_cols // 2
    gain_one = gain_ref[0:1]
    gain_q, gain_k = qk_ref[0:1], qk_ref[1:2]

    def one_block(r, carry):
        block = x_ref[r].astype(F32)
        normed = (block * rms_of(block) * gain_one).astype(BF16)
        norm_ref[r] = normed
        raw = jnp.dot(normed, w_ref[...], preferred_element_type=F32)
        raw_ref[r] = raw
        cos, sin = turn(cos_ref, sin_ref, r)
        q_ref[r] = head_forward(raw[:, :q_cols], gain_q, cos, sin, size).astype(BF16)
        pair = raw[:, q_cols:]
        turned = head_forward(pair, gain_k, cos, sin, size)
        kv_ref[r] = jnp.where(lanes(pair.shape) < size, turned, pair).astype(BF16)
        return carry

    half = count // 2
    for part in range(2):
        lax.fori_loop(part * half, (part + 1) * half, one_block, 0)
        at = pl.ds(part * half, half)
        for slot, (dev, _, _) in enumerate(line):
            mail.send(base + 2 * slot + part, kv_ref.at[at], kvs_ref.at[z, at], dev)
    kvs_ref[z] = kv_ref[...]
    rows.middle()
    rows.end()
    for part in range(2):
        at = pl.ds(part * half, half)
        for slot, (dev, _, back) in enumerate(line):
            mail.arrive(base + 2 * slot + part, kvs_ref.at[back, at], dev)
    mail.close()


def mix_kernel(
    att_ref, wo_ref, x_ref, gain_ref, wd_ref,
    mid_ref, n2_ref, wds_ref,
    ss, rs, parts, own, *bufs,
):
    place = here()
    mail = Mail((ss, rs))
    greet([p[0] for p in line_peers(place)] + list(near(place)))
    down = LineGather(mail, place, wd_ref, wds_ref)

    def make(block):
        parts[block] = jnp.dot(
            att_ref[block], wo_ref[...], preferred_element_type=F32
        ).astype(BF16)

    summed = PlaneScatter(mail, place, parts, mid_ref, bufs, make)
    rows = PlaneGather(mail, place, own, n2_ref)
    summed.begin()
    down.begin()
    summed.middle()
    summed.end()
    middle = x_ref[...].astype(F32) + mid_ref[...]
    mid_ref[...] = middle
    own[...] = (middle * rms_of(middle) * gain_ref[1:2]).astype(BF16)
    rows.begin()
    rows.middle()
    rows.end()
    down.end()
    mail.close()


def narrow_kernel(
    parts_ref, mid_ref, og_ref, gain_ref,
    dmid_ref, dmids_ref, g2_ref,
    ss, rs, own, *bufs,
):
    place = here()
    mail = Mail((ss, rs))
    greet(list(near(place)))
    summed = PlaneScatter(mail, place, parts_ref, dmid_ref, bufs)
    rows = PlaneGather(mail, place, own, dmids_ref)
    summed.begin()
    summed.middle()
    summed.end()
    back, dgain = rms_back(mid_ref[...], gain_ref[1:2], dmid_ref[...])
    dmiddle = og_ref[...].astype(F32) + back
    dmid_ref[...] = dmiddle
    own[...] = dmiddle.astype(BF16)
    g2_ref[...] = dgain
    rows.begin()
    rows.middle()
    rows.end()
    mail.close()


def back_kernel(
    dkv_ref, parts_ref, op_ref, mid_ref,
    kv_ref, out_ref, ops_ref,
    ss, rs, acc, got, op_got, *bufs,
):
    place = here()
    mail = Mail((ss, rs))
    greet(blk_peers(place) + list(near(place)))
    line = LineScatter(mail, place, dkv_ref, got)
    rows = PlaneScatter(mail, place, parts_ref, acc, bufs)
    block = RowsBack(mail, place, op_ref, op_got, ops_ref)
    line.begin()
    rows.begin()
    block.begin()
    rows.middle()
    rows.end()
    out_ref[...] = (mid_ref[...] + acc[...]).astype(BF16)
    kv_ref[...] = line.end().astype(BF16)
    block.end()
    mail.close()


def last_kernel(
    dq_ref, dkv_ref, raw_ref, norm_ref, w_ref, qk_ref, cos_ref, sin_ref,
    x_ref, dmid_ref, gain_ref, g2_ref, dg_ref, *refs,
):
    outer = lax.axis_size("blk") // INNER
    gu_refs, refs = refs[:outer], refs[outer:]
    (in_ref, ws_ref, gus_ref, down_ref, small_ref,
     ss, rs, dqkv, parts, acc, grads, got, held, gu_own, dg_got, small, p_got, z_got, *bufs) = refs
    place = y, c, z, x = here()
    me = rank(y, c, x)
    mail = Mail((ss, rs))
    peers, line = plane_peers(place), line_peers(place)
    greet([p[0] for p in line] + [p[0] for p in peers])
    swap = PlaneSwap(mail, place, gu_own, gus_ref)
    weights = LineScatter(mail, place, grads, got)
    down = LineScatter(mail, place, dg_ref, dg_got)
    total = gu_refs[0][...].astype(F32)
    for ref in gu_refs[1:]:
        total = total + ref[...].astype(F32)
    gu_own[...] = total.astype(BF16).reshape(gu_own.shape)
    swap.begin()

    count, tok, q_cols = dq_ref.shape
    size = q_cols // 2
    gain_q, gain_k = qk_ref[0:1], qk_ref[1:2]

    def one_block(r, sums):
        cos, sin = turn(cos_ref, sin_ref, r)
        raw_q, raw_k = raw_ref[r, :, :q_cols], raw_ref[r, :, q_cols:]
        dq, q_sum = head_back(raw_q, gain_q, cos, sin, size, dq_ref[r].astype(F32))
        dkv = dkv_ref[r].astype(F32)
        dk, k_sum = head_back(raw_k, gain_k, cos, sin, size, dkv)
        dqkv[r, :, :q_cols] = dq.astype(BF16)
        dqkv[r, :, q_cols:] = jnp.where(lanes(dk.shape) < size, dk, dkv).astype(BF16)
        return sums[0] + q_sum, sums[1] + k_sum

    zero = jnp.zeros((1, q_cols), F32)
    q_sum, k_sum = lax.fori_loop(0, count, one_block, (zero, zero))

    width = norm_ref.shape[2]
    flat = dqkv[...].reshape(count * tok, -1)
    w_grad = lax.dot_general(
        norm_ref[...].reshape(count * tok, width),
        flat,
        (((0,), (0,)), ((), ())),
        preferred_element_type=F32,
    ).astype(BF16)
    heads, w_rows = grads.shape[1], grads.shape[3]
    stride = INNER * w_rows
    for oz in range(outer):
        for oh in range(heads):
            first = (oh * outer + oz) * stride
            grads[oz, oh] = w_grad[first : first + stride].reshape(INNER, w_rows, -1)
    weights.begin()

    def make(block):
        parts[block] = lax.dot_general(
            dqkv[block], w_ref[...], NT, preferred_element_type=F32
        ).astype(BF16)

    rows = PlaneScatter(mail, place, parts, acc, bufs, make)
    rows.begin()
    rows.middle()
    down.begin()
    rows.end()
    back, dgain = rms_back(x_ref[...].astype(F32), gain_ref[0:1], acc[...])
    in_ref[...] = (dmid_ref[...] + back).astype(BF16)
    small[...] = jnp.zeros_like(small)
    small[0:1] = dgain
    small[1:2] = g2_ref[...]
    small[2:3, :q_cols] = q_sum
    small[3:4, :q_cols] = k_sum
    p_base, z_base, w_base = mail.take(7), mail.take(len(line)), mail.take(7)
    for slot, (dev, other, _) in enumerate(peers):
        mail.send(p_base + slot, small, p_got.at[me], dev)
    p_got[me] = small[...]
    held[...] = weights.end().reshape(held.shape)
    for slot, (dev, other, _) in enumerate(peers):
        mail.send(w_base + slot, held.at[other], ws_ref.at[me], dev)
    ws_ref[me] = held[me]
    for slot, (dev, other, _) in enumerate(peers):
        mail.arrive(p_base + slot, p_got.at[other], dev)
    z_got[z] = jnp.sum(p_got[...], axis=0)
    for slot, (dev, _, _) in enumerate(line):
        mail.send(z_base + slot, z_got.at[z], z_got.at[z], dev)
    swap.end()
    down_ref[...] = down.end()
    for slot, (dev, other, _) in enumerate(peers):
        mail.arrive(w_base + slot, ws_ref.at[other], dev)
    for slot, (dev, _, back) in enumerate(line):
        mail.arrive(z_base + slot, z_got.at[back], dev)
    small_ref[...] = jnp.sum(z_got[...], axis=0)
    mail.close()


def finish_kernel(own_ref, ws_ref, gus_ref, small_ref, *refs):
    n1_ref, n2_ref, q_ref, k_ref, v_ref, qk_ref, gate_ref, up_ref = refs[-8:]
    passed = refs[:-8]
    for src, dst in zip(passed[: len(passed) // 2], passed[len(passed) // 2 :]):
        dst[...] = src[...]
    plane, w_rows, _ = ws_ref.shape
    q_cols = q_ref.shape[1] // plane
    k_cols = q_cols // 2
    for p in range(0, plane, 2):
        one, two = ws_ref[p], ws_ref[p + 1]
        q_ref[:, p * q_cols : (p + 1) * q_cols] = one[:, :q_cols]
        q_ref[:, (p + 1) * q_cols : (p + 2) * q_cols] = two[:, :q_cols]
        at = slice(p * k_cols, (p + 2) * k_cols)
        left = lanes((w_rows, q_cols)) < k_cols
        one, two = one[:, q_cols:], two[:, q_cols:]
        k_ref[:, at] = jnp.where(left, one, pltpu.roll(two, k_cols, 1))
        v_ref[:, at] = jnp.where(left, pltpu.roll(one, k_cols, 1), two)
    width = small_ref.shape[1]
    move = lax.rem(width - own_ref[0], width)
    totals = pltpu.roll(small_ref[...], move, 1)
    n1_ref[...] = totals[0:1, :w_rows]
    n2_ref[...] = totals[1:2, :w_rows]
    sums = small_ref[...]
    query = sums[2:3, :k_cols] + sums[2:3, k_cols : 2 * k_cols]
    qk_ref[...] = jnp.concatenate([query, sums[3:4, :k_cols]], axis=0)
    outer = lax.axis_size("blk") // INNER
    heads = plane // INNER
    ff = gus_ref.shape[2] // 2
    main = ff // LANES * LANES
    tail = ff - main
    f_rows = ff // outer
    for col, out in ((0, gate_ref), (1, up_ref)):
        for oh in range(heads):
            cols = []
            for ox in range(INNER):
                block = gus_ref[oh * INNER + ox].astype(F32)
                rest = 2 * main + col * tail
                cols.append(
                    jnp.concatenate(
                        [block[:, col * main : (col + 1) * main], block[:, rest : rest + tail]],
                        axis=1,
                    )
                )
            span = INNER * ff
            out[:, oh * span : (oh + 1) * span] = jnp.concatenate(
                [
                    cols[ox][:, oz * f_rows : (oz + 1) * f_rows]
                    for oz in range(outer)
                    for ox in range(INNER)
                ],
                axis=1,
            )


def feed_kernel(z_ref, n2_ref, og_ref, wd_ref, *refs):
    outer = lax.axis_size("blk") // INNER
    pieces, refs = refs[:outer], refs[outer:]
    out_ref, dn_ref, dg_ref = refs[:3]
    chunks = refs[3 : 3 + outer]
    wgu, hid, dgu, gg = refs[3 + outer :]
    z = z_ref[0]
    heads, stride, _ = pieces[0].shape
    ff = wd_ref.shape[0]
    main = ff // LANES * LANES
    tail = ff - main
    for k, piece in enumerate(pieces):
        oz = lax.rem(z + outer - k, outer)
        for oh in range(heads):
            at = pl.multiple_of((oh * outer + oz) * stride, stride)
            wgu[pl.ds(at, stride)] = piece[oh]
    plane, rows, width = n2_ref.shape

    def both(gate, up, dhid):
        sig = 1.0 / (1.0 + jnp.exp(-gate))
        act = gate * sig
        return act * up, dhid * up * (sig * (1.0 + gate * (1.0 - sig))), dhid * act

    def one_block(b, carry):
        pair = pl.ds(2 * b, 2)
        at = pl.ds(pl.multiple_of(b * 2 * rows, 2 * rows), 2 * rows)
        block = n2_ref[pair].reshape(2 * rows, width)
        grad = og_ref[pair].reshape(2 * rows, width)
        gu = jnp.dot(block, wgu[...], preferred_element_type=F32)
        dhid = lax.dot_general(grad, wd_ref[...], NT, preferred_element_type=F32)
        h, dgate, dup = both(gu[:, :main], gu[:, main : 2 * main], dhid[:, :main])
        hid[at, :main] = h.astype(BF16)
        dgu[at, :main] = dgate.astype(BF16)
        dgu[at, main : 2 * main] = dup.astype(BF16)
        ends = gu[:, 2 * main :]
        left = lanes(ends.shape) < tail
        other = pltpu.roll(ends, tail, 1)
        dend = dhid[:, main:]
        dend = jnp.concatenate([dend, dend], axis=1)
        h, dgate, dup = both(jnp.where(left, ends, other), jnp.where(left, other, ends), dend)
        hid[at, main:] = h[:, :tail].astype(BF16)
        dgu[at, 2 * main :] = jnp.where(left, dgate, dup).astype(BF16)
        down = jnp.dot(hid[at], wd_ref[...], preferred_element_type=F32)
        out_ref[pair] = down.astype(BF16).reshape(2, rows, width)
        narrow = lax.dot_general(dgu[at], wgu[...], NT, preferred_element_type=F32)
        dn_ref[pair] = narrow.astype(BF16).reshape(2, rows, width)
        return carry

    lax.fori_loop(0, plane // 2, one_block, 0)
    n2_width = width // heads
    w_rows = stride // INNER

    def one_head(oh, carry):
        cols = pl.ds(pl.multiple_of(oh * n2_width, n2_width), n2_width)
        grad = lax.dot_general(
            n2_ref[:, :, cols].reshape(plane * rows, n2_width),
            dgu[...],
            TN,
            preferred_element_type=F32,
        )
        for oz in range(outer):
            for ox in range(INNER):
                first = oz * stride + ox * w_rows
                gg[oz, oh * INNER + ox] = grad[first : first + w_rows].astype(BF16)
        return carry

    lax.fori_loop(0, heads, one_head, 0)
    for k, chunk in enumerate(chunks):
        chunk[...] = gg[lax.rem(z + k, outer)]
    grads = og_ref[...].reshape(plane * rows, width)
    f_rows = ff // outer
    down = lax.dot_general(hid[...], grads, TN, preferred_element_type=F32)
    for oz in range(outer):
        dg_ref[oz] = down[oz * f_rows : (oz + 1) * f_rows].astype(BF16)


SPANS = 4
LOG2E = math.log2(math.e)


def stack_left(block, size):
    wide = block.astype(F32)
    left = lanes(wide.shape) < size
    first = jnp.where(left, wide, 0.0)
    second = jnp.where(left, pltpu.roll(wide, size, 1), 0.0)
    return jnp.concatenate([first, second], axis=0).astype(BF16)


def stack_right(block, size):
    wide = block.astype(F32)
    right = lanes(wide.shape) >= size
    first = jnp.where(right, pltpu.roll(wide, size, 1), 0.0)
    second = jnp.where(right, wide, 0.0)
    return jnp.concatenate([first, second], axis=0).astype(BF16)


def forward_kernel(own_ref, at_ref, q_ref, kv_ref, out_ref, lse_ref, keys, ones):
    count, rows, size2 = q_ref.shape
    size = size2 // 2
    scale = float(size) ** (-0.5) * LOG2E
    step = SPANS * rows

    def place_rows(p, carry):
        block = kv_ref[at_ref[p]]
        keys[pl.ds(p * rows, rows)] = block
        ones[pl.ds(p * rows, rows)] = jnp.where(lanes(block.shape) < size, 1.0, block).astype(BF16)
        return carry

    lax.fori_loop(0, kv_ref.shape[0], place_rows, 0)

    def one_block(r, carry):
        place = own_ref[r]
        queries = stack_left(q_ref[r], size)

        def weights(c):
            part = keys[pl.ds(c * step, step)]
            scores = lax.dot_general(queries, part, NT, preferred_element_type=F32)
            return jnp.exp2(scores * scale)

        def mix(c, held, total):
            part = ones[pl.ds(c * step, step)]
            return total + jnp.dot(held.astype(BF16), part, preferred_element_type=F32)

        def full(c, total):
            return mix(c, weights(c), total)

        last = place // SPANS
        total = lax.fori_loop(0, last, full, jnp.zeros((2 * rows, size2), F32))
        held = weights(last)
        row = lax.broadcasted_iota(jnp.int32, held.shape, 0)
        row = jnp.where(row >= rows, row - rows, row) + (place - last * SPANS) * rows
        held = jnp.where(lanes(held.shape) <= row, held, 0.0)
        total = mix(last, held, total)
        divided = total / total[:, :1]
        left = lanes((rows, size2)) < size
        out_ref[r] = jnp.where(left, pltpu.roll(divided[:rows], size, 1), divided[rows:]).astype(
            BF16
        )
        lse_ref[r] = jnp.log2(total.T[:8])
        return carry

    lax.fori_loop(0, count, one_block, 0)


def backward_kernel(
    own_ref, at_ref, q_ref, kv_ref, out_ref, do_ref, lse_ref, dq_ref, dkv_ref, keys, turned, sums
):
    count, rows, size2 = q_ref.shape
    size = size2 // 2
    scale = float(size) ** (-0.5)
    step = SPANS * rows
    spans = kv_ref.shape[0]

    def place_rows(p, carry):
        block = kv_ref[at_ref[p]]
        keys[pl.ds(p * rows, rows)] = block
        turned[:, pl.ds(p * rows, rows)] = block.astype(F32).T.astype(BF16)
        return carry

    lax.fori_loop(0, spans, place_rows, 0)
    sums[...] = jnp.zeros_like(sums)

    def one_block(r, carry):
        place = own_ref[r]
        queries = stack_left(q_ref[r], size)
        grads = stack_right(do_ref[r], size)
        both = (do_ref[r].astype(F32) * out_ref[r].astype(F32)).T
        delta = jnp.concatenate(
            [jnp.sum(both[:size], axis=0)[None], jnp.sum(both[size:], axis=0)[None]], axis=1
        )
        lse = lse_ref[r][:1]

        def one_step(c, total, masked):
            at = pl.ds(pl.multiple_of(c * step, step), step)
            part = keys[at]
            scores = lax.dot_general(part, queries, NT, preferred_element_type=F32)
            prob = jnp.exp2(scores * (scale * LOG2E) - lse)
            if masked:
                key = lax.broadcasted_iota(jnp.int32, prob.shape, 0)
                row = lanes(prob.shape)
                row = jnp.where(row >= rows, row - rows, row) + (place - c * SPANS) * rows
                prob = jnp.where(key <= row, prob, 0.0)
            dprob = lax.dot_general(part, grads, NT, preferred_element_type=F32)
            dscore = (prob * (dprob - delta)).astype(BF16)
            sums[at] += jnp.dot(dscore, queries, preferred_element_type=F32) + jnp.dot(
                prob.astype(BF16), grads, preferred_element_type=F32
            )
            return total + jnp.dot(turned[:, at], dscore, preferred_element_type=F32)

        last = place // SPANS
        total = lax.fori_loop(
            0, last, lambda c, t: one_step(c, t, False), jnp.zeros((size2, 2 * rows), F32)
        )
        total = one_step(last, total, True).T * scale
        left = lanes((rows, size2)) < size
        dq_ref[r] = jnp.where(left, total[:rows], pltpu.roll(total[rows:], size, 1)).astype(BF16)
        return carry

    lax.fori_loop(0, count, one_block, 0)

    def give_rows(p, carry):
        block = sums[pl.ds(p * rows, rows)]
        factor = jnp.where(lanes(block.shape) < size, scale, 1.0)
        dkv_ref[at_ref[p]] = (block * factor).astype(BF16)
        return carry

    lax.fori_loop(0, spans, give_rows, 0)


def local_call(body, name, scalars, args, outs, scratch, flops):
    vmem = pl.BlockSpec(memory_space=pltpu.VMEM)
    smem = pl.BlockSpec(memory_space=pltpu.SMEM)
    return pl.pallas_call(
        body,
        name=name,
        out_shape=tuple(jax.ShapeDtypeStruct(shape, dtype) for shape, dtype in outs),
        in_specs=[smem] * len(scalars) + [vmem] * len(args),
        out_specs=tuple([vmem] * len(outs)),
        scratch_shapes=scratch,
        cost_estimate=pl.CostEstimate(flops=flops, bytes_accessed=8 << 20, transcendentals=0),
        compiler_params=pltpu.CompilerParams(vmem_limit_bytes=60 * 1024 * 1024),
    )(*scalars, *args)


def shifts(outer, step):
    return [
        (z * INNER + x, ((z + step) % outer) * INNER + x)
        for z in range(outer)
        for x in range(INNER)
    ]


def local(
    block_input,
    span_order,
    norm1_gain,
    w_query,
    key_weight,
    value_weight,
    qk_gain,
    w_out,
    norm2_gain,
    w_gate,
    w_up,
    w_down,
    out_grad,
):
    heads = lax.axis_size("head")
    blocks = lax.axis_size("blk")
    outer = blocks // INNER
    plane = heads * INNER
    z = lax.axis_index("blk") // INNER
    rows, width = block_input.shape
    size = qk_gain.shape[1]
    w_rows = w_query.shape[0]
    f_rows = w_down.shape[0]
    q_cols = w_query.shape[1] // plane
    a_cols = 2 * q_cols
    ff = f_rows * outer
    spans = outer * plane
    n_line = outer - 1
    stride = INNER * w_rows

    def cut(weight):
        shaped = weight.reshape(w_rows, heads, outer, INNER, f_rows)
        return shaped.transpose(1, 3, 0, 2, 4).reshape(plane, w_rows, ff)

    main = ff // LANES * LANES
    gate8, up8 = cut(w_gate), cut(w_up)
    gu8 = jnp.concatenate(
        [gate8[..., :main], up8[..., :main], gate8[..., main:], up8[..., main:]], axis=-1
    )

    x_all, wqkv, gains, gu_piece, out_mine = call(
        start_kernel,
        "start",
        1,
        [
            ((plane, rows, width), BF16),
            ((heads, outer, INNER, w_rows, a_cols), BF16),
            ((8, width), F32),
            ((plane, w_rows, 2 * ff), BF16),
            ((outer // INNER, INNER, w_rows, width), BF16),
        ],
        (
            block_input,
            w_query,
            key_weight,
            value_weight,
            norm1_gain.reshape(1, w_rows),
            norm2_gain.reshape(1, w_rows),
            gu8,
            w_out,
        ),
        14 + 2 * n_line + PlaneGather.COPIES + PlaneSwap.COPIES + outer,
        [
            pltpu.VMEM((plane, w_rows, a_cols), BF16),
            pltpu.VMEM((16, LANES), BF16),
            pltpu.VMEM((outer, plane, 16, LANES), BF16),
        ],
    )
    wqkv = wqkv.reshape(width, a_cols)
    out_mine = out_mine.reshape(q_cols, width)
    gu_piece = gu_piece.reshape(heads, stride, 2 * ff)
    gu_pieces = [gu_piece] + [
        lax.ppermute(gu_piece, "blk", shifts(outer, step)) for step in range(1, outer)
    ]

    by_place = span_order.reshape(heads, outer, INNER)
    own_spans = lax.dynamic_index_in_dim(by_place, z, 1, keepdims=False).reshape(plane)
    all_spans = by_place.transpose(1, 0, 2).reshape(spans)
    every = jnp.arange(spans, dtype=jnp.int32)
    span_at = jnp.sum(jnp.where(all_spans[:, None] == every[None, :], every[:, None], 0), axis=0)
    where_at = own_spans[:, None] * rows + jnp.arange(rows, dtype=jnp.int32)[None, :]
    half = size // 2
    frequency = jnp.exp(jnp.arange(half, dtype=F32) * F32(-2.0 * math.log(THETA) / size))
    angles = where_at.astype(F32)[:, None, :] * frequency[None, :, None]
    cosine, sine = jnp.cos(angles), jnp.sin(angles)
    ones = jnp.ones((size,), F32)
    qk_rows = jnp.stack(
        [
            jnp.concatenate([qk_gain[0], qk_gain[0]]),
            jnp.concatenate([qk_gain[1], ones]),
        ]
    )

    queries, kv_all, raw, normed, og_all = call(
        line_kernel,
        "line",
        2,
        [
            ((plane, rows, q_cols), BF16),
            ((outer, plane, rows, q_cols), BF16),
            ((plane, rows, a_cols), F32),
            ((plane, rows, width), BF16),
            ((plane, rows, width), BF16),
        ],
        (x_all, wqkv, gains, qk_rows, cosine, sine, out_grad),
        2 * n_line + PlaneGather.COPIES,
        [pltpu.VMEM((plane, rows, q_cols), BF16)],
    )
    kv_blocks = kv_all.reshape(spans, rows, q_cols)
    pairs = plane * rows * spans * rows * q_cols
    attended, log_total = local_call(
        forward_kernel,
        "attend",
        (own_spans, span_at),
        (queries, kv_blocks),
        [((plane, rows, q_cols), BF16), ((plane, 8, 2 * rows), F32)],
        [pltpu.VMEM((spans * rows, q_cols), BF16), pltpu.VMEM((spans * rows, q_cols), BF16)],
        4 * pairs,
    )
    middle, normed2, down_full = call(
        mix_kernel,
        "mix",
        3,
        [((rows, width), F32), ((plane, rows, width), BF16), ((outer, f_rows, width), BF16)],
        (attended, out_mine, block_input, gains, w_down),
        n_line + PlaneScatter.COPIES + PlaneGather.COPIES,
        [pltpu.VMEM((plane, rows, width), BF16), pltpu.VMEM((rows, width), BF16)]
        + PlaneScatter.scratch(rows, width),
    )
    down_full = down_full.reshape(ff, width)

    out_parts, dn_parts, down_grad, *gu_grads = local_call(
        feed_kernel,
        "feed",
        (jnp.reshape(z, (1,)).astype(jnp.int32),),
        (normed2, og_all, down_full, *gu_pieces),
        [
            ((plane, rows, width), BF16),
            ((plane, rows, width), BF16),
            ((outer, f_rows, width), BF16),
        ]
        + [((plane, w_rows, 2 * ff), BF16)] * outer,
        [
            pltpu.VMEM((width, 2 * ff), BF16),
            pltpu.VMEM((plane * rows, ff), BF16),
            pltpu.VMEM((plane * rows, 2 * ff), BF16),
            pltpu.VMEM((outer, plane, w_rows, 2 * ff), BF16),
        ],
        18 * plane * rows * width * ff,
    )
    gu_sums = [gu_grads[0]] + [
        lax.ppermute(gu_grads[step], "blk", shifts(outer, step)) for step in range(1, outer)
    ]
    dmiddle, dmid_all, norm2_grad = call(
        narrow_kernel,
        "narrow",
        4,
        [((rows, width), F32), ((plane, rows, width), BF16), ((1, width), F32)],
        (dn_parts, middle, out_grad, gains),
        PlaneScatter.COPIES + PlaneGather.COPIES,
        [pltpu.VMEM((rows, width), BF16)] + PlaneScatter.scratch(rows, width),
    )

    dmid_rows = dmid_all.reshape(plane * rows, width)
    out_proj = lax.dot_general(
        attended.reshape(plane * rows, q_cols), dmid_rows, TN, preferred_element_type=F32
    )
    dattended = lax.dot_general(dmid_rows, out_mine, NT, preferred_element_type=F32).astype(BF16)
    dqueries, dkv = local_call(
        backward_kernel,
        "attend_back",
        (own_spans, span_at),
        (queries, kv_blocks, attended, dattended.reshape(plane, rows, q_cols), log_total),
        [((plane, rows, q_cols), BF16), ((spans, rows, q_cols), BF16)],
        [
            pltpu.VMEM((spans * rows, q_cols), BF16),
            pltpu.VMEM((q_cols, spans * rows), BF16),
            pltpu.VMEM((spans * rows, q_cols), F32),
        ],
        10 * pairs,
    )
    dkv_own, block_output, out_proj_grad = call(
        back_kernel,
        "back",
        5,
        [((plane, rows, q_cols), BF16), ((rows, width), BF16), ((w_rows, width), F32)],
        (
            dkv.reshape(outer, plane, rows, q_cols),
            out_parts,
            out_proj.astype(BF16).reshape(outer // INNER, INNER, w_rows, width),
            middle,
        ),
        n_line + PlaneScatter.COPIES + outer,
        [
            pltpu.VMEM((rows, width), F32),
            pltpu.VMEM((n_line, plane, rows, q_cols), BF16),
            pltpu.VMEM((outer, w_rows, width), BF16),
        ]
        + PlaneScatter.scratch(rows, width),
    )
    input_grad, w_own, gu_own, down_out, small = call(
        last_kernel,
        "last",
        6,
        [
            ((rows, width), BF16),
            ((plane, w_rows, a_cols), F32),
            ((plane, w_rows, 2 * ff), BF16),
            ((f_rows, width), F32),
            ((8, width), F32),
        ],
        (
            dqueries,
            dkv_own,
            raw,
            normed,
            wqkv,
            qk_rows,
            cosine,
            sine,
            block_input,
            dmiddle,
            gains,
            norm2_grad,
            down_grad,
            *gu_sums,
        ),
        3 * n_line + 14 + PlaneScatter.COPIES + PlaneSwap.COPIES,
        [
            pltpu.VMEM((plane, rows, a_cols), BF16),
            pltpu.VMEM((plane, rows, width), BF16),
            pltpu.VMEM((rows, width), F32),
            pltpu.VMEM((outer, heads, INNER, w_rows, a_cols), BF16),
            pltpu.VMEM((n_line, heads, INNER, w_rows, a_cols), BF16),
            pltpu.VMEM((plane, w_rows, a_cols), F32),
            pltpu.VMEM((plane, w_rows, 2 * ff), BF16),
            pltpu.VMEM((n_line, f_rows, width), BF16),
            pltpu.VMEM((8, width), F32),
            pltpu.VMEM((plane, 8, width), F32),
            pltpu.VMEM((outer, 8, width), F32),
        ]
        + PlaneScatter.scratch(rows, width),
    )
    own = (lax.axis_index("head") * blocks + lax.axis_index("blk")) * w_rows
    outs = local_call(
        finish_kernel,
        "finish",
        (jnp.reshape(own, (1,)).astype(jnp.int32),),
        (w_own, gu_own, small, block_output, input_grad, out_proj_grad, down_out),
        [
            ((rows, width), BF16),
            ((rows, width), BF16),
            ((w_rows, width), F32),
            ((f_rows, width), F32),
            ((1, w_rows), F32),
            ((1, w_rows), F32),
            (w_query.shape, F32),
            (key_weight.shape, F32),
            (value_weight.shape, F32),
            ((2, size), F32),
            (w_gate.shape, F32),
            (w_up.shape, F32),
        ],
        [],
        1 << 20,
    )
    (block_output, input_grad, out_proj_grad, down_grad, norm1_grad, norm2_grad,
     query_grad, key_grad, value_grad, qk_gain_grad, gate_grad, up_grad) = outs
    return (
        block_output,
        input_grad,
        norm1_grad.reshape(w_rows),
        query_grad,
        key_grad,
        value_grad,
        qk_gain_grad,
        out_proj_grad,
        norm2_grad.reshape(w_rows),
        gate_grad,
        up_grad,
        down_grad,
    )


def solution(mesh):
    split = P(("head", "blk"), None)
    line = P(("head", "blk"))
    in_specs = (split, P(), line, split, split, split, P(), split, line, split, split, split, split)
    out_specs = (split, split, line, split, split, split, P(), split, line, split, split, split)
    return jax.shard_map(local, mesh=mesh, in_specs=in_specs, out_specs=out_specs, check_vma=False)
```

```python
import math

import jax
import jax.numpy as jnp
from jax import lax
from jax.experimental import pallas as pl
from jax.experimental.pallas import tpu as pltpu
from jax.sharding import PartitionSpec as P


EPS = 1e-05
THETA = 1000000.0
LANES = 128
CORES = 2
INNER = 2
MESH = pl.DeviceIdType.MESH
F32 = jnp.float32
BF16 = jnp.bfloat16
NT = (((1,), (1,)), ((), ()))
TN = (((0,), (0,)), ((), ()))


def here():
    head = lax.axis_index("head")
    blk = lax.axis_index("blk")
    return head // CORES, head % CORES, blk // INNER, blk % INNER


def device(y, c, z, x):
    return (y * CORES + c, z * INNER + x)


def rank(y, c, x):
    return (y * CORES + c) * INNER + x


def plane_peers(place):
    y, c, z, x = place
    peers = []
    for bits in range(1, 8):
        py = 1 - y if bits & 4 else y
        pc = 1 - c if bits & 2 else c
        px = 1 - x if bits & 1 else x
        peers.append((device(py, pc, z, px), rank(py, pc, px), (py * CORES + pc, px)))
    return peers


def line_peers(place):
    y, c, z, x = place
    outer = lax.axis_size("blk") // INNER
    forth = [lax.rem(z + k, outer) for k in range(1, outer)]
    back = [lax.rem(z + outer - k, outer) for k in range(1, outer)]
    return [(device(y, c, f, x), f, b) for f, b in zip(forth, back)]


def greet(devices):
    barrier = pltpu.get_barrier_semaphore()
    for dev in devices:
        pl.semaphore_signal(barrier, inc=1, device_id=dev, device_id_type=MESH)
    pl.semaphore_wait(barrier, len(devices))


class Mail:
    def __init__(self, sems):
        self.sends, self.recvs = sems
        self.used = 0
        self.open = []

    def take(self, count):
        first = self.used
        self.used += count
        return first

    def copy(self, slot, src, dst, dev, landing=None):
        return pltpu.make_async_remote_copy(
            src_ref=src,
            dst_ref=dst,
            send_sem=self.sends.at[slot],
            recv_sem=self.recvs.at[slot if landing is None else landing],
            device_id=dev,
            device_id_type=MESH,
        )

    def send(self, slot, src, dst, dev, landing=None):
        copy = self.copy(slot, src, dst, dev, landing)
        copy.start()
        self.open.append(copy)

    def arrive(self, slot, dst, dev):
        self.copy(slot, dst, dst, dev).wait_recv()

    def close(self):
        for copy in self.open:
            copy.wait_send()


def near(place):
    y, c, z, x = place
    return device(y, 1 - c, z, x), device(y, c, z, 1 - x), device(1 - y, c, z, x)


class PlaneGather:
    COPIES = 11

    def __init__(self, mail, place, src, out):
        self.mail, self.place, self.src, self.out = mail, place, src, out
        self.base = mail.take(self.COPIES)
        half = src.shape[0] // 2
        self.top, self.bot = pl.ds(0, half), pl.ds(half, half)

    def begin(self):
        y, c, _, x = self.place
        pair, xn, yn = near(self.place)
        me = rank(y, c, x)
        send, base, src, out = self.mail.send, self.base, self.src, self.out
        top, bot = self.top, self.bot
        send(base + 0, src.at[top], out.at[me, top], xn)
        send(base + 1, src.at[bot], out.at[me, bot], yn)
        send(base + 2, src.at[bot], out.at[me, bot], xn)
        send(base + 3, src.at[top], out.at[me, top], yn)
        send(base + 4, src, out.at[me], pair)
        out[me] = src[...]

    def middle(self):
        y, c, _, x = self.place
        pair, xn, yn = near(self.place)
        xr, yr = rank(y, c, 1 - x), rank(1 - y, c, x)
        send, arrive, base, out = self.mail.send, self.mail.arrive, self.base, self.out
        top, bot = self.top, self.bot
        arrive(base + 0, out.at[xr, top], xn)
        send(base + 5, out.at[xr, top], out.at[xr, top], yn)
        arrive(base + 1, out.at[yr, bot], yn)
        send(base + 6, out.at[yr, bot], out.at[yr, bot], xn)
        arrive(base + 2, out.at[xr, bot], xn)
        send(base + 7, out.at[xr], out.at[xr], pair)
        arrive(base + 3, out.at[yr, top], yn)
        send(base + 8, out.at[yr], out.at[yr], pair)

    def end(self):
        y, c, _, x = self.place
        pair, xn, yn = near(self.place)
        dr = rank(1 - y, c, 1 - x)
        send, arrive, base, out = self.mail.send, self.mail.arrive, self.base, self.out
        top, bot = self.top, self.bot
        arrive(base + 5, out.at[dr, top], yn)
        send(base + 9, out.at[dr, top], out.at[dr, top], pair)
        arrive(base + 6, out.at[dr, bot], xn)
        send(base + 10, out.at[dr, bot], out.at[dr, bot], pair)
        arrive(base + 4, out.at[rank(y, 1 - c, x)], pair)
        arrive(base + 7, out.at[rank(y, 1 - c, 1 - x)], pair)
        arrive(base + 8, out.at[rank(1 - y, 1 - c, x)], pair)
        far = rank(1 - y, 1 - c, 1 - x)
        arrive(base + 9, out.at[far, top], pair)
        arrive(base + 10, out.at[far, bot], pair)


class PlaneScatter:
    COPIES = 10

    def __init__(self, mail, place, parts, out, bufs, make=None):
        self.mail, self.place, self.parts, self.out = mail, place, parts, out
        self.make = make or (lambda block: None)
        self.first, self.held, self.via_x, self.via_y, self.last = bufs
        self.base = mail.take(self.COPIES)
        half = out.shape[0] // 2
        self.top, self.bot = pl.ds(0, half), pl.ds(half, half)

    @staticmethod
    def scratch(rows, cols):
        half = rows // 2
        return [
            pltpu.VMEM((2, 2, rows, cols), BF16),
            pltpu.VMEM((2, 2, rows, cols), BF16),
            pltpu.VMEM((2, half, cols), BF16),
            pltpu.VMEM((2, half, cols), BF16),
            pltpu.VMEM((4, half, cols), BF16),
        ]

    def begin(self):
        y, c, _, x = self.place
        pair, _, _ = near(self.place)
        for slot, (py, px) in enumerate(((1 - y, 1 - x), (y, 1 - x), (1 - y, x), (y, x))):
            self.make(rank(py, 1 - c, px))
            self.mail.send(
                self.base + slot,
                self.parts.at[rank(py, 1 - c, px)],
                self.first.at[py, px],
                pair,
            )

    def joined(self, slot, py, px):
        _, c, _, _ = self.place
        pair, _, _ = near(self.place)
        self.make(rank(py, c, px))
        self.mail.arrive(self.base + slot, self.first.at[py, px], pair)
        return self.parts[rank(py, c, px)].astype(F32) + self.first[py, px].astype(F32)

    def middle(self):
        y, _, _, x = self.place
        _, xn, yn = near(self.place)
        send, base, held = self.mail.send, self.base, self.held
        top, bot = self.top, self.bot
        held[1 - y, 1 - x] = self.joined(0, 1 - y, 1 - x).astype(BF16)
        send(base + 4, held.at[1 - y, 1 - x, top], self.via_x.at[1 - y], xn)
        send(base + 5, held.at[1 - y, 1 - x, bot], self.via_y.at[1 - x], yn)
        held[y, 1 - x] = self.joined(1, y, 1 - x).astype(BF16)
        send(base + 6, held.at[y, 1 - x, top], self.via_x.at[y], xn)
        held[1 - y, x] = self.joined(2, 1 - y, x).astype(BF16)
        send(base + 7, held.at[1 - y, x, bot], self.via_y.at[x], yn)
        self.out[...] = self.joined(3, y, x)

    def end(self):
        y, _, _, x = self.place
        _, xn, yn = near(self.place)
        send, arrive, base, held = self.mail.send, self.mail.arrive, self.base, self.held
        top, bot, last, out = self.top, self.bot, self.last, self.out
        arrive(base + 4, self.via_x.at[1 - y], xn)
        last[0] = (held[1 - y, x, top].astype(F32) + self.via_x[1 - y].astype(F32)).astype(BF16)
        send(base + 8, last.at[0], last.at[2], yn)
        arrive(base + 5, self.via_y.at[1 - x], yn)
        last[1] = (held[y, 1 - x, bot].astype(F32) + self.via_y[1 - x].astype(F32)).astype(BF16)
        send(base + 9, last.at[1], last.at[3], xn)
        arrive(base + 6, self.via_x.at[y], xn)
        out[top] = out[top] + self.via_x[y].astype(F32)
        arrive(base + 7, self.via_y.at[x], yn)
        out[bot] = out[bot] + self.via_y[x].astype(F32)
        arrive(base + 8, last.at[2], yn)
        out[top] = out[top] + last[2].astype(F32)
        arrive(base + 9, last.at[3], xn)
        out[bot] = out[bot] + last[3].astype(F32)


class LineScatter:
    def __init__(self, mail, place, parts, got):
        self.mail, self.place, self.parts, self.got = mail, place, parts, got
        self.line = line_peers(place)
        self.base = mail.take(len(self.line))

    def begin(self):
        for slot, (dev, forth, _) in enumerate(self.line):
            self.mail.send(self.base + slot, self.parts.at[forth], self.got.at[slot], dev)

    def end(self):
        total = self.parts[self.place[2]].astype(F32)
        for slot, (dev, _, _) in enumerate(self.line):
            self.mail.arrive(self.base + slot, self.got.at[slot], dev)
            total = total + self.got[slot].astype(F32)
        return total


class PlaneSwap:
    COPIES = 7

    def __init__(self, mail, place, src, out):
        self.mail, self.place, self.src, self.out = mail, place, src, out
        self.base = mail.take(self.COPIES)

    def begin(self):
        y, c, _, x = self.place
        me = rank(y, c, x)
        for slot, (dev, other, _) in enumerate(plane_peers(self.place)):
            self.mail.send(self.base + slot, self.src.at[other], self.out.at[me], dev)
        self.out[me] = self.src[me]

    def end(self):
        for slot, (dev, other, _) in enumerate(plane_peers(self.place)):
            self.mail.arrive(self.base + slot, self.out.at[other], dev)


def blk_peers(place):
    y, c, z, x = place
    outer = lax.axis_size("blk") // INNER
    others = [device(y, c, lax.rem(z + k, outer), 1 - x) for k in range(1, outer)]
    return [p[0] for p in line_peers(place)] + others


class RowsOut:
    def __init__(self, mail, place, src, out):
        self.mail, self.place, self.src, self.out = mail, place, src, out
        self.outer = lax.axis_size("blk") // INNER
        self.per = self.outer // INNER
        self.base = mail.take(self.outer)

    def first(self):
        y, c, z, x = self.place
        return self.mail.copy(
            self.base,
            self.src,
            self.out.at[lax.rem(z, self.per), x],
            device(y, c, z, 1 - x),
            self.base + lax.rem(z, self.per) * INNER + x,
        )

    def begin(self):
        y, c, z, x = self.place
        to = z // self.per
        landing = self.base + lax.rem(z, self.per) * INNER + x
        place_there = self.out.at[lax.rem(z, self.per), x]

        @pl.when(to != x)
        def _():
            self.first().start()

        @pl.when(to == x)
        def _():
            self.out[lax.rem(z, self.per), x] = self.src[...]

        for k in range(1, self.outer):
            dev = device(y, c, lax.rem(z + k, self.outer), to)
            self.mail.send(self.base + k, self.src, place_there, dev, landing)

    def end(self):
        y, c, z, x = self.place

        @pl.when(z // self.per != x)
        def _():
            self.first().wait_send()

        for j in range(self.per):
            for ox in range(INNER):
                oz = x * self.per + j
                own = (oz == z) & (x * 0 + ox == x)

                @pl.when(jnp.logical_not(own))
                def _():
                    self.mail.arrive(
                        self.base + j * INNER + ox, self.out.at[j, ox], device(y, c, oz, ox)
                    )


class RowsBack:
    def __init__(self, mail, place, parts, got, out):
        self.mail, self.place, self.parts, self.got, self.out = mail, place, parts, got, out
        self.outer = lax.axis_size("blk") // INNER
        self.per = self.outer // INNER
        self.base = mail.take(self.outer)

    def copies(self):
        y, c, z, x = self.place
        for j in range(self.per):
            for ox in range(INNER):
                oz = x * self.per + j
                own = (oz == z) & (x * 0 + ox == x)
                copy = self.mail.copy(
                    self.base + j * INNER + ox,
                    self.parts.at[j, ox],
                    self.got.at[z],
                    device(y, c, oz, ox),
                    self.base + z,
                )
                yield j, ox, own, copy

    def begin(self):
        _, _, z, _ = self.place
        for j, ox, own, copy in self.copies():

            @pl.when(own)
            def _():
                self.got[z] = self.parts[j, ox]

            @pl.when(jnp.logical_not(own))
            def _():
                copy.start()

    def end(self):
        y, c, z, x = self.place
        for j, ox, own, copy in self.copies():

            @pl.when(jnp.logical_not(own))
            def _():
                copy.wait_send()

        to = z // self.per
        for oz in range(self.outer):

            @pl.when(jnp.logical_not((z == oz) & (to == x)))
            def _():
                self.mail.arrive(self.base + oz, self.got.at[oz], device(y, c, z * 0 + oz, to))

        total = self.got[0].astype(F32)
        for oz in range(1, self.outer):
            total = total + self.got[oz].astype(F32)
        self.out[...] = total


def call(body, ident, outs, args, copies, scratch=()):
    spec = pl.BlockSpec(memory_space=pltpu.VMEM)
    return remote_call(body, ident, outs, args, copies, scratch, spec)


def remote_call(body, ident, outs, args, copies, scratch, spec):
    return pl.pallas_call(
        body,
        out_shape=tuple(jax.ShapeDtypeStruct(shape, dtype) for shape, dtype in outs),
        in_specs=[spec] * len(args),
        out_specs=tuple([spec] * len(outs)),
        scratch_shapes=[
            pltpu.SemaphoreType.DMA((copies,)),
            pltpu.SemaphoreType.DMA((copies,)),
            *scratch,
        ],
        compiler_params=pltpu.CompilerParams(
            collective_id=ident, has_side_effects=True, vmem_limit_bytes=60 * 1024 * 1024
        ),
    )(*args)


def lanes(shape):
    return lax.broadcasted_iota(jnp.int32, shape, len(shape) - 1)


def rms_of(values):
    return lax.rsqrt(jnp.mean(values * values, axis=-1, keepdims=True) + EPS)


def rms_back(values, gain_vec, grad):
    inverse = rms_of(values)
    shaped = grad * gain_vec
    mean = jnp.mean(values * shaped, axis=-1, keepdims=True)
    dgain = jnp.sum(grad * values * inverse, axis=0, keepdims=True)
    return inverse * shaped - values * (inverse * inverse * inverse * mean), dgain


def per_head(values, size):
    left = lanes(values.shape) < size
    first = jnp.sum(jnp.where(left, values, 0.0), axis=-1, keepdims=True)
    second = jnp.sum(jnp.where(left, 0.0, values), axis=-1, keepdims=True)
    return jnp.where(left, first, second)


def head_rms(values, size):
    return lax.rsqrt(per_head(values * values, size) * (1.0 / size) + EPS)


def swap_halves(values, size):
    half = size // 2
    width = values.shape[-1]
    first = lanes(values.shape) % size < half
    return jnp.where(first, pltpu.roll(values, width - half, 1), pltpu.roll(values, half, 1))


def turn(cos_ref, sin_ref, r):
    cos, sin = cos_ref[r], sin_ref[r]
    return (
        jnp.concatenate([cos, cos, cos, cos], axis=0).T,
        jnp.concatenate([-sin, sin, -sin, sin], axis=0).T,
    )


def head_forward(raw, gain_vec, cos, sin, size):
    values = raw * head_rms(raw, size) * gain_vec
    return values * cos + swap_halves(values, size) * sin


def head_back(raw, gain_vec, cos, sin, size, grad):
    grad = grad * cos - swap_halves(grad, size) * sin
    inverse = head_rms(raw, size)
    shaped = grad * gain_vec
    mean = per_head(raw * shaped, size) * (1.0 / size)
    dgain = jnp.sum(grad * raw * inverse, axis=0, keepdims=True)
    return inverse * shaped - raw * (inverse * inverse * inverse * mean), dgain


def all_peers(place):
    y, c, z, x = place
    outer = lax.axis_size("blk") // INNER
    peers = []
    for k in range(outer):
        forth, back = lax.rem(z + k, outer), lax.rem(z + outer - k, outer)
        for bits in range(0 if k else 1, 8):
            py = 1 - y if bits & 4 else y
            pc = 1 - c if bits & 2 else c
            px = 1 - x if bits & 1 else x
            peers.append((device(py, pc, forth, px), device(py, pc, back, px), py, pc, back, px))
    return peers


def start_kernel(
    x_ref, q_ref, k_ref, v_ref, g1_ref, g2_ref, gate_ref, up_ref, wo_ref,
    xp_ref, wq_ref, gain_ref, gu_ref, wos_ref,
    ss, rs, w_ref, g_ref, gs_ref,
):
    place = y, c, z, x = here()
    me = rank(y, c, x)
    head = y * CORES + c
    mail = Mail((ss, rs))
    peers = all_peers(place)
    plane, w_rows, _ = w_ref.shape
    heads, outer = wq_ref.shape[:2]
    q_cols = q_ref.shape[1] // plane
    k_cols = k_ref.shape[1] // plane
    g_ref[...] = jnp.zeros_like(g_ref)
    g_ref[0:1, :w_rows] = g1_ref[...].astype(F32)
    g_ref[0:1, LANES // 2 : LANES // 2 + w_rows] = g2_ref[...].astype(F32)
    keys, values = k_ref[...].astype(F32), v_ref[...].astype(F32)
    for p in range(plane):
        at = slice(p * k_cols, (p + 1) * k_cols)
        pair = jnp.concatenate([keys[:, at], values[:, at]], axis=1)
        w_ref[p, :, :q_cols] = q_ref[:, p * q_cols : (p + 1) * q_cols]
        w_ref[p, :, q_cols:] = pair.astype(BF16)
    greet([p[0] for p in peers])
    w_base, g_base = mail.take(len(peers)), mail.take(len(peers))
    rows = PlaneGather(mail, place, x_ref, xp_ref)
    block = RowsOut(mail, place, wo_ref, wos_ref)
    for slot, (dev, _, py, pc, _, px) in reversed(list(enumerate(peers))):
        mail.send(g_base + slot, g_ref, gs_ref.at[z, me], dev)
        mail.send(w_base + slot, w_ref.at[rank(py, pc, px)], wq_ref.at[head, z, x], dev)
    rows.begin()
    gs_ref[z, me] = g_ref[...]
    wq_ref[head, z, x] = w_ref[me]
    block.begin()
    f_cols = gate_ref.shape[1] // (heads * outer * INNER)
    main = outer * f_cols // LANES * LANES
    for oh in range(heads):
        span = outer * INNER * f_cols
        cut = []
        for ref in (gate_ref, up_ref):
            wide = ref[:, oh * span : (oh + 1) * span].astype(F32)
            cut.append(
                [
                    jnp.concatenate(
                        [
                            wide[:, (oz * INNER + ox) * f_cols : (oz * INNER + ox + 1) * f_cols]
                            for oz in range(outer)
                        ],
                        axis=1,
                    )
                    for ox in range(INNER)
                ]
            )
        for ox in range(INNER):
            gate, up = cut[0][ox], cut[1][ox]
            p = oh * INNER + ox
            gu_ref[p, :, :main] = gate[:, :main].astype(BF16)
            gu_ref[p, :, main : 2 * main] = up[:, :main].astype(BF16)
            tails = jnp.concatenate([gate[:, main:], up[:, main:]], axis=1)
            gu_ref[p, :, 2 * main :] = tails.astype(BF16)
    rows.middle()
    rows.end()
    for slot, (_, dev, py, pc, oz, px) in enumerate(peers):
        mail.arrive(g_base + slot, gs_ref.at[oz, rank(py, pc, px)], dev)
    gain_ref[...] = jnp.zeros_like(gain_ref)
    for row in range(2):
        first = row * LANES // 2
        gain_ref[row : row + 1] = jnp.concatenate(
            [
                gs_ref[oz, oh * INNER + ox][:, first : first + w_rows]
                for oh in range(heads)
                for oz in range(outer)
                for ox in range(INNER)
            ],
            axis=1,
        )
    for slot, (_, dev, py, pc, oz, px) in enumerate(peers):
        mail.arrive(w_base + slot, wq_ref.at[py * CORES + pc, oz, px], dev)
    block.end()
    mail.close()


def line_kernel(
    x_ref, w_ref, gain_ref, qk_ref, cos_ref, sin_ref, og_ref, gu_ref,
    q_ref, kvs_ref, raw_ref, norm_ref, ogs_ref, gus_ref,
    ss, rs, kv_ref,
):
    place = y, c, z, x = here()
    mail = Mail((ss, rs))
    line = line_peers(place)
    greet([p[0] for p in line] + [p[0] for p in plane_peers(place)])
    rows = PlaneGather(mail, place, og_ref, ogs_ref)
    swap = PlaneSwap(mail, place, gu_ref, gus_ref)
    base = mail.take(2 * len(line))
    rows.begin()
    count, _, _ = x_ref.shape
    q_cols = q_ref.shape[2]
    size = q_cols // 2
    gain_one = gain_ref[0:1]
    gain_q, gain_k = qk_ref[0:1], qk_ref[1:2]

    def one_block(r, carry):
        block = x_ref[r].astype(F32)
        normed = (block * rms_of(block) * gain_one).astype(BF16)
        norm_ref[r] = normed
        raw = jnp.dot(normed, w_ref[...], preferred_element_type=F32)
        raw_ref[r] = raw
        cos, sin = turn(cos_ref, sin_ref, r)
        q_ref[r] = head_forward(raw[:, :q_cols], gain_q, cos, sin, size).astype(BF16)
        pair = raw[:, q_cols:]
        turned = head_forward(pair, gain_k, cos, sin, size)
        kv_ref[r] = jnp.where(lanes(pair.shape) < size, turned, pair).astype(BF16)
        return carry

    half = count // 2
    for part in range(2):
        lax.fori_loop(part * half, (part + 1) * half, one_block, 0)
        at = pl.ds(part * half, half)
        for slot, (dev, _, _) in enumerate(line):
            mail.send(base + 2 * slot + part, kv_ref.at[at], kvs_ref.at[z, at], dev)
    kvs_ref[z] = kv_ref[...]
    rows.middle()
    swap.begin()
    rows.end()
    swap.end()
    for part in range(2):
        at = pl.ds(part * half, half)
        for slot, (dev, _, back) in enumerate(line):
            mail.arrive(base + 2 * slot + part, kvs_ref.at[back, at], dev)
    mail.close()


def mix_kernel(
    att_ref, wo_ref, x_ref, gain_ref,
    mid_ref, n2_ref,
    ss, rs, parts, own, *bufs,
):
    place = here()
    mail = Mail((ss, rs))
    greet(list(near(place)))

    def make(block):
        parts[block] = jnp.dot(
            att_ref[block], wo_ref[...], preferred_element_type=F32
        ).astype(BF16)

    summed = PlaneScatter(mail, place, parts, mid_ref, bufs, make)
    rows = PlaneGather(mail, place, own, n2_ref)
    summed.begin()
    summed.middle()
    summed.end()
    middle = x_ref[...].astype(F32) + mid_ref[...]
    mid_ref[...] = middle
    own[...] = (middle * rms_of(middle) * gain_ref[1:2]).astype(BF16)
    rows.begin()
    rows.middle()
    rows.end()
    mail.close()


def narrow_kernel(
    parts_ref, mid_ref, og_ref, gain_ref,
    dmid_ref, dmids_ref, g2_ref,
    ss, rs, own, *bufs,
):
    place = here()
    mail = Mail((ss, rs))
    greet(list(near(place)))
    summed = PlaneScatter(mail, place, parts_ref, dmid_ref, bufs)
    rows = PlaneGather(mail, place, own, dmids_ref)
    summed.begin()
    summed.middle()
    summed.end()
    back, dgain = rms_back(mid_ref[...], gain_ref[1:2], dmid_ref[...])
    dmiddle = og_ref[...].astype(F32) + back
    dmid_ref[...] = dmiddle
    own[...] = dmiddle.astype(BF16)
    g2_ref[...] = dgain
    rows.begin()
    rows.middle()
    rows.end()
    mail.close()


def back_kernel(
    dkv_ref, parts_ref, op_ref, mid_ref,
    kv_ref, out_ref, ops_ref,
    ss, rs, acc, got, op_got, *bufs,
):
    place = here()
    mail = Mail((ss, rs))
    greet(blk_peers(place) + list(near(place)))
    line = LineScatter(mail, place, dkv_ref, got)
    rows = PlaneScatter(mail, place, parts_ref, acc, bufs)
    block = RowsBack(mail, place, op_ref, op_got, ops_ref)
    line.begin()
    rows.begin()
    block.begin()
    rows.middle()
    rows.end()
    out_ref[...] = (mid_ref[...] + acc[...]).astype(BF16)
    kv_ref[...] = line.end().astype(BF16)
    block.end()
    mail.close()


def last_kernel(
    dq_ref, dkv_ref, raw_ref, norm_ref, w_ref, qk_ref, cos_ref, sin_ref,
    x_ref, dmid_ref, gain_ref, g2_ref, dg_ref, *refs,
):
    outer = lax.axis_size("blk") // INNER
    gu_refs, refs = refs[:outer], refs[outer:]
    (in_ref, ws_ref, gus_ref, down_ref, small_ref,
     ss, rs, dqkv, parts, acc, grads, got, held, gu_own, dg_got, small, p_got, z_got, *bufs) = refs
    place = y, c, z, x = here()
    me = rank(y, c, x)
    mail = Mail((ss, rs))
    peers, line = plane_peers(place), line_peers(place)
    greet([p[0] for p in line] + [p[0] for p in peers])
    swap = PlaneSwap(mail, place, gu_own, gus_ref)
    weights = LineScatter(mail, place, grads, got)
    down = LineScatter(mail, place, dg_ref, dg_got)
    total = gu_refs[0][...].astype(F32)
    for ref in gu_refs[1:]:
        total = total + ref[...].astype(F32)
    gu_own[...] = total.astype(BF16).reshape(gu_own.shape)
    swap.begin()

    count, tok, q_cols = dq_ref.shape
    size = q_cols // 2
    gain_q, gain_k = qk_ref[0:1], qk_ref[1:2]

    def one_block(r, sums):
        cos, sin = turn(cos_ref, sin_ref, r)
        raw_q, raw_k = raw_ref[r, :, :q_cols], raw_ref[r, :, q_cols:]
        dq, q_sum = head_back(raw_q, gain_q, cos, sin, size, dq_ref[r].astype(F32))
        dkv = dkv_ref[r].astype(F32)
        dk, k_sum = head_back(raw_k, gain_k, cos, sin, size, dkv)
        dqkv[r, :, :q_cols] = dq.astype(BF16)
        dqkv[r, :, q_cols:] = jnp.where(lanes(dk.shape) < size, dk, dkv).astype(BF16)
        return sums[0] + q_sum, sums[1] + k_sum

    zero = jnp.zeros((1, q_cols), F32)
    q_sum, k_sum = lax.fori_loop(0, count, one_block, (zero, zero))

    width = norm_ref.shape[2]
    flat = dqkv[...].reshape(count * tok, -1)
    w_grad = lax.dot_general(
        norm_ref[...].reshape(count * tok, width),
        flat,
        (((0,), (0,)), ((), ())),
        preferred_element_type=F32,
    ).astype(BF16)
    heads, w_rows = grads.shape[1], grads.shape[3]
    stride = INNER * w_rows
    for oz in range(outer):
        for oh in range(heads):
            first = (oh * outer + oz) * stride
            grads[oz, oh] = w_grad[first : first + stride].reshape(INNER, w_rows, -1)
    weights.begin()

    def make(block):
        parts[block] = lax.dot_general(
            dqkv[block], w_ref[...], NT, preferred_element_type=F32
        ).astype(BF16)

    rows = PlaneScatter(mail, place, parts, acc, bufs, make)
    rows.begin()
    rows.middle()
    down.begin()
    rows.end()
    back, dgain = rms_back(x_ref[...].astype(F32), gain_ref[0:1], acc[...])
    in_ref[...] = (dmid_ref[...] + back).astype(BF16)
    small[...] = jnp.zeros_like(small)
    small[0:1] = dgain
    small[1:2] = g2_ref[...]
    small[2:3, :q_cols] = q_sum
    small[3:4, :q_cols] = k_sum
    p_base, z_base, w_base = mail.take(7), mail.take(len(line)), mail.take(7)
    for slot, (dev, other, _) in enumerate(peers):
        mail.send(p_base + slot, small, p_got.at[me], dev)
    p_got[me] = small[...]
    held[...] = weights.end().reshape(held.shape)
    for slot, (dev, other, _) in enumerate(peers):
        mail.send(w_base + slot, held.at[other], ws_ref.at[me], dev)
    ws_ref[me] = held[me]
    for slot, (dev, other, _) in enumerate(peers):
        mail.arrive(p_base + slot, p_got.at[other], dev)
    z_got[z] = jnp.sum(p_got[...], axis=0)
    for slot, (dev, _, _) in enumerate(line):
        mail.send(z_base + slot, z_got.at[z], z_got.at[z], dev)
    swap.end()
    down_ref[...] = down.end()
    for slot, (dev, other, _) in enumerate(peers):
        mail.arrive(w_base + slot, ws_ref.at[other], dev)
    for slot, (dev, _, back) in enumerate(line):
        mail.arrive(z_base + slot, z_got.at[back], dev)
    small_ref[...] = jnp.sum(z_got[...], axis=0)
    mail.close()


def finish_kernel(own_ref, ws_ref, gus_ref, small_ref, *refs):
    n1_ref, n2_ref, q_ref, k_ref, v_ref, qk_ref, gate_ref, up_ref = refs[-8:]
    passed = refs[:-8]
    for src, dst in zip(passed[: len(passed) // 2], passed[len(passed) // 2 :]):
        dst[...] = src[...]
    plane, w_rows, _ = ws_ref.shape
    q_cols = q_ref.shape[1] // plane
    k_cols = q_cols // 2
    for p in range(0, plane, 2):
        one, two = ws_ref[p], ws_ref[p + 1]
        q_ref[:, p * q_cols : (p + 1) * q_cols] = one[:, :q_cols]
        q_ref[:, (p + 1) * q_cols : (p + 2) * q_cols] = two[:, :q_cols]
        at = slice(p * k_cols, (p + 2) * k_cols)
        left = lanes((w_rows, q_cols)) < k_cols
        one, two = one[:, q_cols:], two[:, q_cols:]
        k_ref[:, at] = jnp.where(left, one, pltpu.roll(two, k_cols, 1))
        v_ref[:, at] = jnp.where(left, pltpu.roll(one, k_cols, 1), two)
    width = small_ref.shape[1]
    move = lax.rem(width - own_ref[0], width)
    totals = pltpu.roll(small_ref[...], move, 1)
    n1_ref[...] = totals[0:1, :w_rows]
    n2_ref[...] = totals[1:2, :w_rows]
    sums = small_ref[...]
    query = sums[2:3, :k_cols] + sums[2:3, k_cols : 2 * k_cols]
    qk_ref[...] = jnp.concatenate([query, sums[3:4, :k_cols]], axis=0)
    outer = lax.axis_size("blk") // INNER
    heads = plane // INNER
    ff = gus_ref.shape[2] // 2
    main = ff // LANES * LANES
    tail = ff - main
    f_rows = ff // outer
    for col, out in ((0, gate_ref), (1, up_ref)):
        for oh in range(heads):
            cols = []
            for ox in range(INNER):
                block = gus_ref[oh * INNER + ox].astype(F32)
                rest = 2 * main + col * tail
                cols.append(
                    jnp.concatenate(
                        [block[:, col * main : (col + 1) * main], block[:, rest : rest + tail]],
                        axis=1,
                    )
                )
            span = INNER * ff
            out[:, oh * span : (oh + 1) * span] = jnp.concatenate(
                [
                    cols[ox][:, oz * f_rows : (oz + 1) * f_rows]
                    for oz in range(outer)
                    for ox in range(INNER)
                ],
                axis=1,
            )


def down_rows(ref, oz, f_rows, piece):
    pack = math.gcd(f_rows, 16)
    if pack == 16:
        ref[pl.ds(pl.multiple_of(oz * f_rows, pack), f_rows)] = piece[...]
        return
    for at in range(ref.shape[0] // f_rows):

        @pl.when(oz == at)
        def _():
            ref[at * f_rows : (at + 1) * f_rows] = piece[...]


def feed_kernel(z_ref, n2_ref, og_ref, *refs):
    outer = lax.axis_size("blk") // INNER
    pieces, downs, refs = refs[:outer], refs[outer : 2 * outer], refs[2 * outer :]
    out_ref, dn_ref, dg_ref = refs[:3]
    chunks = refs[3 : 3 + outer]
    wgu, wd_ref, hid, dgu, gg = refs[3 + outer :]
    z = z_ref[0]
    heads, stride, _ = pieces[0].shape
    ff = wd_ref.shape[0]
    main = ff // LANES * LANES
    tail = ff - main
    for k, piece in enumerate(pieces):
        oz = lax.rem(z + outer - k, outer)
        for oh in range(heads):
            at = pl.multiple_of((oh * outer + oz) * stride, stride)
            wgu[pl.ds(at, stride)] = piece[oh]
    f_rows = ff // outer
    for k, piece in enumerate(downs):
        down_rows(wd_ref, lax.rem(z + outer - k, outer), f_rows, piece)
    plane, rows, width = n2_ref.shape

    def both(gate, up, dhid):
        sig = 1.0 / (1.0 + jnp.exp(-gate))
        act = gate * sig
        return act * up, dhid * up * (sig * (1.0 + gate * (1.0 - sig))), dhid * act

    def one_block(b, carry):
        pair = pl.ds(2 * b, 2)
        at = pl.ds(pl.multiple_of(b * 2 * rows, 2 * rows), 2 * rows)
        block = n2_ref[pair].reshape(2 * rows, width)
        grad = og_ref[pair].reshape(2 * rows, width)
        gu = jnp.dot(block, wgu[...], preferred_element_type=F32)
        dhid = lax.dot_general(grad, wd_ref[...], NT, preferred_element_type=F32)
        h, dgate, dup = both(gu[:, :main], gu[:, main : 2 * main], dhid[:, :main])
        hid[at, :main] = h.astype(BF16)
        dgu[at, :main] = dgate.astype(BF16)
        dgu[at, main : 2 * main] = dup.astype(BF16)
        ends = gu[:, 2 * main :]
        left = lanes(ends.shape) < tail
        other = pltpu.roll(ends, tail, 1)
        dend = dhid[:, main:]
        dend = jnp.concatenate([dend, dend], axis=1)
        h, dgate, dup = both(jnp.where(left, ends, other), jnp.where(left, other, ends), dend)
        hid[at, main:] = h[:, :tail].astype(BF16)
        dgu[at, 2 * main :] = jnp.where(left, dgate, dup).astype(BF16)
        down = jnp.dot(hid[at], wd_ref[...], preferred_element_type=F32)
        out_ref[pair] = down.astype(BF16).reshape(2, rows, width)
        narrow = lax.dot_general(dgu[at], wgu[...], NT, preferred_element_type=F32)
        dn_ref[pair] = narrow.astype(BF16).reshape(2, rows, width)
        return carry

    lax.fori_loop(0, plane // 2, one_block, 0)
    n2_width = width // heads
    w_rows = stride // INNER

    def one_head(oh, carry):
        cols = pl.ds(pl.multiple_of(oh * n2_width, n2_width), n2_width)
        grad = lax.dot_general(
            n2_ref[:, :, cols].reshape(plane * rows, n2_width),
            dgu[...],
            TN,
            preferred_element_type=F32,
        )
        for oz in range(outer):
            for ox in range(INNER):
                first = oz * stride + ox * w_rows
                gg[oz, oh * INNER + ox] = grad[first : first + w_rows].astype(BF16)
        return carry

    lax.fori_loop(0, heads, one_head, 0)
    for k, chunk in enumerate(chunks):
        chunk[...] = gg[lax.rem(z + k, outer)]
    grads = og_ref[...].reshape(plane * rows, width)
    down = lax.dot_general(hid[...], grads, TN, preferred_element_type=F32)
    for oz in range(outer):
        dg_ref[oz] = down[oz * f_rows : (oz + 1) * f_rows].astype(BF16)


SPANS = 4
LOG2E = math.log2(math.e)


def stack_left(block, size):
    wide = block.astype(F32)
    left = lanes(wide.shape) < size
    first = jnp.where(left, wide, 0.0)
    second = jnp.where(left, pltpu.roll(wide, size, 1), 0.0)
    return jnp.concatenate([first, second], axis=0).astype(BF16)


def stack_right(block, size):
    wide = block.astype(F32)
    right = lanes(wide.shape) >= size
    first = jnp.where(right, pltpu.roll(wide, size, 1), 0.0)
    second = jnp.where(right, wide, 0.0)
    return jnp.concatenate([first, second], axis=0).astype(BF16)


def forward_kernel(own_ref, at_ref, q_ref, kv_ref, out_ref, lse_ref, keys, ones):
    count, rows, size2 = q_ref.shape
    size = size2 // 2
    scale = float(size) ** (-0.5) * LOG2E
    step = SPANS * rows

    def place_rows(p, carry):
        block = kv_ref[at_ref[p]]
        keys[pl.ds(p * rows, rows)] = block
        ones[pl.ds(p * rows, rows)] = jnp.where(lanes(block.shape) < size, 1.0, block).astype(BF16)
        return carry

    lax.fori_loop(0, kv_ref.shape[0], place_rows, 0)

    def one_block(r, carry):
        place = own_ref[r]
        queries = stack_left(q_ref[r], size)

        def weights(c):
            part = keys[pl.ds(c * step, step)]
            scores = lax.dot_general(queries, part, NT, preferred_element_type=F32)
            return jnp.exp2(scores * scale)

        def mix(c, held, total):
            part = ones[pl.ds(c * step, step)]
            return total + jnp.dot(held.astype(BF16), part, preferred_element_type=F32)

        def full(c, total):
            return mix(c, weights(c), total)

        last = place // SPANS
        total = lax.fori_loop(0, last, full, jnp.zeros((2 * rows, size2), F32))
        held = weights(last)
        row = lax.broadcasted_iota(jnp.int32, held.shape, 0)
        row = jnp.where(row >= rows, row - rows, row) + (place - last * SPANS) * rows
        held = jnp.where(lanes(held.shape) <= row, held, 0.0)
        total = mix(last, held, total)
        divided = total / total[:, :1]
        left = lanes((rows, size2)) < size
        out_ref[r] = jnp.where(left, pltpu.roll(divided[:rows], size, 1), divided[rows:]).astype(
            BF16
        )
        lse_ref[r] = jnp.log2(total.T[:8])
        return carry

    lax.fori_loop(0, count, one_block, 0)


def backward_kernel(
    own_ref, at_ref, q_ref, kv_ref, out_ref, do_ref, lse_ref, dq_ref, dkv_ref, keys, turned, sums
):
    count, rows, size2 = q_ref.shape
    size = size2 // 2
    scale = float(size) ** (-0.5)
    step = SPANS * rows
    spans = kv_ref.shape[0]

    def place_rows(p, carry):
        block = kv_ref[at_ref[p]]
        keys[pl.ds(p * rows, rows)] = block
        turned[:, pl.ds(p * rows, rows)] = block.astype(F32).T.astype(BF16)
        return carry

    lax.fori_loop(0, spans, place_rows, 0)
    sums[...] = jnp.zeros_like(sums)

    def one_block(r, carry):
        place = own_ref[r]
        queries = stack_left(q_ref[r], size)
        grads = stack_right(do_ref[r], size)
        both = (do_ref[r].astype(F32) * out_ref[r].astype(F32)).T
        delta = jnp.concatenate(
            [jnp.sum(both[:size], axis=0)[None], jnp.sum(both[size:], axis=0)[None]], axis=1
        )
        lse = lse_ref[r][:1]

        def one_step(c, total, masked):
            at = pl.ds(pl.multiple_of(c * step, step), step)
            part = keys[at]
            scores = lax.dot_general(part, queries, NT, preferred_element_type=F32)
            prob = jnp.exp2(scores * (scale * LOG2E) - lse)
            if masked:
                key = lax.broadcasted_iota(jnp.int32, prob.shape, 0)
                row = lanes(prob.shape)
                row = jnp.where(row >= rows, row - rows, row) + (place - c * SPANS) * rows
                prob = jnp.where(key <= row, prob, 0.0)
            dprob = lax.dot_general(part, grads, NT, preferred_element_type=F32)
            dscore = (prob * (dprob - delta)).astype(BF16)
            sums[at] += jnp.dot(dscore, queries, preferred_element_type=F32) + jnp.dot(
                prob.astype(BF16), grads, preferred_element_type=F32
            )
            return total + jnp.dot(turned[:, at], dscore, preferred_element_type=F32)

        last = place // SPANS
        total = lax.fori_loop(
            0, last, lambda c, t: one_step(c, t, False), jnp.zeros((size2, 2 * rows), F32)
        )
        total = one_step(last, total, True).T * scale
        left = lanes((rows, size2)) < size
        dq_ref[r] = jnp.where(left, total[:rows], pltpu.roll(total[rows:], size, 1)).astype(BF16)
        return carry

    lax.fori_loop(0, count, one_block, 0)

    def give_rows(p, carry):
        block = sums[pl.ds(p * rows, rows)]
        factor = jnp.where(lanes(block.shape) < size, scale, 1.0)
        dkv_ref[at_ref[p]] = (block * factor).astype(BF16)
        return carry

    lax.fori_loop(0, spans, give_rows, 0)


def local_call(body, scalars, args, outs, scratch, flops):
    vmem = pl.BlockSpec(memory_space=pltpu.VMEM)
    smem = pl.BlockSpec(memory_space=pltpu.SMEM)
    return pl.pallas_call(
        body,
        out_shape=tuple(jax.ShapeDtypeStruct(shape, dtype) for shape, dtype in outs),
        in_specs=[smem] * len(scalars) + [vmem] * len(args),
        out_specs=tuple([vmem] * len(outs)),
        scratch_shapes=scratch,
        cost_estimate=pl.CostEstimate(flops=flops, bytes_accessed=8 << 20, transcendentals=0),
        compiler_params=pltpu.CompilerParams(vmem_limit_bytes=60 * 1024 * 1024),
    )(*scalars, *args)


def shifts(outer, step):
    return [
        (z * INNER + x, ((z + step) % outer) * INNER + x)
        for z in range(outer)
        for x in range(INNER)
    ]


def local(
    block_input,
    span_order,
    norm1_gain,
    w_query,
    key_weight,
    value_weight,
    qk_gain,
    w_out,
    norm2_gain,
    w_gate,
    w_up,
    w_down,
    out_grad,
):
    heads = lax.axis_size("head")
    blocks = lax.axis_size("blk")
    outer = blocks // INNER
    plane = heads * INNER
    z = lax.axis_index("blk") // INNER
    rows, width = block_input.shape
    size = qk_gain.shape[1]
    w_rows = w_query.shape[0]
    f_rows = w_down.shape[0]
    q_cols = w_query.shape[1] // plane
    a_cols = 2 * q_cols
    ff = f_rows * outer
    spans = outer * plane
    n_line = outer - 1
    stride = INNER * w_rows

    def along(piece):
        moved = [
            lax.ppermute(piece, "blk", shifts(outer, step)) for step in range(1, outer)
        ]
        return [piece] + moved

    down_pieces = along(w_down)
    x_all, wqkv, gains, gu8, out_mine = call(
        start_kernel,
        1,
        [
            ((plane, rows, width), BF16),
            ((heads, outer, INNER, w_rows, a_cols), BF16),
            ((8, width), F32),
            ((plane, w_rows, 2 * ff), BF16),
            ((outer // INNER, INNER, w_rows, width), BF16),
        ],
        (
            block_input,
            w_query,
            key_weight,
            value_weight,
            norm1_gain.reshape(1, w_rows),
            norm2_gain.reshape(1, w_rows),
            w_gate,
            w_up,
            w_out,
        ),
        2 * (outer * plane - 1) + PlaneGather.COPIES + outer,
        [
            pltpu.VMEM((plane, w_rows, a_cols), BF16),
            pltpu.VMEM((1, LANES), F32),
            pltpu.VMEM((outer, plane, 1, LANES), F32),
        ],
    )
    wqkv = wqkv.reshape(width, a_cols)
    out_mine = out_mine.reshape(q_cols, width)

    by_place = span_order.reshape(heads, outer, INNER)
    own_spans = lax.dynamic_index_in_dim(by_place, z, 1, keepdims=False).reshape(plane)
    all_spans = by_place.transpose(1, 0, 2).reshape(spans)
    every = jnp.arange(spans, dtype=jnp.int32)
    span_at = jnp.sum(jnp.where(all_spans[:, None] == every[None, :], every[:, None], 0), axis=0)
    where_at = own_spans[:, None] * rows + jnp.arange(rows, dtype=jnp.int32)[None, :]
    half = size // 2
    frequency = jnp.exp(jnp.arange(half, dtype=F32) * F32(-2.0 * math.log(THETA) / size))
    angles = where_at.astype(F32)[:, None, :] * frequency[None, :, None]
    cosine, sine = jnp.cos(angles), jnp.sin(angles)
    ones = jnp.ones((size,), F32)
    qk_rows = jnp.stack(
        [
            jnp.concatenate([qk_gain[0], qk_gain[0]]),
            jnp.concatenate([qk_gain[1], ones]),
        ]
    )

    queries, kv_all, raw, normed, og_all, gu_piece = call(
        line_kernel,
        2,
        [
            ((plane, rows, q_cols), BF16),
            ((outer, plane, rows, q_cols), BF16),
            ((plane, rows, a_cols), F32),
            ((plane, rows, width), BF16),
            ((plane, rows, width), BF16),
            ((plane, w_rows, 2 * ff), BF16),
        ],
        (x_all, wqkv, gains, qk_rows, cosine, sine, out_grad, gu8),
        2 * n_line + PlaneGather.COPIES + PlaneSwap.COPIES,
        [pltpu.VMEM((plane, rows, q_cols), BF16)],
    )
    gu_pieces = along(gu_piece.reshape(heads, stride, 2 * ff))
    kv_blocks = kv_all.reshape(spans, rows, q_cols)
    pairs = plane * rows * spans * rows * q_cols
    attended, log_total = local_call(
        forward_kernel,
        (own_spans, span_at),
        (queries, kv_blocks),
        [((plane, rows, q_cols), BF16), ((plane, 8, 2 * rows), F32)],
        [pltpu.VMEM((spans * rows, q_cols), BF16), pltpu.VMEM((spans * rows, q_cols), BF16)],
        4 * pairs,
    )
    middle, normed2 = call(
        mix_kernel,
        3,
        [((rows, width), F32), ((plane, rows, width), BF16)],
        (attended, out_mine, block_input, gains),
        PlaneScatter.COPIES + PlaneGather.COPIES,
        [pltpu.VMEM((plane, rows, width), BF16), pltpu.VMEM((rows, width), BF16)]
        + PlaneScatter.scratch(rows, width),
    )

    out_parts, dn_parts, down_grad, *gu_grads = local_call(
        feed_kernel,
        (jnp.reshape(z, (1,)).astype(jnp.int32),),
        (normed2, og_all, *gu_pieces, *down_pieces),
        [
            ((plane, rows, width), BF16),
            ((plane, rows, width), BF16),
            ((outer, f_rows, width), BF16),
        ]
        + [((plane, w_rows, 2 * ff), BF16)] * outer,
        [
            pltpu.VMEM((width, 2 * ff), BF16),
            pltpu.VMEM((ff, width), BF16),
            pltpu.VMEM((plane * rows, ff), BF16),
            pltpu.VMEM((plane * rows, 2 * ff), BF16),
            pltpu.VMEM((outer, plane, w_rows, 2 * ff), BF16),
        ],
        18 * plane * rows * width * ff,
    )
    gu_sums = [gu_grads[0]] + [
        lax.ppermute(gu_grads[step], "blk", shifts(outer, step)) for step in range(1, outer)
    ]
    dmiddle, dmid_all, norm2_grad = call(
        narrow_kernel,
        4,
        [((rows, width), F32), ((plane, rows, width), BF16), ((1, width), F32)],
        (dn_parts, middle, out_grad, gains),
        PlaneScatter.COPIES + PlaneGather.COPIES,
        [pltpu.VMEM((rows, width), BF16)] + PlaneScatter.scratch(rows, width),
    )

    dmid_rows = dmid_all.reshape(plane * rows, width)
    out_proj = lax.dot_general(
        attended.reshape(plane * rows, q_cols), dmid_rows, TN, preferred_element_type=F32
    )
    dattended = lax.dot_general(dmid_rows, out_mine, NT, preferred_element_type=F32).astype(BF16)
    dqueries, dkv = local_call(
        backward_kernel,
        (own_spans, span_at),
        (queries, kv_blocks, attended, dattended.reshape(plane, rows, q_cols), log_total),
        [((plane, rows, q_cols), BF16), ((spans, rows, q_cols), BF16)],
        [
            pltpu.VMEM((spans * rows, q_cols), BF16),
            pltpu.VMEM((q_cols, spans * rows), BF16),
            pltpu.VMEM((spans * rows, q_cols), F32),
        ],
        10 * pairs,
    )
    dkv_own, block_output, out_proj_grad = call(
        back_kernel,
        5,
        [((plane, rows, q_cols), BF16), ((rows, width), BF16), ((w_rows, width), F32)],
        (
            dkv.reshape(outer, plane, rows, q_cols),
            out_parts,
            out_proj.astype(BF16).reshape(outer // INNER, INNER, w_rows, width),
            middle,
        ),
        n_line + PlaneScatter.COPIES + outer,
        [
            pltpu.VMEM((rows, width), F32),
            pltpu.VMEM((n_line, plane, rows, q_cols), BF16),
            pltpu.VMEM((outer, w_rows, width), BF16),
        ]
        + PlaneScatter.scratch(rows, width),
    )
    input_grad, w_own, gu_own, down_out, small = call(
        last_kernel,
        6,
        [
            ((rows, width), BF16),
            ((plane, w_rows, a_cols), F32),
            ((plane, w_rows, 2 * ff), BF16),
            ((f_rows, width), F32),
            ((8, width), F32),
        ],
        (
            dqueries,
            dkv_own,
            raw,
            normed,
            wqkv,
            qk_rows,
            cosine,
            sine,
            block_input,
            dmiddle,
            gains,
            norm2_grad,
            down_grad,
            *gu_sums,
        ),
        3 * n_line + 14 + PlaneScatter.COPIES + PlaneSwap.COPIES,
        [
            pltpu.VMEM((plane, rows, a_cols), BF16),
            pltpu.VMEM((plane, rows, width), BF16),
            pltpu.VMEM((rows, width), F32),
            pltpu.VMEM((outer, heads, INNER, w_rows, a_cols), BF16),
            pltpu.VMEM((n_line, heads, INNER, w_rows, a_cols), BF16),
            pltpu.VMEM((plane, w_rows, a_cols), F32),
            pltpu.VMEM((plane, w_rows, 2 * ff), BF16),
            pltpu.VMEM((n_line, f_rows, width), BF16),
            pltpu.VMEM((8, width), F32),
            pltpu.VMEM((plane, 8, width), F32),
            pltpu.VMEM((outer, 8, width), F32),
        ]
        + PlaneScatter.scratch(rows, width),
    )
    own = (lax.axis_index("head") * blocks + lax.axis_index("blk")) * w_rows
    outs = local_call(
        finish_kernel,
        (jnp.reshape(own, (1,)).astype(jnp.int32),),
        (w_own, gu_own, small, block_output, input_grad, out_proj_grad, down_out),
        [
            ((rows, width), BF16),
            ((rows, width), BF16),
            ((w_rows, width), F32),
            ((f_rows, width), F32),
            ((1, w_rows), F32),
            ((1, w_rows), F32),
            (w_query.shape, F32),
            (key_weight.shape, F32),
            (value_weight.shape, F32),
            ((2, size), F32),
            (w_gate.shape, F32),
            (w_up.shape, F32),
        ],
        [],
        1 << 20,
    )
    (block_output, input_grad, out_proj_grad, down_grad, norm1_grad, norm2_grad,
     query_grad, key_grad, value_grad, qk_gain_grad, gate_grad, up_grad) = outs
    return (
        block_output,
        input_grad,
        norm1_grad.reshape(w_rows),
        query_grad,
        key_grad,
        value_grad,
        qk_gain_grad,
        out_proj_grad,
        norm2_grad.reshape(w_rows),
        gate_grad,
        up_grad,
        down_grad,
    )


def solution(mesh):
    split = P(("head", "blk"), None)
    line = P(("head", "blk"))
    in_specs = (split, P(), line, split, split, split, P(), split, line, split, split, split, split)
    out_specs = (split, split, line, split, split, split, P(), split, line, split, split, split)
    return jax.shard_map(local, mesh=mesh, in_specs=in_specs, out_specs=out_specs, check_vma=False)
```

```python
import math

import jax
import jax.numpy as jnp
from jax import lax
from jax.experimental import pallas as pl
from jax.experimental.pallas import tpu as pltpu
from jax.sharding import PartitionSpec as P


EPS = 1e-05
THETA = 1000000.0
LANES = 128
CORES = 2
INNER = 2
MESH = pl.DeviceIdType.MESH
F32 = jnp.float32
BF16 = jnp.bfloat16
NT = (((1,), (1,)), ((), ()))
TN = (((0,), (0,)), ((), ()))


def here():
    head = lax.axis_index("head")
    blk = lax.axis_index("blk")
    return head // CORES, head % CORES, blk // INNER, blk % INNER


def device(y, c, z, x):
    return (y * CORES + c, z * INNER + x)


def rank(y, c, x):
    return (y * CORES + c) * INNER + x


def plane_peers(place):
    y, c, z, x = place
    peers = []
    for bits in range(1, 8):
        py = 1 - y if bits & 4 else y
        pc = 1 - c if bits & 2 else c
        px = 1 - x if bits & 1 else x
        peers.append((device(py, pc, z, px), rank(py, pc, px), (py * CORES + pc, px)))
    return peers


def line_peers(place):
    y, c, z, x = place
    outer = lax.axis_size("blk") // INNER
    forth = [lax.rem(z + k, outer) for k in range(1, outer)]
    back = [lax.rem(z + outer - k, outer) for k in range(1, outer)]
    return [(device(y, c, f, x), f, b) for f, b in zip(forth, back)]


def greet(devices):
    barrier = pltpu.get_barrier_semaphore()
    for dev in devices:
        pl.semaphore_signal(barrier, inc=1, device_id=dev, device_id_type=MESH)
    pl.semaphore_wait(barrier, len(devices))


class Mail:
    def __init__(self, sems):
        self.sends, self.recvs = sems
        self.used = 0
        self.open = []
        self.guarded = []

    def take(self, count):
        first = self.used
        self.used += count
        return first

    def copy(self, slot, src, dst, dev, landing=None):
        return pltpu.make_async_remote_copy(
            src_ref=src,
            dst_ref=dst,
            send_sem=self.sends.at[slot],
            recv_sem=self.recvs.at[slot if landing is None else landing],
            device_id=dev,
            device_id_type=MESH,
        )

    def send(self, slot, src, dst, dev, landing=None):
        copy = self.copy(slot, src, dst, dev, landing)
        copy.start()
        self.open.append(copy)

    def arrive(self, slot, dst, dev):
        self.copy(slot, dst, dst, dev).wait_recv()

    def send_if(self, when, slot, src, dst, dev):
        copy = self.copy(slot, src, dst, dev)
        pl.when(when)(copy.start)
        self.guarded.append((when, copy))

    def arrive_if(self, when, slot, dst, dev):
        pl.when(when)(self.copy(slot, dst, dst, dev).wait_recv)

    def close(self):
        for copy in self.open:
            copy.wait_send()
        for when, copy in self.guarded:
            pl.when(when)(copy.wait_send)


def near(place):
    y, c, z, x = place
    return device(y, 1 - c, z, x), device(y, c, z, 1 - x), device(1 - y, c, z, x)


class PlaneGather:
    COPIES = 11

    def __init__(self, mail, place, src, out):
        self.mail, self.place, self.src, self.out = mail, place, src, out
        self.base = mail.take(self.COPIES)
        half = src.shape[0] // 2
        self.top, self.bot = pl.ds(0, half), pl.ds(half, half)

    def begin(self):
        y, c, _, x = self.place
        pair, xn, yn = near(self.place)
        me = rank(y, c, x)
        send, base, src, out = self.mail.send, self.base, self.src, self.out
        top, bot = self.top, self.bot
        send(base + 0, src.at[top], out.at[me, top], xn)
        send(base + 1, src.at[bot], out.at[me, bot], yn)
        send(base + 2, src.at[bot], out.at[me, bot], xn)
        send(base + 3, src.at[top], out.at[me, top], yn)
        send(base + 4, src, out.at[me], pair)
        out[me] = src[...]

    def middle(self):
        y, c, _, x = self.place
        pair, xn, yn = near(self.place)
        xr, yr = rank(y, c, 1 - x), rank(1 - y, c, x)
        send, arrive, base, out = self.mail.send, self.mail.arrive, self.base, self.out
        top, bot = self.top, self.bot
        arrive(base + 0, out.at[xr, top], xn)
        send(base + 5, out.at[xr, top], out.at[xr, top], yn)
        arrive(base + 1, out.at[yr, bot], yn)
        send(base + 6, out.at[yr, bot], out.at[yr, bot], xn)
        arrive(base + 2, out.at[xr, bot], xn)
        send(base + 7, out.at[xr], out.at[xr], pair)
        arrive(base + 3, out.at[yr, top], yn)
        send(base + 8, out.at[yr], out.at[yr], pair)

    def end(self):
        y, c, _, x = self.place
        pair, xn, yn = near(self.place)
        dr = rank(1 - y, c, 1 - x)
        send, arrive, base, out = self.mail.send, self.mail.arrive, self.base, self.out
        top, bot = self.top, self.bot
        arrive(base + 5, out.at[dr, top], yn)
        send(base + 9, out.at[dr, top], out.at[dr, top], pair)
        arrive(base + 6, out.at[dr, bot], xn)
        send(base + 10, out.at[dr, bot], out.at[dr, bot], pair)
        arrive(base + 4, out.at[rank(y, 1 - c, x)], pair)
        arrive(base + 7, out.at[rank(y, 1 - c, 1 - x)], pair)
        arrive(base + 8, out.at[rank(1 - y, 1 - c, x)], pair)
        far = rank(1 - y, 1 - c, 1 - x)
        arrive(base + 9, out.at[far, top], pair)
        arrive(base + 10, out.at[far, bot], pair)


class PlaneScatter:
    COPIES = 10

    def __init__(self, mail, place, parts, out, bufs, make=None):
        self.mail, self.place, self.parts, self.out = mail, place, parts, out
        self.make = make or (lambda block: None)
        self.first, self.held, self.via_x, self.via_y, self.last = bufs
        self.base = mail.take(self.COPIES)
        half = out.shape[0] // 2
        self.top, self.bot = pl.ds(0, half), pl.ds(half, half)

    @staticmethod
    def scratch(rows, cols):
        half = rows // 2
        return [
            pltpu.VMEM((2, 2, rows, cols), BF16),
            pltpu.VMEM((2, 2, rows, cols), BF16),
            pltpu.VMEM((2, half, cols), BF16),
            pltpu.VMEM((2, half, cols), BF16),
            pltpu.VMEM((4, half, cols), BF16),
        ]

    def begin(self):
        y, c, _, x = self.place
        pair, _, _ = near(self.place)
        for slot, (py, px) in enumerate(((1 - y, 1 - x), (y, 1 - x), (1 - y, x), (y, x))):
            self.make(rank(py, 1 - c, px))
            self.mail.send(
                self.base + slot,
                self.parts.at[rank(py, 1 - c, px)],
                self.first.at[py, px],
                pair,
            )

    def joined(self, slot, py, px):
        _, c, _, _ = self.place
        pair, _, _ = near(self.place)
        self.make(rank(py, c, px))
        self.mail.arrive(self.base + slot, self.first.at[py, px], pair)
        return self.parts[rank(py, c, px)].astype(F32) + self.first[py, px].astype(F32)

    def middle(self):
        y, _, _, x = self.place
        _, xn, yn = near(self.place)
        send, base, held = self.mail.send, self.base, self.held
        top, bot = self.top, self.bot
        held[1 - y, 1 - x] = self.joined(0, 1 - y, 1 - x).astype(BF16)
        send(base + 4, held.at[1 - y, 1 - x, top], self.via_x.at[1 - y], xn)
        send(base + 5, held.at[1 - y, 1 - x, bot], self.via_y.at[1 - x], yn)
        held[y, 1 - x] = self.joined(1, y, 1 - x).astype(BF16)
        send(base + 6, held.at[y, 1 - x, top], self.via_x.at[y], xn)
        held[1 - y, x] = self.joined(2, 1 - y, x).astype(BF16)
        send(base + 7, held.at[1 - y, x, bot], self.via_y.at[x], yn)
        self.out[...] = self.joined(3, y, x)

    def end(self):
        y, _, _, x = self.place
        _, xn, yn = near(self.place)
        send, arrive, base, held = self.mail.send, self.mail.arrive, self.base, self.held
        top, bot, last, out = self.top, self.bot, self.last, self.out
        arrive(base + 4, self.via_x.at[1 - y], xn)
        last[0] = (held[1 - y, x, top].astype(F32) + self.via_x[1 - y].astype(F32)).astype(BF16)
        send(base + 8, last.at[0], last.at[2], yn)
        arrive(base + 5, self.via_y.at[1 - x], yn)
        last[1] = (held[y, 1 - x, bot].astype(F32) + self.via_y[1 - x].astype(F32)).astype(BF16)
        send(base + 9, last.at[1], last.at[3], xn)
        arrive(base + 6, self.via_x.at[y], xn)
        out[top] = out[top] + self.via_x[y].astype(F32)
        arrive(base + 7, self.via_y.at[x], yn)
        out[bot] = out[bot] + self.via_y[x].astype(F32)
        arrive(base + 8, last.at[2], yn)
        out[top] = out[top] + last[2].astype(F32)
        arrive(base + 9, last.at[3], xn)
        out[bot] = out[bot] + last[3].astype(F32)


class LineGather:
    def __init__(self, mail, place, src, view):
        self.mail, self.place, self.src, self.view = mail, place, src, view
        self.outer = lax.axis_size("blk") // INNER
        self.base = mail.take(self.copies(self.outer))

    @staticmethod
    def copies(outer):
        return 2 * (outer - 1)

    def sides(self):
        _, _, z, _ = self.place
        outer = self.outer

        def along(sign):
            def at(k):
                there = z + sign * k
                exists = (there >= 0) & (there < outer)
                return lax.rem(there + 2 * outer, outer), exists

            return at

        return ((self.base, along(1)), (self.base + outer - 1, along(-1)))

    def begin(self):
        y, c, z, x = self.place
        for base, at in self.sides():
            to, exists = at(1)
            self.mail.send_if(exists, base, self.src, self.view(z), device(y, c, to, x))

    def relay(self):
        y, c, _, x = self.place
        for base, at in self.sides():
            back, has = at(-1)
            self.mail.arrive_if(has, base, self.view(back), device(y, c, back, x))
            for k in range(1, self.outer - 1):
                to, exists = at(k)
                self.mail.send_if(
                    has & exists,
                    base + k,
                    self.view(back),
                    self.view(back),
                    device(y, c, to, x),
                )

    def end(self):
        y, c, _, x = self.place
        for base, at in self.sides():
            for k in range(1, self.outer - 1):
                sender, _ = at(-k)
                owner, has = at(-k - 1)
                self.mail.arrive_if(has, base + k, self.view(owner), device(y, c, sender, x))


class LineScatter:
    def __init__(self, mail, place, parts, bufs):
        self.mail, self.place, self.parts = mail, place, parts
        self.far, self.staged, self.final = bufs
        self.outer = lax.axis_size("blk") // INNER
        self.base = mail.take(LineGather.copies(self.outer))
        self.far[...] = jnp.zeros_like(self.far)
        self.final[...] = jnp.zeros_like(self.final)

    sides = LineGather.sides

    @staticmethod
    def scratch(outer, shape):
        return [
            pltpu.VMEM((2, outer - 2, *shape), BF16),
            pltpu.VMEM((2, *shape), BF16),
            pltpu.VMEM((2, *shape), BF16),
        ]

    def begin(self):
        y, c, _, x = self.place
        for side, (base, at) in enumerate(self.sides()):
            for k in range(1, self.outer - 1):
                to, _ = at(k)
                owner, exists = at(k + 1)
                self.mail.send_if(
                    exists,
                    base + k,
                    self.parts.at[owner],
                    self.far.at[side, k - 1],
                    device(y, c, to, x),
                )

    def relay(self):
        y, c, _, x = self.place
        for side, (base, at) in enumerate(self.sides()):
            owner, exists = at(1)
            for k in range(1, self.outer - 1):
                sender, has = at(-k)
                self.mail.arrive_if(
                    exists & has, base + k, self.far.at[side, k - 1], device(y, c, sender, x)
                )
            total = self.parts[owner].astype(F32)
            for k in range(self.outer - 2):
                total = total + self.far[side, k].astype(F32)
            self.staged[side] = total.astype(BF16)
            self.mail.send_if(
                exists, base, self.staged.at[side], self.final.at[side], device(y, c, owner, x)
            )

    def end(self):
        y, c, z, x = self.place
        total = self.parts[z].astype(F32)
        for side, (base, at) in enumerate(self.sides()):
            sender, has = at(-1)
            self.mail.arrive_if(has, base, self.final.at[side], device(y, c, sender, x))
            total = total + self.final[side].astype(F32)
        return total


class PlaneSwap:
    COPIES = 7

    def __init__(self, mail, place, src, out):
        self.mail, self.place, self.src, self.out = mail, place, src, out
        self.base = mail.take(self.COPIES)

    def begin(self):
        y, c, _, x = self.place
        me = rank(y, c, x)
        for slot, (dev, other, _) in enumerate(plane_peers(self.place)):
            self.mail.send(self.base + slot, self.src.at[other], self.out.at[me], dev)
        self.out[me] = self.src[me]

    def end(self):
        for slot, (dev, other, _) in enumerate(plane_peers(self.place)):
            self.mail.arrive(self.base + slot, self.out.at[other], dev)


def blk_peers(place):
    y, c, z, x = place
    outer = lax.axis_size("blk") // INNER
    others = [device(y, c, lax.rem(z + k, outer), 1 - x) for k in range(1, outer)]
    return [p[0] for p in line_peers(place)] + others


class RowsOut:
    def __init__(self, mail, place, src, out):
        self.mail, self.place, self.src, self.out = mail, place, src, out
        self.outer = lax.axis_size("blk") // INNER
        self.per = self.outer // INNER
        self.base = mail.take(self.outer)

    def first(self):
        y, c, z, x = self.place
        return self.mail.copy(
            self.base,
            self.src,
            self.out.at[lax.rem(z, self.per), x],
            device(y, c, z, 1 - x),
            self.base + lax.rem(z, self.per) * INNER + x,
        )

    def begin(self):
        y, c, z, x = self.place
        to = z // self.per
        landing = self.base + lax.rem(z, self.per) * INNER + x
        place_there = self.out.at[lax.rem(z, self.per), x]

        @pl.when(to != x)
        def _():
            self.first().start()

        @pl.when(to == x)
        def _():
            self.out[lax.rem(z, self.per), x] = self.src[...]

        for k in range(1, self.outer):
            dev = device(y, c, lax.rem(z + k, self.outer), to)
            self.mail.send(self.base + k, self.src, place_there, dev, landing)

    def end(self):
        y, c, z, x = self.place

        @pl.when(z // self.per != x)
        def _():
            self.first().wait_send()

        for j in range(self.per):
            for ox in range(INNER):
                oz = x * self.per + j
                own = (oz == z) & (x * 0 + ox == x)

                @pl.when(jnp.logical_not(own))
                def _():
                    self.mail.arrive(
                        self.base + j * INNER + ox, self.out.at[j, ox], device(y, c, oz, ox)
                    )


class RowsBack:
    def __init__(self, mail, place, parts, got, out):
        self.mail, self.place, self.parts, self.got, self.out = mail, place, parts, got, out
        self.outer = lax.axis_size("blk") // INNER
        self.per = self.outer // INNER
        self.base = mail.take(self.outer)

    def copies(self):
        y, c, z, x = self.place
        for j in range(self.per):
            for ox in range(INNER):
                oz = x * self.per + j
                own = (oz == z) & (x * 0 + ox == x)
                copy = self.mail.copy(
                    self.base + j * INNER + ox,
                    self.parts.at[j, ox],
                    self.got.at[z],
                    device(y, c, oz, ox),
                    self.base + z,
                )
                yield j, ox, own, copy

    def begin(self):
        _, _, z, _ = self.place
        for j, ox, own, copy in self.copies():

            @pl.when(own)
            def _():
                self.got[z] = self.parts[j, ox]

            @pl.when(jnp.logical_not(own))
            def _():
                copy.start()

    def end(self):
        y, c, z, x = self.place
        for j, ox, own, copy in self.copies():

            @pl.when(jnp.logical_not(own))
            def _():
                copy.wait_send()

        to = z // self.per
        for oz in range(self.outer):

            @pl.when(jnp.logical_not((z == oz) & (to == x)))
            def _():
                self.mail.arrive(self.base + oz, self.got.at[oz], device(y, c, z * 0 + oz, to))

        total = self.got[0].astype(F32)
        for oz in range(1, self.outer):
            total = total + self.got[oz].astype(F32)
        self.out[...] = total


def call(body, ident, outs, args, copies, scratch=(), scalars=()):
    spec = pl.BlockSpec(memory_space=pltpu.VMEM)
    return remote_call(body, ident, outs, args, copies, scratch, scalars, spec)


def remote_call(body, ident, outs, args, copies, scratch, scalars, spec):
    return pl.pallas_call(
        body,
        out_shape=tuple(jax.ShapeDtypeStruct(shape, dtype) for shape, dtype in outs),
        in_specs=[pl.BlockSpec(memory_space=pltpu.SMEM)] * len(scalars) + [spec] * len(args),
        out_specs=tuple([spec] * len(outs)),
        scratch_shapes=[
            pltpu.SemaphoreType.DMA((copies,)),
            pltpu.SemaphoreType.DMA((copies,)),
            *scratch,
        ],
        compiler_params=pltpu.CompilerParams(
            collective_id=ident, has_side_effects=True, vmem_limit_bytes=60 * 1024 * 1024
        ),
    )(*scalars, *args)


def lanes(shape):
    return lax.broadcasted_iota(jnp.int32, shape, len(shape) - 1)


def rms_of(values):
    return lax.rsqrt(jnp.mean(values * values, axis=-1, keepdims=True) + EPS)


def rms_back(values, gain_vec, grad):
    inverse = rms_of(values)
    shaped = grad * gain_vec
    mean = jnp.mean(values * shaped, axis=-1, keepdims=True)
    dgain = jnp.sum(grad * values * inverse, axis=0, keepdims=True)
    return inverse * shaped - values * (inverse * inverse * inverse * mean), dgain


def per_head(values, size):
    left = lanes(values.shape) < size
    first = jnp.sum(jnp.where(left, values, 0.0), axis=-1, keepdims=True)
    second = jnp.sum(jnp.where(left, 0.0, values), axis=-1, keepdims=True)
    return jnp.where(left, first, second)


def head_rms(values, size):
    return lax.rsqrt(per_head(values * values, size) * (1.0 / size) + EPS)


def swap_halves(values, size):
    half = size // 2
    width = values.shape[-1]
    first = lanes(values.shape) % size < half
    return jnp.where(first, pltpu.roll(values, width - half, 1), pltpu.roll(values, half, 1))


def turn(cos_ref, sin_ref, r):
    cos, sin = cos_ref[r], sin_ref[r]
    return (
        jnp.concatenate([cos, cos, cos, cos], axis=0).T,
        jnp.concatenate([-sin, sin, -sin, sin], axis=0).T,
    )


def place_of(span_ref, oz, r):
    blocks = lax.axis_size("blk")
    return span_ref[r // INNER * blocks + oz * INNER + r % INNER]


def qk_rows(qk_ref):
    gains = qk_ref[...]
    one = jnp.ones((1, gains.shape[1]), F32)
    query = jnp.concatenate([gains[0:1], gains[0:1]], axis=1)
    return query, jnp.concatenate([gains[1:2], one], axis=1)


def head_forward(raw, gain_vec, cos, sin, size):
    values = raw * head_rms(raw, size) * gain_vec
    return values * cos + swap_halves(values, size) * sin


def head_back(raw, gain_vec, cos, sin, size, grad):
    grad = grad * cos - swap_halves(grad, size) * sin
    inverse = head_rms(raw, size)
    shaped = grad * gain_vec
    mean = per_head(raw * shaped, size) * (1.0 / size)
    dgain = jnp.sum(grad * raw * inverse, axis=0, keepdims=True)
    return inverse * shaped - raw * (inverse * inverse * inverse * mean), dgain


def all_peers(place):
    y, c, z, x = place
    outer = lax.axis_size("blk") // INNER
    peers = []
    for k in range(outer):
        forth, back = lax.rem(z + k, outer), lax.rem(z + outer - k, outer)
        for bits in range(0 if k else 1, 8):
            py = 1 - y if bits & 4 else y
            pc = 1 - c if bits & 2 else c
            px = 1 - x if bits & 1 else x
            peers.append((device(py, pc, forth, px), device(py, pc, back, px), py, pc, back, px))
    return peers


def open_kernel(
    span_ref, x_ref, q_ref, k_ref, v_ref, g1_ref, g2_ref, gate_ref, up_ref, wo_ref, wd_ref, og_ref,
    qk_ref, freq_ref,
    qs_ref, kvs_ref, raw_ref, norm_ref, ogs_ref, gus_ref, wq_ref, gain_ref, wos_ref, wds_ref,
    cos_ref, sin_ref,
    ss, rs, w_ref, g_ref, gs_ref, xp_ref, gu_ref, kv_ref,
):
    place = y, c, z, x = here()
    me = rank(y, c, x)
    head = y * CORES + c
    mail = Mail((ss, rs))
    peers = all_peers(place)
    plane, w_rows, cols = w_ref.shape
    heads, outer = wq_ref.shape[:2]
    q_cols = q_ref.shape[1] // plane
    k_cols = k_ref.shape[1] // plane
    g_ref[...] = jnp.zeros_like(g_ref)
    g_ref[0:1, :w_rows] = g1_ref[...].astype(F32)
    g_ref[0:1, LANES // 2 : LANES // 2 + w_rows] = g2_ref[...].astype(F32)
    keys, values = k_ref[...].astype(F32), v_ref[...].astype(F32)
    for p in range(plane):
        at = slice(p * k_cols, (p + 1) * k_cols)
        pair = jnp.concatenate([keys[:, at], values[:, at]], axis=1)
        w_ref[p, :, :q_cols] = q_ref[:, p * q_cols : (p + 1) * q_cols]
        w_ref[p, :, q_cols:] = pair.astype(BF16)
    greet([p[0] for p in peers])
    w_base, g_base = mail.take(len(peers)), mail.take(len(peers))
    rows = PlaneGather(mail, place, x_ref, xp_ref)
    grads = PlaneGather(mail, place, og_ref, ogs_ref)
    swap = PlaneSwap(mail, place, gu_ref, gus_ref)
    block = RowsOut(mail, place, wo_ref, wos_ref)
    down = LineGather(mail, place, wd_ref, lambda oz: wds_ref.at[oz])
    half = plane // 2
    pairs = []
    for part in range(2):
        at = pl.ds(part * half, half)
        pairs.append(
            LineGather(mail, place, kv_ref.at[at], lambda oz, at=at: kvs_ref.at[oz, at])
        )
    for slot, (dev, _, py, pc, _, px) in reversed(list(enumerate(peers))):
        mail.send(g_base + slot, g_ref, gs_ref.at[z, me], dev)
        mail.send(w_base + slot, w_ref.at[rank(py, pc, px)], wq_ref.at[head, z, x], dev)
    rows.begin()
    gs_ref[z, me] = g_ref[...]
    wq_ref[head, z, x] = w_ref[me]
    wds_ref[z] = wd_ref[...]
    f_cols = gate_ref.shape[1] // (heads * outer * INNER)
    main = outer * f_cols // LANES * LANES
    for oh in range(heads):
        span = outer * INNER * f_cols
        cut = []
        for ref in (gate_ref, up_ref):
            wide = ref[:, oh * span : (oh + 1) * span].astype(F32)
            cut.append(
                [
                    jnp.concatenate(
                        [
                            wide[:, (oz * INNER + ox) * f_cols : (oz * INNER + ox + 1) * f_cols]
                            for oz in range(outer)
                        ],
                        axis=1,
                    )
                    for ox in range(INNER)
                ]
            )
        for ox in range(INNER):
            gate, up = cut[0][ox], cut[1][ox]
            p = oh * INNER + ox
            gu_ref[p, :, :main] = gate[:, :main].astype(BF16)
            gu_ref[p, :, main : 2 * main] = up[:, :main].astype(BF16)
            tails = jnp.concatenate([gate[:, main:], up[:, main:]], axis=1)
            gu_ref[p, :, 2 * main :] = tails.astype(BF16)
    rows.middle()
    tok = x_ref.shape[0]
    for r in range(plane):
        first = place_of(span_ref, z, r) * tok
        where_at = (first + lanes((1, tok))).astype(F32)
        angles = where_at * freq_ref[...]
        cos_ref[r] = jnp.cos(angles)
        sin_ref[r] = jnp.sin(angles)
    rows.end()
    for slot, (_, dev, py, pc, oz, px) in enumerate(peers):
        mail.arrive(g_base + slot, gs_ref.at[oz, rank(py, pc, px)], dev)
    gain_ref[...] = jnp.zeros_like(gain_ref)
    for row in range(2):
        first = row * LANES // 2
        gain_ref[row : row + 1] = jnp.concatenate(
            [
                gs_ref[oz, oh * INNER + ox][:, first : first + w_rows]
                for oh in range(heads)
                for oz in range(outer)
                for ox in range(INNER)
            ],
            axis=1,
        )
    gain_one = gain_ref[0:1]

    def one_norm(r, carry):
        rows_in = xp_ref[r].astype(F32)
        norm_ref[r] = (rows_in * rms_of(rows_in) * gain_one).astype(BF16)
        return carry

    lax.fori_loop(0, plane, one_norm, 0)
    for slot, (_, dev, py, pc, oz, px) in enumerate(peers):
        mail.arrive(w_base + slot, wq_ref.at[py * CORES + pc, oz, px], dev)
    block.begin()
    grads.begin()
    down.begin()
    size = q_cols // 2
    gain_q, gain_k = qk_rows(qk_ref)
    weights = wq_ref[...].reshape(heads * outer * INNER * w_rows, cols)

    def one_block(r, carry):
        raw = jnp.dot(norm_ref[r], weights, preferred_element_type=F32)
        raw_ref[r] = raw
        cos, sin = turn(cos_ref, sin_ref, r)
        qs_ref[r] = head_forward(raw[:, :q_cols], gain_q, cos, sin, size).astype(BF16)
        pair = raw[:, q_cols:]
        turned = head_forward(pair, gain_k, cos, sin, size)
        kv_ref[r] = jnp.where(lanes(pair.shape) < size, turned, pair).astype(BF16)
        return carry

    for part in range(2):
        lax.fori_loop(part * half, (part + 1) * half, one_block, 0)
        pairs[part].begin()
    kvs_ref[z] = kv_ref[...]
    grads.middle()
    swap.begin()
    pairs[0].relay()
    pairs[1].relay()
    down.relay()
    grads.end()
    swap.end()
    block.end()
    pairs[0].end()
    pairs[1].end()
    down.end()
    mail.close()


def mix_kernel(
    att_ref, wo_ref, x_ref, gain_ref,
    mid_ref, n2_ref,
    ss, rs, parts, own, *bufs,
):
    place = here()
    mail = Mail((ss, rs))
    greet(list(near(place)))

    def make(block):
        parts[block] = jnp.dot(
            att_ref[block], wo_ref[...], preferred_element_type=F32
        ).astype(BF16)

    summed = PlaneScatter(mail, place, parts, mid_ref, bufs, make)
    rows = PlaneGather(mail, place, own, n2_ref)
    summed.begin()
    summed.middle()
    summed.end()
    middle = x_ref[...].astype(F32) + mid_ref[...]
    mid_ref[...] = middle
    own[...] = (middle * rms_of(middle) * gain_ref[1:2]).astype(BF16)
    rows.begin()
    rows.middle()
    rows.end()
    mail.close()


def narrow_kernel(
    parts_ref, mid_ref, og_ref, gain_ref,
    dmid_ref, dmids_ref, g2_ref,
    ss, rs, own, *bufs,
):
    place = here()
    mail = Mail((ss, rs))
    greet(list(near(place)))
    summed = PlaneScatter(mail, place, parts_ref, dmid_ref, bufs)
    rows = PlaneGather(mail, place, own, dmids_ref)
    summed.begin()
    summed.middle()
    summed.end()
    back, dgain = rms_back(mid_ref[...], gain_ref[1:2], dmid_ref[...])
    dmiddle = og_ref[...].astype(F32) + back
    dmid_ref[...] = dmiddle
    own[...] = dmiddle.astype(BF16)
    g2_ref[...] = dgain
    rows.begin()
    rows.middle()
    rows.end()
    mail.close()


def close_kernel(
    dq_ref, dkv_ref, outp_ref, op_ref, mid_ref, raw_ref, norm_ref, w_ref, qk_ref, cos_ref, sin_ref,
    x_ref, dmid_ref, gain_ref, g2_ref, dg_ref, *refs,
):
    outer = lax.axis_size("blk") // INNER
    gu_refs, refs = refs[:outer], refs[outer:]
    (out_ref, ops_ref, in_ref, ws_ref, gus_ref, down_ref, small_ref,
     ss, rs, dqkv, parts, acc, grads, held, gu_own, small, p_got, z_got, op_got, *bufs) = refs
    place = y, c, z, x = here()
    me = rank(y, c, x)
    mail = Mail((ss, rs))
    peers, line = plane_peers(place), line_peers(place)
    swap = PlaneSwap(mail, place, gu_own, gus_ref)
    pairs = LineScatter(mail, place, dkv_ref, bufs[0:3])
    weights = LineScatter(mail, place, grads, bufs[3:6])
    down = LineScatter(mail, place, dg_ref, bufs[6:9])
    block = RowsBack(mail, place, op_ref, op_got, ops_ref)

    def make(oblock):
        parts[oblock] = lax.dot_general(
            dqkv[oblock], w_ref[...], NT, preferred_element_type=F32
        ).astype(BF16)

    outs = PlaneScatter(mail, place, outp_ref, acc, bufs[9:14])
    rows = PlaneScatter(mail, place, parts, acc, bufs[14:19], make)
    greet([p[0] for p in peers] + blk_peers(place))
    pairs.begin()
    outs.begin()
    block.begin()

    count, tok, q_cols = dq_ref.shape
    size = q_cols // 2
    gain_q, gain_k = qk_rows(qk_ref)

    def one_query(r, total):
        cos, sin = turn(cos_ref, sin_ref, r)
        raw = raw_ref[r, :, :q_cols]
        dq, part = head_back(raw, gain_q, cos, sin, size, dq_ref[r].astype(F32))
        dqkv[r, :, :q_cols] = dq.astype(BF16)
        return total + part

    zero = jnp.zeros((1, q_cols), F32)
    q_sum = lax.fori_loop(0, count, one_query, zero)
    pairs.relay()
    down.begin()
    outs.middle()
    total = gu_refs[0][...].astype(F32)
    for ref in gu_refs[1:]:
        total = total + ref[...].astype(F32)
    gu_own[...] = total.astype(BF16).reshape(gu_own.shape)
    outs.end()
    swap.begin()
    out_ref[...] = (mid_ref[...] + acc[...]).astype(BF16)
    dqkv[:, :, q_cols:] = pairs.end().astype(BF16)

    def one_key(r, total):
        cos, sin = turn(cos_ref, sin_ref, r)
        dkv = dqkv[r, :, q_cols:].astype(F32)
        dk, part = head_back(raw_ref[r, :, q_cols:], gain_k, cos, sin, size, dkv)
        dqkv[r, :, q_cols:] = jnp.where(lanes(dk.shape) < size, dk, dkv).astype(BF16)
        return total + part

    k_sum = lax.fori_loop(0, count, one_key, zero)
    width = norm_ref.shape[2]
    w_grad = lax.dot_general(
        norm_ref[...].reshape(count * tok, width),
        dqkv[...].reshape(count * tok, -1),
        TN,
        preferred_element_type=F32,
    ).astype(BF16)
    heads, w_rows = grads.shape[1], grads.shape[3]
    stride = INNER * w_rows
    for oz in range(outer):
        for oh in range(heads):
            first = (oh * outer + oz) * stride
            grads[oz, oh] = w_grad[first : first + stride].reshape(INNER, w_rows, -1)
    weights.begin()
    rows.begin()
    rows.middle()
    weights.relay()
    rows.end()
    back, dgain = rms_back(x_ref[...].astype(F32), gain_ref[0:1], acc[...])
    in_ref[...] = (dmid_ref[...] + back).astype(BF16)
    small[...] = jnp.zeros_like(small)
    small[0:1] = dgain
    small[1:2] = g2_ref[...]
    small[2:3, :q_cols] = q_sum
    small[3:4, :q_cols] = k_sum
    p_base, z_base, w_base = mail.take(7), mail.take(len(line)), mail.take(7)
    for slot, (dev, other, _) in enumerate(peers):
        mail.send(p_base + slot, small, p_got.at[me], dev)
    p_got[me] = small[...]
    down.relay()
    held[...] = weights.end().reshape(held.shape)
    for slot, (dev, other, _) in enumerate(peers):
        mail.send(w_base + slot, held.at[other], ws_ref.at[me], dev)
    ws_ref[me] = held[me]
    for slot, (dev, other, _) in enumerate(peers):
        mail.arrive(p_base + slot, p_got.at[other], dev)
    z_got[z] = jnp.sum(p_got[...], axis=0)
    for slot, (dev, _, _) in enumerate(line):
        mail.send(z_base + slot, z_got.at[z], z_got.at[z], dev)
    swap.end()
    block.end()
    down_ref[...] = down.end()
    for slot, (dev, other, _) in enumerate(peers):
        mail.arrive(w_base + slot, ws_ref.at[other], dev)
    for slot, (dev, _, back) in enumerate(line):
        mail.arrive(z_base + slot, z_got.at[back], dev)
    small_ref[...] = jnp.sum(z_got[...], axis=0)
    mail.close()


def finish_kernel(ws_ref, gus_ref, small_ref, *refs):
    n1_ref, n2_ref, q_ref, k_ref, v_ref, qk_ref, gate_ref, up_ref = refs[-8:]
    passed = refs[:-8]
    for src, dst in zip(passed[: len(passed) // 2], passed[len(passed) // 2 :]):
        dst[...] = src[...]
    plane, w_rows, _ = ws_ref.shape
    q_cols = q_ref.shape[1] // plane
    k_cols = q_cols // 2
    for p in range(0, plane, 2):
        one, two = ws_ref[p], ws_ref[p + 1]
        q_ref[:, p * q_cols : (p + 1) * q_cols] = one[:, :q_cols]
        q_ref[:, (p + 1) * q_cols : (p + 2) * q_cols] = two[:, :q_cols]
        at = slice(p * k_cols, (p + 2) * k_cols)
        left = lanes((w_rows, q_cols)) < k_cols
        one, two = one[:, q_cols:], two[:, q_cols:]
        k_ref[:, at] = jnp.where(left, one, pltpu.roll(two, k_cols, 1))
        v_ref[:, at] = jnp.where(left, pltpu.roll(one, k_cols, 1), two)
    width = small_ref.shape[1]
    own = (lax.axis_index("head") * lax.axis_size("blk") + lax.axis_index("blk")) * w_rows
    move = lax.rem(width - own, width)
    totals = pltpu.roll(small_ref[...], move, 1)
    n1_ref[...] = totals[0:1, :w_rows]
    n2_ref[...] = totals[1:2, :w_rows]
    sums = small_ref[...]
    query = sums[2:3, :k_cols] + sums[2:3, k_cols : 2 * k_cols]
    qk_ref[...] = jnp.concatenate([query, sums[3:4, :k_cols]], axis=0)
    outer = lax.axis_size("blk") // INNER
    heads = plane // INNER
    ff = gus_ref.shape[2] // 2
    main = ff // LANES * LANES
    tail = ff - main
    f_rows = ff // outer
    for col, out in ((0, gate_ref), (1, up_ref)):
        for oh in range(heads):
            cols = []
            for ox in range(INNER):
                block = gus_ref[oh * INNER + ox].astype(F32)
                rest = 2 * main + col * tail
                cols.append(
                    jnp.concatenate(
                        [block[:, col * main : (col + 1) * main], block[:, rest : rest + tail]],
                        axis=1,
                    )
                )
            span = INNER * ff
            out[:, oh * span : (oh + 1) * span] = jnp.concatenate(
                [
                    cols[ox][:, oz * f_rows : (oz + 1) * f_rows]
                    for oz in range(outer)
                    for ox in range(INNER)
                ],
                axis=1,
            )


def feed_kernel(n2_ref, og_ref, wd_ref, *refs):
    outer = lax.axis_size("blk") // INNER
    pieces, refs = refs[:outer], refs[outer:]
    out_ref, dn_ref, dg_ref = refs[:3]
    chunks = refs[3 : 3 + outer]
    wgu, hid, dgu, gg = refs[3 + outer :]
    z = here()[2]
    heads, stride, _ = pieces[0].shape
    ff = wd_ref.shape[0]
    main = ff // LANES * LANES
    tail = ff - main
    for k, piece in enumerate(pieces):
        oz = lax.rem(z + outer - k, outer)
        for oh in range(heads):
            at = pl.multiple_of((oh * outer + oz) * stride, stride)
            wgu[pl.ds(at, stride)] = piece[oh]
    f_rows = ff // outer
    plane, rows, width = n2_ref.shape

    def both(gate, up, dhid):
        sig = 1.0 / (1.0 + jnp.exp(-gate))
        act = gate * sig
        return act * up, dhid * up * (sig * (1.0 + gate * (1.0 - sig))), dhid * act

    def one_block(b, carry):
        pair = pl.ds(2 * b, 2)
        at = pl.ds(pl.multiple_of(b * 2 * rows, 2 * rows), 2 * rows)
        block = n2_ref[pair].reshape(2 * rows, width)
        grad = og_ref[pair].reshape(2 * rows, width)
        gu = jnp.dot(block, wgu[...], preferred_element_type=F32)
        dhid = lax.dot_general(grad, wd_ref[...], NT, preferred_element_type=F32)
        h, dgate, dup = both(gu[:, :main], gu[:, main : 2 * main], dhid[:, :main])
        hid[at, :main] = h.astype(BF16)
        dgu[at, :main] = dgate.astype(BF16)
        dgu[at, main : 2 * main] = dup.astype(BF16)
        ends = gu[:, 2 * main :]
        left = lanes(ends.shape) < tail
        other = pltpu.roll(ends, tail, 1)
        dend = dhid[:, main:]
        dend = jnp.concatenate([dend, dend], axis=1)
        h, dgate, dup = both(jnp.where(left, ends, other), jnp.where(left, other, ends), dend)
        hid[at, main:] = h[:, :tail].astype(BF16)
        dgu[at, 2 * main :] = jnp.where(left, dgate, dup).astype(BF16)
        down = jnp.dot(hid[at], wd_ref[...], preferred_element_type=F32)
        out_ref[pair] = down.astype(BF16).reshape(2, rows, width)
        narrow = lax.dot_general(dgu[at], wgu[...], NT, preferred_element_type=F32)
        dn_ref[pair] = narrow.astype(BF16).reshape(2, rows, width)
        return carry

    lax.fori_loop(0, plane // 2, one_block, 0)
    n2_width = width // heads
    w_rows = stride // INNER

    def one_head(oh, carry):
        cols = pl.ds(pl.multiple_of(oh * n2_width, n2_width), n2_width)
        grad = lax.dot_general(
            n2_ref[:, :, cols].reshape(plane * rows, n2_width),
            dgu[...],
            TN,
            preferred_element_type=F32,
        )
        for oz in range(outer):
            for ox in range(INNER):
                first = oz * stride + ox * w_rows
                gg[oz, oh * INNER + ox] = grad[first : first + w_rows].astype(BF16)
        return carry

    lax.fori_loop(0, heads, one_head, 0)
    for k, chunk in enumerate(chunks):
        chunk[...] = gg[lax.rem(z + k, outer)]
    grads = og_ref[...].reshape(plane * rows, width)
    down = lax.dot_general(hid[...], grads, TN, preferred_element_type=F32)
    for oz in range(outer):
        dg_ref[oz] = down[oz * f_rows : (oz + 1) * f_rows].astype(BF16)


SPANS = 4
LOG2E = math.log2(math.e)


def stack_left(block, size):
    wide = block.astype(F32)
    left = lanes(wide.shape) < size
    first = jnp.where(left, wide, 0.0)
    second = jnp.where(left, pltpu.roll(wide, size, 1), 0.0)
    return jnp.concatenate([first, second], axis=0).astype(BF16)


def stack_right(block, size):
    wide = block.astype(F32)
    right = lanes(wide.shape) >= size
    first = jnp.where(right, pltpu.roll(wide, size, 1), 0.0)
    second = jnp.where(right, wide, 0.0)
    return jnp.concatenate([first, second], axis=0).astype(BF16)


def span_table(span_ref, at_ref, plane):
    def one(block, carry):
        at_ref[place_of(span_ref, block // plane, block % plane)] = block
        return carry

    lax.fori_loop(0, at_ref.shape[0], one, 0)


def forward_kernel(span_ref, q_ref, kv_ref, out_ref, lse_ref, at_ref, keys, ones):
    count, rows, size2 = q_ref.shape
    size = size2 // 2
    scale = float(size) ** (-0.5) * LOG2E
    step = SPANS * rows
    z = here()[2]
    span_table(span_ref, at_ref, count)

    def place_rows(p, carry):
        block = kv_ref[at_ref[p]]
        keys[pl.ds(p * rows, rows)] = block
        ones[pl.ds(p * rows, rows)] = jnp.where(lanes(block.shape) < size, 1.0, block).astype(BF16)
        return carry

    lax.fori_loop(0, kv_ref.shape[0], place_rows, 0)

    def one_block(r, carry):
        place = place_of(span_ref, z, r)
        queries = stack_left(q_ref[r], size)

        def weights(c):
            part = keys[pl.ds(c * step, step)]
            scores = lax.dot_general(queries, part, NT, preferred_element_type=F32)
            return jnp.exp2(scores * scale)

        def mix(c, held, total):
            part = ones[pl.ds(c * step, step)]
            return total + jnp.dot(held.astype(BF16), part, preferred_element_type=F32)

        def full(c, total):
            return mix(c, weights(c), total)

        last = place // SPANS
        total = lax.fori_loop(0, last, full, jnp.zeros((2 * rows, size2), F32))
        held = weights(last)
        row = lax.broadcasted_iota(jnp.int32, held.shape, 0)
        row = jnp.where(row >= rows, row - rows, row) + (place - last * SPANS) * rows
        held = jnp.where(lanes(held.shape) <= row, held, 0.0)
        total = mix(last, held, total)
        divided = total / total[:, :1]
        left = lanes((rows, size2)) < size
        out_ref[r] = jnp.where(left, pltpu.roll(divided[:rows], size, 1), divided[rows:]).astype(
            BF16
        )
        lse_ref[r] = jnp.log2(total.T[:8])
        return carry

    lax.fori_loop(0, count, one_block, 0)


def backward_kernel(
    span_ref, q_ref, kv_ref, out_ref, dmid_ref, wo_ref, lse_ref,
    dq_ref, dkv_ref, op_ref,
    at_ref, keys, turned, sums,
):
    count, rows, size2 = q_ref.shape
    size = size2 // 2
    scale = float(size) ** (-0.5)
    step = SPANS * rows
    spans = kv_ref.shape[0]
    z = here()[2]
    span_table(span_ref, at_ref, count)
    width = dmid_ref.shape[2]
    op = lax.dot_general(
        out_ref[...].reshape(count * rows, size2),
        dmid_ref[...].reshape(count * rows, width),
        TN,
        preferred_element_type=F32,
    )
    per, inner, w_rows, _ = op_ref.shape
    for j in range(per):
        for ox in range(inner):
            first = (j * inner + ox) * w_rows
            op_ref[j, ox] = op[first : first + w_rows].astype(BF16)

    def place_rows(p, carry):
        block = kv_ref[at_ref[p]]
        keys[pl.ds(p * rows, rows)] = block
        turned[:, pl.ds(p * rows, rows)] = block.astype(F32).T.astype(BF16)
        return carry

    lax.fori_loop(0, spans, place_rows, 0)
    sums[...] = jnp.zeros_like(sums)

    def one_block(r, carry):
        place = place_of(span_ref, z, r)
        queries = stack_left(q_ref[r], size)
        grad = lax.dot_general(dmid_ref[r], wo_ref[...], NT, preferred_element_type=F32)
        grad = grad.astype(BF16)
        grads = stack_right(grad, size)
        both = (grad.astype(F32) * out_ref[r].astype(F32)).T
        delta = jnp.concatenate(
            [jnp.sum(both[:size], axis=0)[None], jnp.sum(both[size:], axis=0)[None]], axis=1
        )
        lse = lse_ref[r][:1]

        def one_step(c, total, masked):
            at = pl.ds(pl.multiple_of(c * step, step), step)
            part = keys[at]
            scores = lax.dot_general(part, queries, NT, preferred_element_type=F32)
            prob = jnp.exp2(scores * (scale * LOG2E) - lse)
            if masked:
                key = lax.broadcasted_iota(jnp.int32, prob.shape, 0)
                row = lanes(prob.shape)
                row = jnp.where(row >= rows, row - rows, row) + (place - c * SPANS) * rows
                prob = jnp.where(key <= row, prob, 0.0)
            dprob = lax.dot_general(part, grads, NT, preferred_element_type=F32)
            dscore = (prob * (dprob - delta)).astype(BF16)
            sums[at] += jnp.dot(dscore, queries, preferred_element_type=F32) + jnp.dot(
                prob.astype(BF16), grads, preferred_element_type=F32
            )
            return total + jnp.dot(turned[:, at], dscore, preferred_element_type=F32)

        last = place // SPANS
        total = lax.fori_loop(
            0, last, lambda c, t: one_step(c, t, False), jnp.zeros((size2, 2 * rows), F32)
        )
        total = one_step(last, total, True).T * scale
        left = lanes((rows, size2)) < size
        dq_ref[r] = jnp.where(left, total[:rows], pltpu.roll(total[rows:], size, 1)).astype(BF16)
        return carry

    lax.fori_loop(0, count, one_block, 0)

    def give_rows(p, carry):
        block = sums[pl.ds(p * rows, rows)]
        factor = jnp.where(lanes(block.shape) < size, scale, 1.0)
        dkv_ref[at_ref[p]] = (block * factor).astype(BF16)
        return carry

    lax.fori_loop(0, spans, give_rows, 0)


def local_call(body, scalars, args, outs, scratch, flops):
    vmem = pl.BlockSpec(memory_space=pltpu.VMEM)
    smem = pl.BlockSpec(memory_space=pltpu.SMEM)
    return pl.pallas_call(
        body,
        out_shape=tuple(jax.ShapeDtypeStruct(shape, dtype) for shape, dtype in outs),
        in_specs=[smem] * len(scalars) + [vmem] * len(args),
        out_specs=tuple([vmem] * len(outs)),
        scratch_shapes=scratch,
        cost_estimate=pl.CostEstimate(flops=flops, bytes_accessed=8 << 20, transcendentals=0),
        compiler_params=pltpu.CompilerParams(vmem_limit_bytes=60 * 1024 * 1024),
    )(*scalars, *args)


def shifts(outer, step):
    return [
        (z * INNER + x, ((z + step) % outer) * INNER + x)
        for z in range(outer)
        for x in range(INNER)
    ]


def local(
    block_input,
    span_order,
    norm1_gain,
    w_query,
    key_weight,
    value_weight,
    qk_gain,
    w_out,
    norm2_gain,
    w_gate,
    w_up,
    w_down,
    out_grad,
):
    heads = lax.axis_size("head")
    blocks = lax.axis_size("blk")
    outer = blocks // INNER
    plane = heads * INNER
    rows, width = block_input.shape
    size = qk_gain.shape[1]
    w_rows = w_query.shape[0]
    f_rows = w_down.shape[0]
    q_cols = w_query.shape[1] // plane
    a_cols = 2 * q_cols
    ff = f_rows * outer
    spans = outer * plane
    n_line = outer - 1
    stride = INNER * w_rows

    def along(piece):
        moved = [
            lax.ppermute(piece, "blk", shifts(outer, step)) for step in range(1, outer)
        ]
        return [piece] + moved

    half = size // 2
    frequency = jnp.exp(jnp.arange(half, dtype=F32) * F32(-2.0 * math.log(THETA) / size))
    frequency = jnp.broadcast_to(frequency[:, None], (half, rows))
    (queries, kv_all, raw, normed, og_all, gu_piece, wqkv, gains, out_mine, down_full,
     cosine, sine) = call(
        open_kernel,
        1,
        [
            ((plane, rows, q_cols), BF16),
            ((outer, plane, rows, q_cols), BF16),
            ((plane, rows, a_cols), F32),
            ((plane, rows, width), BF16),
            ((plane, rows, width), BF16),
            ((plane, w_rows, 2 * ff), BF16),
            ((heads, outer, INNER, w_rows, a_cols), BF16),
            ((8, width), F32),
            ((outer // INNER, INNER, w_rows, width), BF16),
            ((outer, f_rows, width), BF16),
            ((plane, half, rows), F32),
            ((plane, half, rows), F32),
        ],
        (
            block_input,
            w_query,
            key_weight,
            value_weight,
            norm1_gain.reshape(1, w_rows),
            norm2_gain.reshape(1, w_rows),
            w_gate,
            w_up,
            w_out,
            w_down,
            out_grad,
            qk_gain,
            frequency,
        ),
        2 * (outer * plane - 1)
        + 2 * PlaneGather.COPIES
        + PlaneSwap.COPIES
        + outer
        + 3 * LineGather.copies(outer),
        [
            pltpu.VMEM((plane, w_rows, a_cols), BF16),
            pltpu.VMEM((1, LANES), F32),
            pltpu.VMEM((outer, plane, 1, LANES), F32),
            pltpu.VMEM((plane, rows, width), BF16),
            pltpu.VMEM((plane, w_rows, 2 * ff), BF16),
            pltpu.VMEM((plane, rows, q_cols), BF16),
        ],
        (span_order,),
    )
    wqkv = wqkv.reshape(width, a_cols)
    out_mine = out_mine.reshape(q_cols, width)
    down_full = down_full.reshape(ff, width)
    gu_pieces = along(gu_piece.reshape(heads, stride, 2 * ff))
    kv_blocks = kv_all.reshape(spans, rows, q_cols)
    pairs = plane * rows * spans * rows * q_cols
    attended, log_total = local_call(
        forward_kernel,
        (span_order,),
        (queries, kv_blocks),
        [((plane, rows, q_cols), BF16), ((plane, 8, 2 * rows), F32)],
        [
            pltpu.SMEM((spans,), jnp.int32),
            pltpu.VMEM((spans * rows, q_cols), BF16),
            pltpu.VMEM((spans * rows, q_cols), BF16),
        ],
        4 * pairs,
    )
    middle, normed2 = call(
        mix_kernel,
        3,
        [((rows, width), F32), ((plane, rows, width), BF16)],
        (attended, out_mine, block_input, gains),
        PlaneScatter.COPIES + PlaneGather.COPIES,
        [pltpu.VMEM((plane, rows, width), BF16), pltpu.VMEM((rows, width), BF16)]
        + PlaneScatter.scratch(rows, width),
    )

    out_parts, dn_parts, down_grad, *gu_grads = local_call(
        feed_kernel,
        (),
        (normed2, og_all, down_full, *gu_pieces),
        [
            ((plane, rows, width), BF16),
            ((plane, rows, width), BF16),
            ((outer, f_rows, width), BF16),
        ]
        + [((plane, w_rows, 2 * ff), BF16)] * outer,
        [
            pltpu.VMEM((width, 2 * ff), BF16),
            pltpu.VMEM((plane * rows, ff), BF16),
            pltpu.VMEM((plane * rows, 2 * ff), BF16),
            pltpu.VMEM((outer, plane, w_rows, 2 * ff), BF16),
        ],
        18 * plane * rows * width * ff,
    )
    gu_sums = [gu_grads[0]] + [
        lax.ppermute(gu_grads[step], "blk", shifts(outer, step)) for step in range(1, outer)
    ]
    dmiddle, dmid_all, norm2_grad = call(
        narrow_kernel,
        4,
        [((rows, width), F32), ((plane, rows, width), BF16), ((1, width), F32)],
        (dn_parts, middle, out_grad, gains),
        PlaneScatter.COPIES + PlaneGather.COPIES,
        [pltpu.VMEM((rows, width), BF16)] + PlaneScatter.scratch(rows, width),
    )

    dqueries, dkv, out_proj = local_call(
        backward_kernel,
        (span_order,),
        (queries, kv_blocks, attended, dmid_all, out_mine, log_total),
        [
            ((plane, rows, q_cols), BF16),
            ((spans, rows, q_cols), BF16),
            ((outer // INNER, INNER, w_rows, width), BF16),
        ],
        [
            pltpu.SMEM((spans,), jnp.int32),
            pltpu.VMEM((spans * rows, q_cols), BF16),
            pltpu.VMEM((q_cols, spans * rows), BF16),
            pltpu.VMEM((spans * rows, q_cols), F32),
        ],
        10 * pairs,
    )
    block_output, out_proj_grad, input_grad, w_own, gu_own, down_out, small = call(
        close_kernel,
        5,
        [
            ((rows, width), BF16),
            ((w_rows, width), F32),
            ((rows, width), BF16),
            ((plane, w_rows, a_cols), F32),
            ((plane, w_rows, 2 * ff), BF16),
            ((f_rows, width), F32),
            ((8, width), F32),
        ],
        (
            dqueries,
            dkv.reshape(outer, plane, rows, q_cols),
            out_parts,
            out_proj,
            middle,
            raw,
            normed,
            wqkv,
            qk_gain,
            cosine,
            sine,
            block_input,
            dmiddle,
            gains,
            norm2_grad,
            down_grad,
            *gu_sums,
        ),
        3 * LineGather.copies(outer)
        + n_line
        + 14
        + outer
        + 2 * PlaneScatter.COPIES
        + PlaneSwap.COPIES,
        [
            pltpu.VMEM((plane, rows, a_cols), BF16),
            pltpu.VMEM((plane, rows, width), BF16),
            pltpu.VMEM((rows, width), F32),
            pltpu.VMEM((outer, heads, INNER, w_rows, a_cols), BF16),
            pltpu.VMEM((plane, w_rows, a_cols), F32),
            pltpu.VMEM((plane, w_rows, 2 * ff), BF16),
            pltpu.VMEM((8, width), F32),
            pltpu.VMEM((plane, 8, width), F32),
            pltpu.VMEM((outer, 8, width), F32),
            pltpu.VMEM((outer, w_rows, width), BF16),
        ]
        + LineScatter.scratch(outer, (plane, rows, q_cols))
        + LineScatter.scratch(outer, (heads, INNER, w_rows, a_cols))
        + LineScatter.scratch(outer, (f_rows, width))
        + PlaneScatter.scratch(rows, width)
        + PlaneScatter.scratch(rows, width),
    )
    outs = local_call(
        finish_kernel,
        (),
        (w_own, gu_own, small, block_output, input_grad, out_proj_grad, down_out),
        [
            ((rows, width), BF16),
            ((rows, width), BF16),
            ((w_rows, width), F32),
            ((f_rows, width), F32),
            ((1, w_rows), F32),
            ((1, w_rows), F32),
            (w_query.shape, F32),
            (key_weight.shape, F32),
            (value_weight.shape, F32),
            ((2, size), F32),
            (w_gate.shape, F32),
            (w_up.shape, F32),
        ],
        [],
        1 << 20,
    )
    (block_output, input_grad, out_proj_grad, down_grad, norm1_grad, norm2_grad,
     query_grad, key_grad, value_grad, qk_gain_grad, gate_grad, up_grad) = outs
    return (
        block_output,
        input_grad,
        norm1_grad.reshape(w_rows),
        query_grad,
        key_grad,
        value_grad,
        qk_gain_grad,
        out_proj_grad,
        norm2_grad.reshape(w_rows),
        gate_grad,
        up_grad,
        down_grad,
    )


def solution(mesh):
    split = P(("head", "blk"), None)
    line = P(("head", "blk"))
    in_specs = (split, P(), line, split, split, split, P(), split, line, split, split, split, split)
    out_specs = (split, split, line, split, split, split, P(), split, line, split, split, split)
    return jax.shard_map(local, mesh=mesh, in_specs=in_specs, out_specs=out_specs, check_vma=False)
```
